128 devices in a mesh: cp: 16 (over y, x), tp: 8 (over z, core).
Axes of the slice: x: 4, y: 4, z: 4, core: 2. Of those that a mesh axis runs over, the one named last changes fastest.
Arguments:
- tokens: bfloat16 [8192, 4096], P('cp'), may hold values from -150 to 150
- gain: bfloat16 [4096], replicated, may hold values from 0.099609375 to 1.8984375
- w_query: bfloat16 [4096, 4096], P(None, 'tp'), may hold values from -3 to 3
- w_key: bfloat16 [4096, 1024], P(None, 'tp'), may hold values from -1 to 1
- w_value: bfloat16 [4096, 1024], P(None, 'tp'), may hold values from -0.09375 to 0.09375
- w_out: bfloat16 [4096, 4096], P('tp'), may hold values from -0.09375 to 0.09375
- doc_ids: int32 [8192], replicated, may hold values from 0 to 15, as said below
Outputs:
- mixed: bfloat16 [8192, 4096], P('cp', 'tp')
The draws below stay inside these ranges and needn't reach their ends.
Inputs may be any that keep to these rules, and one draw needn't show every extreme that they name: `doc_ids`: document numbers never fall along the sequence, and every number of the range is used; every document covers at most 2305 positions; two documents cover exactly 2305, each beginning at the first position of a stretch, one in the first 4096 positions and one starting in the last 4096.
All inputs are finite; a program needn't handle non-finite values.
Results may differ from the reference program's by a relative error of at most 0.015.
Values may be sent and summed in bfloat16 or wider, within the bound.
A program may use at most 128 MiB of HBM per device.

```python
import math
import jax
import jax.numpy as jnp
from jax import lax

D = 4096
HEADS = 32
KV_HEADS = 8
HD = 128
TOK_DEV = 512
REACH = 9
STRETCH = 256
STRETCHES = 32
TOKENS = 8192
DOC_MOST = 2305
DOCS = 16
N_CP = 16
N_TP = 8


def draw_tokens(key, part):
    keys = jax.random.split(jax.random.fold_in(key, 5), 3)
    row_scale = jnp.exp(jax.random.uniform(keys[1], (TOKENS, 1), jnp.float32, 0.0, jnp.log(10.0)))
    col_scale = jnp.exp(jax.random.uniform(keys[2], (1, D), jnp.float32, jnp.log(0.3), jnp.log(3.0)))
    base = jax.random.normal(keys[0], (TOKENS, D), jnp.float32)
    base = jnp.clip(base, -5.0, 5.0)
    return (base * row_scale * col_scale).astype(jnp.bfloat16)


def paired_weights(key):
    keys = jax.random.split(jax.random.fold_in(key, 11), 3)
    fan_scale = D ** (-0.5)
    key_weight = jnp.clip(jax.random.normal(keys[0], (D, KV_HEADS * HD), jnp.float32), -5.0, 5.0) * fan_scale
    query_weight = jnp.clip(jax.random.normal(keys[2], (D, HEADS * HD), jnp.float32), -5.0, 5.0) * fan_scale
    return (jnp.clip(query_weight, -3.0, 3.0), jnp.clip(key_weight, -1.0, 1.0))


def draw_w_query(key, part):
    return paired_weights(key)[0].astype(jnp.bfloat16)


def draw_w_key(key, part):
    return paired_weights(key)[1].astype(jnp.bfloat16)


def draw_doc_ids(key, part):
    keys = jax.random.split(jax.random.fold_in(key, 23), 3)
    first_start = (jax.random.randint(keys[0], (), 1, N_CP // 2 - 1) * STRETCH).astype(jnp.int32)
    second_start = (jax.random.randint(keys[1], (), N_CP, 2 * N_CP - REACH) * STRETCH).astype(jnp.int32)
    places = jnp.arange(TOKENS, dtype=jnp.int32)
    inside_first = (places >= first_start) & (places <= first_start + DOC_MOST)
    inside_second = (places >= second_start) & (places <= second_start + DOC_MOST)
    blocked = inside_first | inside_second | (places == 0)
    ranks = jax.random.permutation(keys[2], TOKENS).astype(jnp.int32)
    scores = jnp.where(blocked, TOKENS + places, ranks).astype(jnp.int32)
    extra_cuts = jnp.argsort(scores, stable=True)[:DOCS - 5].astype(jnp.int32)
    fixed_cuts = jnp.stack([first_start, first_start + DOC_MOST, second_start, second_start + DOC_MOST]).astype(jnp.int32)
    cuts = jnp.concatenate([fixed_cuts, extra_cuts])
    return jnp.sum((places[:, None] >= cuts[None, :]).astype(jnp.int32), axis=1).astype(jnp.int32)


def block_scale(stream_key, extent, shards, low, high):
    loudness = 1.0
    for axis_at, shards_of in shards:
        heights = jax.random.uniform(jax.random.fold_in(jax.random.fold_in(stream_key, 6), axis_at), (shards_of,), jnp.float32, low / len(shards), high / len(shards))
        loudness = loudness * jnp.repeat(jnp.exp(heights), extent[axis_at] // shards_of).reshape((-1,) + (1,) * (len(extent) - 1 - axis_at))
    return loudness


def centred(key, dims, spread, limit, cuts=(), kind=jnp.bfloat16):
    factor_of = block_scale(key, dims, cuts, -0.22, 0.18) if cuts else 1.0
    values = jax.random.normal(key, dims, jnp.float32) * spread * factor_of
    return jnp.minimum(jnp.maximum(values, -limit), limit).astype(kind)


def setup_inputs(seed: int = 0) -> dict:
    splits = jax.random.split(jax.random.key(seed), 8)
    return {
        "tokens": draw_tokens(jax.random.fold_in(splits[7], 71), 0),
        "gain": jnp.clip(1.0 + 0.18 * jax.random.normal(splits[1], (D,), jnp.float32), 0.099609375, 1.8984375).astype(jnp.bfloat16),
        "w_query": draw_w_query(jax.random.fold_in(splits[7], 71), 0),
        "w_key": draw_w_key(jax.random.fold_in(splits[7], 71), 0),
        "w_value": centred(splits[4], (D, KV_HEADS * HD), D ** -0.5, 0.09375, ((1, 8),)),
        "w_out": centred(splits[5], (HEADS * HD, D), (HEADS * HD) ** -0.5, 0.09375, ((0, 8),)),
        "doc_ids": draw_doc_ids(jax.random.fold_in(splits[7], 71), 0),
    }


rope_theta = 500000.0
norm_epsilon = 1e-05
masked_score = -1e+30

def global_positions(row_index, tok_dev, cp_size):
    half_rows = tok_dev // 2
    device = row_index // tok_dev
    within = row_index % tok_dev
    stretch_index = jnp.where(within < half_rows, device, 2 * cp_size - 1 - device)
    return (stretch_index * half_rows + within % half_rows).astype(jnp.int32)

def rotary(heads, positions):
    head_size = heads.shape[-1]
    half_size = head_size // 2
    index = jnp.arange(half_size).astype(jnp.float32)
    freqs = jnp.power(jnp.float32(rope_theta), -2.0 * index / head_size)
    angles = positions.astype(jnp.float32)[:, None] * freqs[None, :]
    cosine = jnp.cos(angles)[:, None, :]
    sine = jnp.sin(angles)[:, None, :]
    lower = heads[..., :half_size]
    upper = heads[..., half_size:]
    return jnp.concatenate([lower * cosine - upper * sine, upper * cosine + lower * sine], axis=-1)

def normalize(tokens, gain):
    widened = tokens.astype(jnp.float32)
    factor = lax.rsqrt(lax.optimization_barrier(jnp.mean(widened * widened, axis=-1, keepdims=True)) + norm_epsilon)
    return (widened * factor * gain.astype(jnp.float32)).astype(jnp.bfloat16)

def reference(tokens, gain, w_query, w_key, w_value, w_out, doc_ids):
    group_size = HEADS // KV_HEADS
    scale = 1.0 / math.sqrt(HD)
    row_index = jnp.arange(TOKENS, dtype=jnp.int32)
    positions = global_positions(row_index, TOK_DEV, N_CP)
    normed = lax.optimization_barrier(normalize(tokens, gain))
    query = jnp.dot(normed, w_query, preferred_element_type=jnp.float32).reshape(TOKENS, HEADS, HD)
    query = lax.optimization_barrier(rotary(query, positions).astype(jnp.bfloat16))
    key_heads = jnp.dot(normed, w_key, preferred_element_type=jnp.float32).reshape(TOKENS, KV_HEADS, HD)
    key_heads = lax.optimization_barrier(rotary(key_heads, positions).astype(jnp.bfloat16))
    value_heads = jnp.dot(normed, w_value, preferred_element_type=jnp.float32).astype(jnp.bfloat16)
    value_heads = lax.optimization_barrier(value_heads).reshape(TOKENS, KV_HEADS, HD)
    order = jnp.zeros((TOKENS,), jnp.int32).at[positions].set(row_index)
    query_seq = query[order]
    pad_rows = REACH * STRETCH
    key_pad = jnp.concatenate([jnp.zeros((pad_rows, KV_HEADS, HD), jnp.bfloat16), key_heads[order]], axis=0)
    value_pad = jnp.concatenate([jnp.zeros((pad_rows, KV_HEADS, HD), jnp.bfloat16), value_heads[order]], axis=0)
    doc_pad = jnp.concatenate([jnp.full((pad_rows,), -1, jnp.int32), doc_ids.astype(jnp.int32)], axis=0)
    span = (REACH + 1) * STRETCH

    def one_stretch(stretch_index):
        start = (stretch_index * STRETCH).astype(jnp.int32)
        query_block = lax.dynamic_slice_in_dim(query_seq, start, STRETCH, 0).astype(jnp.float32)
        query_block = query_block.reshape(STRETCH, KV_HEADS, group_size, HD)
        key_block = lax.dynamic_slice_in_dim(key_pad, start, span, 0).astype(jnp.float32)
        value_block = lax.dynamic_slice_in_dim(value_pad, start, span, 0).astype(jnp.float32)
        query_doc = lax.dynamic_slice_in_dim(doc_ids.astype(jnp.int32), start, STRETCH, 0)
        key_doc = lax.dynamic_slice_in_dim(doc_pad, start, span, 0)
        query_pos = start + jnp.arange(STRETCH, dtype=jnp.int32)
        key_pos = start - pad_rows + jnp.arange(span, dtype=jnp.int32)
        allowed = (key_doc[None, :] == query_doc[:, None]) & (key_pos[None, :] <= query_pos[:, None])
        scores = jnp.einsum('tkgd,skd->kgts', query_block, key_block) * scale
        scores = jnp.where(allowed[None, None], scores, masked_score)
        row_max = lax.optimization_barrier(jnp.max(scores, axis=-1, keepdims=True))
        weights = jnp.where(allowed[None, None], jnp.exp(scores - row_max), 0.0)
        weight_total = lax.optimization_barrier(jnp.sum(weights, axis=-1))
        rounded = lax.optimization_barrier(weights.astype(jnp.bfloat16)).astype(jnp.float32)
        summed = jnp.einsum('kgts,skd->tkgd', rounded, value_block)
        result = summed / jnp.transpose(weight_total, (2, 0, 1))[..., None]
        return result.astype(jnp.bfloat16).reshape(STRETCH, HEADS * HD)
    attention_seq = lax.map(one_stretch, jnp.arange(STRETCHES, dtype=jnp.int32)).reshape(TOKENS, HEADS * HD)
    attention = attention_seq[positions]
    group_cols = HEADS // N_TP * HD
    mixed = jnp.zeros((TOKENS, D), jnp.float32)
    for group_index in range(N_TP):
        low = group_index * group_cols
        partial_value = jnp.dot(attention[:, low:low + group_cols], w_out[low:low + group_cols], preferred_element_type=jnp.float32)
        mixed = mixed + lax.optimization_barrier(partial_value.astype(jnp.bfloat16)).astype(jnp.float32)
    return mixed.astype(jnp.bfloat16)
```

```python
import math

import jax
import jax.numpy as jnp
import numpy as np
from jax import lax
from jax.experimental import pallas as pl
from jax.experimental.pallas import tpu as pltpu
from jax.sharding import PartitionSpec as P

D = 4096
HEADS = 32
HD = 128
GROUP = 4
STRETCH = 256
N_CP = 16
REACH = 9
CHUNK = 512
N_CHUNK = D // CHUNK
NEG = -1e30
EPS = 1e-05
THETA = 500000.0
QSCALE = math.log2(math.e) / math.sqrt(HD)
ONES = 16
F32 = jnp.float32
BF16 = jnp.bfloat16


def rope_tables():
    half = HD // 2
    freqs = THETA ** (-2.0 * np.arange(half) / HD)
    inner = np.arange(STRETCH)[:, None] * freqs[None, :]
    outer = (np.arange(2 * N_CP) * STRETCH)[:, None] * freqs[None, :]

    def both(angles):
        c, s = np.cos(angles), np.sin(angles)
        return np.stack([np.concatenate([c, c], 1), np.concatenate([s, s], 1)])

    return both(inner).astype(np.float32), both(outer).astype(np.float32)


def kernel(
    tokens, gain, wq, wk, wv, wo, docs, rope_in, rope_out, out,
    x, xg, wkv, wqv, wo_own, wo_sib, acckv, accq, ssq, kvbuf, qs,
    m_ref, acc_ref, attn_own, attn_sib, send_a, recv_a, send_b, recv_b, qstart,
    in_sems, wq_sems, wo_sems, wos_send, wos_recv, kv_send, kv_recv,
    at_send, at_recv, a_send, a_recv, b_send, b_recv,
):
    d = lax.axis_index("cp")
    t = lax.axis_index("tp")
    z, core = t // 2, t % 2
    sib = t + 1 - 2 * core
    t_up = lax.rem(z + 1, 4) * 2 + core
    t_dn = lax.rem(z + 3, 4) * 2 + core
    zs = [z, lax.rem(z + 1, 4), lax.rem(z + 3, 4), lax.rem(z + 2, 4)]
    cl, cu = d, 2 * N_CP - 1 - d

    def in_copies(i):
        rows = pl.ds(i * CHUNK, CHUNK)
        return (
            pltpu.make_async_copy(tokens.at[:, rows], x.at[:, rows], in_sems.at[0, i]),
            pltpu.make_async_copy(wk.at[rows, :], wkv.at[rows, 0:HD], in_sems.at[1, i]),
            pltpu.make_async_copy(wv.at[rows, :], wkv.at[rows, HD : 2 * HD], in_sems.at[2, i]),
        )

    def wq_copy(i):
        rows = pl.ds(i * CHUNK, CHUNK)
        return pltpu.make_async_copy(wq.at[rows, :], wqv.at[rows, :], wq_sems.at[i])

    def wo_copy(i):
        cols = pl.ds(pl.multiple_of((2 * i + core) * 512, 512), 512)
        return pltpu.make_async_copy(wo.at[:, cols], wo_own.at[i], wo_sems.at[i])

    for i in range(N_CHUNK):
        for c in in_copies(i):
            c.start()

    barrier = pltpu.get_barrier_semaphore()
    for r in range(1, N_CP):
        pl.semaphore_signal(barrier, 1, device_id={"cp": lax.rem(d + r, N_CP), "tp": t})
    for other in (sib, t_up, t_dn):
        pl.semaphore_signal(barrier, 1, device_id={"cp": d, "tp": other})

    for i in range(N_CHUNK):
        wq_copy(i).start()
    for i in range(4):
        wo_copy(i).start()

    table = docs[...]
    rows = [docs[pl.ds(cl, 1), :], docs[pl.ds(cu, 1), :]]
    starts = [jnp.zeros((1, STRETCH), F32) for _ in rows]
    for v in range(1, 16):
        below = jnp.where(table < v, 1.0, 0.0)
        count = jnp.sum(jnp.sum(below, axis=0, keepdims=True), axis=1, keepdims=True)
        starts = [jnp.where(r >= v, count, s) for r, s in zip(rows, starts)]
    qstart[0:1, :] = starts[0].astype(jnp.int32)
    qstart[1:2, :] = starts[1].astype(jnp.int32)

    acckv[...] = jnp.zeros_like(acckv)
    ssq[...] = jnp.zeros_like(ssq)

    def kv_step(i, carry):
        for c in in_copies(i):
            c.wait()
        cols = pl.ds(pl.multiple_of(i * CHUNK, CHUNK), CHUNK)
        xf = x[:, cols].astype(F32)
        sq = xf * xf
        ssq[...] += sq[:, 0:128] + sq[:, 128:256] + sq[:, 256:384] + sq[:, 384:512]
        scaled = (xf * gain[:, cols].astype(F32)).astype(BF16)
        xg[:, cols] = scaled
        acckv[...] += jnp.dot(scaled, wkv[cols, :], preferred_element_type=F32)
        return carry

    lax.fori_loop(0, N_CHUNK, kv_step, 0)
    mean = jnp.sum(ssq[...], axis=1, keepdims=True) * (1.0 / D)
    factor = lax.rsqrt(mean + EPS)
    ssq[...] = jnp.broadcast_to(factor, (2 * STRETCH, HD))

    sign = jnp.where(lax.broadcasted_iota(jnp.int32, (1, HD), 1) < HD // 2, -1.0, 1.0)

    def rope(h):
        c = cl if h == 0 else cu
        co, so = rope_out[0, pl.ds(c, 1), :], rope_out[1, pl.ds(c, 1), :]
        ci, si = rope_in[0], rope_in[1]
        return ci * co - si * so, (ci * so + si * co) * sign

    for h, c in ((0, cl), (1, cu)):
        rs = slice(h * STRETCH, (h + 1) * STRETCH)
        cosine, sine = rope(h)
        kf = acckv[rs, 0:HD] * ssq[rs, :]
        kvbuf[c, 0:STRETCH, :] = (kf * cosine + pltpu.roll(kf, HD // 2, 1) * sine).astype(BF16)
        vf = acckv[rs, HD : 2 * HD] * ssq[rs, :]
        kvbuf[c, STRETCH : STRETCH + HD, :] = vf[0:HD, :].T.astype(BF16)
        kvbuf[c, STRETCH + HD : STRETCH + 2 * HD, :] = vf[HD : 2 * HD, :].T.astype(BF16)

    pl.semaphore_wait(barrier, N_CP - 1 + 3)

    def kv_copy(c, e, s):
        return pltpu.make_async_remote_copy(
            src_ref=kvbuf.at[c], dst_ref=kvbuf.at[c], send_sem=kv_send.at[s],
            recv_sem=kv_recv.at[c], device_id={"cp": e, "tp": t},
        )

    def kv_sends(act):
        for r in range(1, REACH + 1):
            @pl.when(d + r < N_CP)
            def _():
                act(kv_copy(cl, d + r, r - 1))
        for r in range(1, REACH + 1):
            @pl.when(d - r >= 0)
            def _():
                act(kv_copy(cu, d - r, REACH + r - 1))
        for r in range(1, N_CP):
            e = lax.rem(d + r, N_CP)
            direct = (d + r < N_CP) & (r <= REACH)
            @pl.when((e >= 22 - d) & (e <= 30 - d) & jnp.logical_not(direct))
            def _():
                act(kv_copy(cl, e, 2 * REACH + r - 1))

    kv_sends(lambda c: c.start())

    def wos_copy(i):
        cols = pl.ds(pl.multiple_of((2 * i + 1 - core) * 512, 512), 512)
        return pltpu.make_async_remote_copy(
            src_ref=wo.at[:, cols], dst_ref=wo_sib.at[i], send_sem=wos_send.at[i],
            recv_sem=wos_recv.at[i], device_id={"cp": d, "tp": sib},
        )

    for i in range(4):
        wos_copy(i).start()

    accq[...] = jnp.zeros_like(accq)

    def q_step(i, carry):
        wq_copy(i).wait()
        cols = pl.ds(pl.multiple_of(i * CHUNK, CHUNK), CHUNK)
        accq[...] += jnp.dot(xg[:, cols], wqv[cols, :], preferred_element_type=F32)
        return carry

    lax.fori_loop(0, N_CHUNK, q_step, 0)
    for h in range(2):
        rs = slice(h * STRETCH, (h + 1) * STRETCH)
        cosine, sine = rope(h)
        scale = ssq[rs, :] * QSCALE
        for g in range(GROUP):
            qf = accq[rs, g * HD : (g + 1) * HD] * scale
            qs[h, g * STRETCH : (g + 1) * STRETCH, :] = (
                qf * cosine + pltpu.roll(qf, HD // 2, 1) * sine
            ).astype(BF16)

    key_row = lax.broadcasted_iota(jnp.int32, (STRETCH, STRETCH), 0)
    query_col = lax.broadcasted_iota(jnp.int32, (STRETCH, STRETCH), 1)
    ones = jnp.ones((ONES, STRETCH), BF16)

    def block(h, s, first):
        keys = kvbuf[s, 0:STRETCH, :]
        vt = jnp.concatenate(
            [kvbuf[s, STRETCH : STRETCH + HD, :], kvbuf[s, STRETCH + HD : STRETCH + 2 * HD, :]], axis=1
        )
        vt = jnp.concatenate([vt, ones], axis=0)
        mask = key_row >= qstart[h : h + 1, :] - s * STRETCH
        if first:
            mask = mask & (key_row <= query_col)
        for g in range(GROUP):
            q = qs[h, g * STRETCH : (g + 1) * STRETCH, :]
            scores = lax.dot_general(keys, q, (((1,), (1,)), ((), ())), preferred_element_type=F32)
            scores = jnp.where(mask, scores, NEG)
            top = jnp.max(scores, axis=0, keepdims=True)
            if not first:
                before = m_ref[h, g : g + 1, :]
                top = jnp.maximum(top, before)
            weights = jnp.exp2(scores - top).astype(BF16)
            added = jnp.dot(vt, weights, preferred_element_type=F32)
            if first:
                acc_ref[h, g] = added
            else:
                acc_ref[h, g] = acc_ref[h, g] * jnp.exp2(before - top) + added
            m_ref[h, g : g + 1, :] = top

    def finish(h):
        for g in range(GROUP):
            o = acc_ref[h, g, 0:HD, :] / acc_ref[h, g, HD : HD + 1, :]
            attn_own[h, :, g * HD : (g + 1) * HD] = o.T.astype(BF16)

    def kv_wait(s):
        kv_copy(s, d, 0).wait_recv()

    def lower_step(k, carry):
        @pl.when(cl >= k)
        def _():
            kv_wait(cl - k)
            block(0, cl - k, False)
        return carry

    def upper_step(k, carry):
        s = cu - k
        @pl.when((s != d) & ((s > d) | (s < d - REACH)))
        def _():
            kv_wait(s)
        block(1, s, False)
        return carry

    def at_copy(h):
        return pltpu.make_async_remote_copy(
            src_ref=attn_own.at[h], dst_ref=attn_sib.at[h], send_sem=at_send.at[h],
            recv_sem=at_recv.at[h], device_id={"cp": d, "tp": sib},
        )

    def project(h, i):
        zz = zs[i]
        return jnp.dot(attn_own[h], wo_own[zz], preferred_element_type=F32) + jnp.dot(
            attn_sib[h], wo_sib[zz], preferred_element_type=F32
        )

    def a_copy(h, way):
        return pltpu.make_async_remote_copy(
            src_ref=send_a.at[h, way], dst_ref=recv_a.at[h, way], send_sem=a_send.at[h, way],
            recv_sem=a_recv.at[h, way], device_id={"cp": d, "tp": t_up if way == 0 else t_dn},
        )

    def b_copy(h, way, piece):
        return pltpu.make_async_remote_copy(
            src_ref=send_b.at[h, way, piece], dst_ref=recv_b.at[h, way, piece],
            send_sem=b_send.at[h, way, piece], recv_sem=b_recv.at[h, way, piece],
            device_id={"cp": d, "tp": t_up if way == 0 else t_dn},
        )

    summed = [slice(0, 256), slice(256, 512)]
    plain = [slice(256, 512), slice(0, 256)]
    held = [None, None]

    def scatter_first(h):
        at_copy(h).wait_recv()
        far = project(h, 3)
        for way in range(2):
            send_a[h, way] = far[:, summed[way]].astype(BF16)
            a_copy(h, way).start()
        for way in range(2):
            near = project(h, 1 + way)
            acckv_like = near[:, summed[way]]
            accq[h * STRETCH : (h + 1) * STRETCH, way * 256 : (way + 1) * 256] = acckv_like
            send_b[h, way, 1] = near[:, plain[way]].astype(BF16)
            b_copy(h, way, 1).start()

    def scatter_second(h):
        for way in range(2):
            a_copy(h, way).wait_recv()
            own = accq[h * STRETCH : (h + 1) * STRETCH, way * 256 : (way + 1) * 256]
            send_b[h, way, 0] = (own + recv_a[h, way].astype(F32)).astype(BF16)
            b_copy(h, way, 0).start()

    def scatter_last(h):
        mine = project(h, 0)
        for way in range(2):
            for piece in range(2):
                b_copy(h, way, piece).wait_recv()
        rs = slice(h * STRETCH, (h + 1) * STRETCH)
        out[rs, 0:256] = (
            mine[:, 0:256] + recv_b[h, 0, 0].astype(F32) + recv_b[h, 1, 1].astype(F32)
        ).astype(BF16)
        out[rs, 256:512] = (
            mine[:, 256:512] + recv_b[h, 0, 1].astype(F32) + recv_b[h, 1, 0].astype(F32)
        ).astype(BF16)

    block(0, cl, True)
    block(1, cu, True)
    lax.fori_loop(1, REACH + 1, lower_step, 0)
    finish(0)
    at_copy(0).start()
    for i in range(4):
        wo_copy(i).wait()
        wos_copy(i).wait_recv()
    lax.fori_loop(1, 3, upper_step, 0)
    scatter_first(0)
    lax.fori_loop(3, 7, upper_step, 0)
    scatter_second(0)
    lax.fori_loop(7, REACH + 1, upper_step, 0)
    finish(1)
    at_copy(1).start()
    scatter_last(0)
    scatter_first(1)
    scatter_second(1)
    scatter_last(1)

    kv_sends(lambda c: c.wait_send())
    for i in range(4):
        wos_copy(i).wait_send()
    for h in range(2):
        at_copy(h).wait_send()
        for way in range(2):
            a_copy(h, way).wait_send()
            for piece in range(2):
                b_copy(h, way, piece).wait_send()


def step(tokens, gain, w_query, w_key, w_value, w_out, doc_ids):
    rope_in, rope_out = rope_tables()
    any_space = pl.BlockSpec(memory_space=pl.ANY)
    vmem = pl.BlockSpec(memory_space=pltpu.VMEM)
    rows = 2 * STRETCH
    dma = pltpu.SemaphoreType.DMA
    return pl.pallas_call(
        kernel,
        out_shape=jax.ShapeDtypeStruct((rows, 512), BF16),
        in_specs=[any_space, vmem, any_space, any_space, any_space, any_space, vmem, vmem, vmem],
        out_specs=vmem,
        scratch_shapes=[
            pltpu.VMEM((rows, D), BF16),
            pltpu.VMEM((rows, D), BF16),
            pltpu.VMEM((D, 2 * HD), BF16),
            pltpu.VMEM((D, GROUP * HD), BF16),
            pltpu.VMEM((4, 512, 512), BF16),
            pltpu.VMEM((4, 512, 512), BF16),
            pltpu.VMEM((rows, 2 * HD), F32),
            pltpu.VMEM((rows, GROUP * HD), F32),
            pltpu.VMEM((rows, HD), F32),
            pltpu.VMEM((2 * N_CP, 2 * STRETCH, HD), BF16),
            pltpu.VMEM((2, GROUP * STRETCH, HD), BF16),
            pltpu.VMEM((2, 8, STRETCH), F32),
            pltpu.VMEM((2, GROUP, HD + ONES, STRETCH), F32),
            pltpu.VMEM((2, STRETCH, 512), BF16),
            pltpu.VMEM((2, STRETCH, 512), BF16),
            pltpu.VMEM((2, 2, STRETCH, 256), BF16),
            pltpu.VMEM((2, 2, STRETCH, 256), BF16),
            pltpu.VMEM((2, 2, 2, STRETCH, 256), BF16),
            pltpu.VMEM((2, 2, 2, STRETCH, 256), BF16),
            pltpu.VMEM((8, STRETCH), jnp.int32),
            dma((3, N_CHUNK)),
            dma((N_CHUNK,)),
            dma((4,)),
            dma((4,)),
            dma((4,)),
            dma((2 * REACH + N_CP - 1,)),
            dma((2 * N_CP,)),
            dma((2,)),
            dma((2,)),
            dma((2, 2)),
            dma((2, 2)),
            dma((2, 2, 2)),
            dma((2, 2, 2)),
        ],
        compiler_params=pltpu.CompilerParams(
            collective_id=0, has_side_effects=True, vmem_limit_bytes=60 * 1024 * 1024
        ),
        name="block",
    )(
        tokens, gain.reshape(1, D), w_query, w_key, w_value, w_out,
        doc_ids.reshape(2 * N_CP, STRETCH), jnp.asarray(rope_in), jnp.asarray(rope_out),
    )


def solution(mesh):
    in_specs = (P("cp", None), P(), P(None, "tp"), P(None, "tp"), P(None, "tp"), P("tp", None), P())
    return jax.shard_map(step, mesh=mesh, in_specs=in_specs, out_specs=P("cp", "tp"), check_vma=False)
```

```python
import math

import jax
import jax.numpy as jnp
import numpy as np
from jax import lax
from jax.experimental import pallas as pl
from jax.experimental.pallas import tpu as pltpu
from jax.sharding import PartitionSpec as P

D = 4096
HEADS = 32
HD = 128
GROUP = 4
STRETCH = 256
N_CP = 16
REACH = 9
CHUNK = 512
N_CHUNK = D // CHUNK
NEG = -1e30
EPS = 1e-05
THETA = 500000.0
QSCALE = math.log2(math.e) / math.sqrt(HD)
ONES = 16
F32 = jnp.float32
BF16 = jnp.bfloat16

TABLE = [
    [64, 385, 384, 65, 1271, 1081, 1084, 3318, 3128, 3133, 121, 1199, 1072, 1076, 111, 3246, 3121, 1082, 113, 3125, 3131, 180, 1459, 1069, 3122, 3244],
    [322, 188, 323, 189, 1344, 1204, 1082, 3073, 3189, 3131, 186, 116, 187, 1069, 1075, 1079, 109, 179, 3116, 3122, 3126, 108, 178, 1080, 3129, 1066, 3115, 1135, 3118, 1072, 3121],
    [68, 261, 186, 260, 69, 187, 1346, 1203, 1081, 3139, 3250, 3128, 114, 184, 1280, 3073, 1067, 235, 3114, 1072, 1077, 106, 176, 3121, 3124, 1064, 117, 3113, 1325, 1078, 109, 3116, 3127, 1071, 3118],
    [262, 249, 263, 248, 1153, 1284, 1136, 3328, 3077, 3185, 176, 1282, 1192, 1079, 3331, 3113, 3254, 1074, 183, 1071, 1323, 3246, 3114, 1076, 3125, 1062, 3123, 1069, 3116, 3111],
    [72, 393, 567, 392, 73, 566, 1473, 1583, 1072, 1076, 3328, 3822, 3121, 3125, 239, 565, 1026, 1286, 1062, 230, 3075, 3335, 1581, 173, 113, 3111, 1064, 3628, 258, 103, 172, 1284, 3077, 3113, 104, 1061, 1322, 3108, 3115, 1075, 3122],
    [331, 692, 330, 693, 1410, 1096, 1581, 1074, 3523, 3081, 3628, 3123, 73, 172, 1024, 3073, 1285, 1578, 133, 108, 3332, 1060, 1582, 100, 170, 3109, 3115, 3119, 257, 101, 171, 1030, 1059, 1062, 178, 3079, 3106, 1073, 3111, 1065, 3120, 3112],
    [268, 77, 178, 563, 76, 269, 562, 179, 1477, 1035, 1579, 1073, 3204, 3338, 3626, 3120, 75, 260, 74, 171, 561, 1026, 1030, 1032, 1065, 390, 553, 106, 3075, 3079, 1058, 391, 98, 3081, 3107, 3112, 1024, 99, 176, 3073, 1068, 1056, 1380, 1070, 3109, 3119, 3117, 3105, 1062, 3111],
    [270, 624, 177, 271, 176, 625, 1222, 1033, 1293, 1576, 3271, 3080, 3084, 3625, 262, 263, 232, 1025, 1028, 3077, 1056, 129, 324, 3072, 1035, 1054, 1070, 174, 3082, 3103, 3119, 1026, 175, 1830, 1066, 3075, 166, 3105, 1058, 1069, 3107, 3623, 3116, 3115, 1060, 3109],
    [144, 337, 559, 336, 145, 558, 1481, 1574, 1065, 1068, 3528, 3111, 3112, 3629, 102, 679, 1025, 1291, 1038, 1057, 139, 78, 553, 3072, 3082, 3343, 1061, 64, 677, 1054, 3103, 3108, 1286, 70, 676, 1036, 3085, 3104, 3335, 71, 1027, 1052, 3074, 284, 103, 1029, 3101, 1059, 3076, 3106, 1066, 3115],
    [274, 83, 172, 557, 82, 275, 556, 173, 1483, 1041, 1061, 1578, 3466, 3152, 3620, 3115, 1051, 81, 164, 549, 1026, 1033, 1292, 1571, 66, 140, 3075, 3080, 3341, 3618, 195, 1062, 1065, 264, 1029, 1053, 133, 102, 553, 1038, 3100, 3076, 3098, 162, 101, 1024, 3087, 3073, 1055, 171, 1030, 3112, 3079, 1056, 3105, 3102, 3111],
    [276, 85, 170, 555, 84, 277, 554, 171, 1484, 1043, 1058, 1577, 3469, 3090, 3107, 3112, 83, 546, 1052, 82, 547, 169, 1029, 1035, 1294, 3101, 69, 156, 3082, 3343, 1040, 1568, 74, 143, 3076, 3089, 1055, 267, 1050, 98, 168, 1026, 1030, 1033, 3617, 90, 160, 3075, 3079, 3080, 3230, 99, 1062, 3623, 1049, 1061, 3108, 3096, 3099],
    [278, 552, 233, 279, 232, 553, 1486, 1040, 1045, 1568, 3535, 3089, 3092, 1566, 2070, 3743, 276, 94, 1033, 1036, 3085, 1052, 137, 333, 1030, 3080, 1043, 3617, 136, 275, 92, 3079, 3090, 1063, 3165, 679, 1028, 3077, 1035, 1049, 3082, 1573, 1179, 1058, 3108, 3110, 3096, 3098, 3107],
    [88, 153, 550, 152, 89, 551, 1233, 1569, 1060, 3280, 1055, 3621, 2072, 1050, 3104, 607, 1033, 1170, 1046, 73, 544, 3080, 3091, 3095, 86, 1035, 1102, 1571, 3087, 3082, 3102, 79, 1044, 3093, 1030, 1036, 3085, 3079, 3099, 1053, 3100, 3106],
    [90, 164, 549, 91, 548, 165, 154, 539, 1106, 1048, 1059, 146, 547, 3155, 3097, 3106, 2074, 147, 546, 1053, 88, 1035, 1041, 541, 163, 1044, 81, 3082, 3088, 138, 538, 3093, 74, 1055, 148, 543, 1036, 3100, 1033, 140, 3085, 1569, 1046, 157, 3080, 3104, 1038, 162, 3095, 3087, 3102],
    [92, 546, 163, 93, 162, 547, 540, 157, 1044, 1114, 1056, 148, 541, 3093, 3163, 1054, 2076, 149, 544, 3105, 85, 1036, 1042, 538, 156, 1049, 76, 3085, 3091, 673, 1046, 3096, 542, 160, 1038, 3095, 1041, 151, 537, 3087, 3088, 1034, 536, 158, 3083, 3103],
    [672, 97, 670, 95, 543, 96, 161, 1046, 1049, 1052, 86, 153, 540, 3095, 3096, 3101, 2078, 150, 87, 545, 1038, 1041, 1050, 78, 151, 541, 3087, 3088, 3099, 144, 537, 94, 1044, 3093, 85, 539, 159, 1036, 3085, 1042, 77, 536, 3091, 91],
]
MARKS = [
    [4, 4, 6, 4, 6, 4, 8, 6, 6, 8, 8, 6, 6, 8, 8, 7],
    [4, 7, 15, 14, 32, 35, 39, 35, 48, 52, 49, 40, 37, 49, 44, 42],
    [10, 13, 21, 19, 37, 41, 44, 40, 51, 56, 54, 45, 41, 50, 45, 43],
    [23, 29, 33, 27, 40, 41, 49, 45, 51, 56, 58, 48, 41, 50, 45, 43],
    [26, 31, 35, 30, 41, 42, 50, 46, 52, 57, 59, 49, 42, 51, 46, 44],
]
ENTRIES = max(len(row) for row in TABLE)


def rope_tables():
    half = HD // 2
    freqs = THETA ** (-2.0 * np.arange(half) / HD)
    inner = np.arange(STRETCH)[:, None] * freqs[None, :]
    outer = (np.arange(2 * N_CP) * STRETCH)[:, None] * freqs[None, :]

    def both(angles):
        c, s = np.cos(angles), np.sin(angles)
        return np.stack([np.concatenate([c, c], 1), np.concatenate([s, s], 1)])

    return both(inner).astype(np.float32), both(outer).astype(np.float32)


def kernel(
    tokens, gain, wq, wk, wv, wo, docs, rope_in, rope_out, out,
    x, xg, wkv, wqv, wo_own, wo_sib, acckv, accq, ssq, kvbuf, qs,
    m_ref, acc_ref, attn_own, attn_sib, send_a, recv_a, send_b, recv_b, qstart,
    in_sems, wq_sems, wo_sems, wos_send, wos_recv, kv_send, kv_recv,
    at_send, at_recv, a_send, a_recv, b_send, b_recv,
):
    d = lax.axis_index("cp")
    t = lax.axis_index("tp")
    z, core = t // 2, t % 2
    sib = t + 1 - 2 * core
    t_up = lax.rem(z + 1, 4) * 2 + core
    t_dn = lax.rem(z + 3, 4) * 2 + core
    zs = [z, lax.rem(z + 1, 4), lax.rem(z + 3, 4), lax.rem(z + 2, 4)]
    cl, cu = d, 2 * N_CP - 1 - d
    px, py = lax.rem(d, 4), lax.div(d, 4)
    beside = [
        py * 4 + lax.rem(px + 1, 4),
        py * 4 + lax.rem(px + 3, 4),
        lax.rem(py + 1, 4) * 4 + px,
        lax.rem(py + 3, 4) * 4 + px,
    ]

    def in_copies(i):
        rows = pl.ds(i * CHUNK, CHUNK)
        return (
            pltpu.make_async_copy(tokens.at[:, rows], x.at[:, rows], in_sems.at[0, i]),
            pltpu.make_async_copy(wk.at[rows, :], wkv.at[rows, 0:HD], in_sems.at[1, i]),
            pltpu.make_async_copy(wv.at[rows, :], wkv.at[rows, HD : 2 * HD], in_sems.at[2, i]),
        )

    def wq_copy(i):
        rows = pl.ds(i * CHUNK, CHUNK)
        return pltpu.make_async_copy(wq.at[rows, :], wqv.at[rows, :], wq_sems.at[i])

    def wo_copy(i):
        cols = pl.ds(pl.multiple_of((2 * i + core) * 512, 512), 512)
        return pltpu.make_async_copy(wo.at[:, cols], wo_own.at[i], wo_sems.at[i])

    for i in range(N_CHUNK):
        for c in in_copies(i):
            c.start()

    barrier = pltpu.get_barrier_semaphore()
    for e in beside:
        pl.semaphore_signal(barrier, 1, device_id={"cp": e, "tp": t})
    for other in (sib, t_up, t_dn):
        pl.semaphore_signal(barrier, 1, device_id={"cp": d, "tp": other})

    here = [(d == e).astype(jnp.int32) for e in range(N_CP)]

    def pick(values):
        total = jnp.int32(0)
        for e, v in enumerate(values):
            if v:
                total = total + here[e] * v
        return total

    def entry_of(row, i):
        return row[i] if i < len(row) else 0

    words = [
        pick([entry_of(row, i) + 4096 * entry_of(row, i + 1) for row in TABLE])
        for i in range(0, ENTRIES, 2)
    ]

    def entry(i):
        j = lax.div(i, 2)
        word = jnp.int32(0)
        for k, w in enumerate(words):
            word = jnp.where(j == k, w, word)
        return jnp.where(lax.rem(i, 2) == 0, lax.rem(word, 4096), lax.div(word, 4096))

    at_query, at_whole, at_first, at_second, n_entries = [pick(m) for m in MARKS]

    table = docs[...]
    rows = [docs[pl.ds(cl, 1), :], docs[pl.ds(cu, 1), :]]
    starts = [jnp.zeros((1, STRETCH), F32) for _ in rows]
    for v in range(1, 16):
        below = jnp.where(table < v, 1.0, 0.0)
        count = jnp.sum(jnp.sum(below, axis=0, keepdims=True), axis=1, keepdims=True)
        starts = [jnp.where(r >= v, count, s) for r, s in zip(rows, starts)]
    qstart[0:1, :] = starts[0].astype(jnp.int32)
    qstart[1:2, :] = starts[1].astype(jnp.int32)
    m_ref[...] = jnp.full_like(m_ref, NEG)
    acc_ref[...] = jnp.zeros_like(acc_ref)

    acckv[...] = jnp.zeros_like(acckv)
    ssq[...] = jnp.zeros_like(ssq)

    def kv_step(i, carry):
        for c in in_copies(i):
            c.wait()
        wq_copy(i).start()
        cols = pl.ds(pl.multiple_of(i * CHUNK, CHUNK), CHUNK)
        xf = x[:, cols].astype(F32)
        sq = xf * xf
        ssq[...] += sq[:, 0:128] + sq[:, 128:256] + sq[:, 256:384] + sq[:, 384:512]
        scaled = (xf * gain[:, cols].astype(F32)).astype(BF16)
        xg[:, cols] = scaled
        acckv[...] += jnp.dot(scaled, wkv[cols, :], preferred_element_type=F32)
        return carry

    lax.fori_loop(0, N_CHUNK, kv_step, 0)
    for i in range(4):
        wo_copy(i).start()
    mean = jnp.sum(ssq[...], axis=1, keepdims=True) * (1.0 / D)
    factor = lax.rsqrt(mean + EPS)
    ssq[...] = jnp.broadcast_to(factor, (2 * STRETCH, HD))

    sign = jnp.where(lax.broadcasted_iota(jnp.int32, (1, HD), 1) < HD // 2, -1.0, 1.0)

    def rope(h):
        c = cl if h == 0 else cu
        co, so = rope_out[0, pl.ds(c, 1), :], rope_out[1, pl.ds(c, 1), :]
        ci, si = rope_in[0], rope_in[1]
        return ci * co - si * so, (ci * so + si * co) * sign

    for h, c in ((0, cl), (1, cu)):
        rs = slice(h * STRETCH, (h + 1) * STRETCH)
        cosine, sine = rope(h)
        kf = acckv[rs, 0:HD] * ssq[rs, :]
        kvbuf[2 * c] = (kf * cosine + pltpu.roll(kf, HD // 2, 1) * sine).astype(BF16)
        vf = acckv[rs, HD : 2 * HD] * ssq[rs, :]
        kvbuf[2 * c + 1, 0:HD, :] = vf[0:HD, :].T.astype(BF16)
        kvbuf[2 * c + 1, HD : 2 * HD, :] = vf[HD : 2 * HD, :].T.astype(BF16)

    pl.semaphore_wait(barrier, 7)

    def kv_copy(p, way):
        return pltpu.make_async_remote_copy(
            src_ref=kvbuf.at[p], dst_ref=kvbuf.at[p], send_sem=kv_send.at[way, p],
            recv_sem=kv_recv.at[p], device_id={"cp": beside[way], "tp": t},
        )

    def pass_on(e, act):
        p, ways = lax.rem(e, 64), lax.rem(lax.div(e, 64), 16)
        for way in range(4):
            @pl.when(lax.rem(lax.div(ways, 2**way), 2) == 1)
            def _():
                act(kv_copy(p, way))

    def send_only(i, carry):
        pass_on(entry(i), lambda c: c.start())
        return carry

    lax.fori_loop(0, at_query, send_only, 0)

    def wos_copy(i):
        cols = pl.ds(pl.multiple_of((2 * i + 1 - core) * 512, 512), 512)
        return pltpu.make_async_remote_copy(
            src_ref=wo.at[:, cols], dst_ref=wo_sib.at[i], send_sem=wos_send.at[i],
            recv_sem=wos_recv.at[i], device_id={"cp": d, "tp": sib},
        )

    for i in range(4):
        wos_copy(i).start()

    for i in range(N_CHUNK):
        wq_copy(i).wait()

    def q_step(i, carry):
        cols = pl.ds(pl.multiple_of(i * 256, 256), 256)
        accq[:, cols] = jnp.dot(xg[...], wqv[:, cols], preferred_element_type=F32)
        return carry

    lax.fori_loop(0, 2, q_step, 0)
    for h in range(2):
        rs = slice(h * STRETCH, (h + 1) * STRETCH)
        cosine, sine = rope(h)
        scale = ssq[rs, :] * QSCALE
        for g in range(GROUP):
            qf = accq[rs, g * HD : (g + 1) * HD] * scale
            qs[h, g * STRETCH : (g + 1) * STRETCH, :] = (
                qf * cosine + pltpu.roll(qf, HD // 2, 1) * sine
            ).astype(BF16)

    key_row = lax.broadcasted_iota(jnp.int32, (STRETCH, STRETCH), 0)
    query_col = lax.broadcasted_iota(jnp.int32, (STRETCH, STRETCH), 1)
    ones = jnp.ones((ONES, STRETCH), BF16)

    def block(h, s, own):
        keys = kvbuf[2 * s]
        vt = jnp.concatenate([kvbuf[2 * s + 1, 0:HD, :], kvbuf[2 * s + 1, HD : 2 * HD, :]], axis=1)
        vt = jnp.concatenate([vt, ones], axis=0)
        mask = key_row >= qstart[h : h + 1, :] - s * STRETCH
        if own:
            mask = mask & (key_row <= query_col)
        scores = [
            lax.dot_general(
                keys, qs[h, g * STRETCH : (g + 1) * STRETCH, :], (((1,), (1,)), ((), ())),
                preferred_element_type=F32,
            )
            for g in range(GROUP)
        ]
        before = [m_ref[h, g : g + 1, :] for g in range(GROUP)]
        held = [acc_ref[h, g] for g in range(GROUP)]
        tops, added = [], []
        for g in range(GROUP):
            sc = jnp.where(mask, scores[g], NEG)
            top = jnp.maximum(jnp.max(sc, axis=0, keepdims=True), before[g])
            weights = jnp.exp2(sc - top).astype(BF16)
            tops.append(top)
            added.append(jnp.dot(vt, weights, preferred_element_type=F32))
        for g in range(GROUP):
            acc_ref[h, g] = held[g] * jnp.exp2(before[g] - tops[g]) + added[g]
            m_ref[h, g : g + 1, :] = tops[g]

    def finish(h):
        for g in range(GROUP):
            o = acc_ref[h, g, 0:HD, :] / acc_ref[h, g, HD : HD + 1, :]
            attn_own[h, :, g * HD : (g + 1) * HD] = o.T.astype(BF16)

    def at_copy(h):
        return pltpu.make_async_remote_copy(
            src_ref=attn_own.at[h], dst_ref=attn_sib.at[h], send_sem=at_send.at[h],
            recv_sem=at_recv.at[h], device_id={"cp": d, "tp": sib},
        )

    def project(h, i):
        zz = zs[i]
        return jnp.dot(attn_own[h], wo_own[zz], preferred_element_type=F32) + jnp.dot(
            attn_sib[h], wo_sib[zz], preferred_element_type=F32
        )

    def a_copy(h, way):
        return pltpu.make_async_remote_copy(
            src_ref=send_a.at[h, way], dst_ref=recv_a.at[h, way], send_sem=a_send.at[h, way],
            recv_sem=a_recv.at[h, way], device_id={"cp": d, "tp": t_up if way == 0 else t_dn},
        )

    def b_copy(h, way, piece):
        return pltpu.make_async_remote_copy(
            src_ref=send_b.at[h, way, piece], dst_ref=recv_b.at[h, way, piece],
            send_sem=b_send.at[h, way, piece], recv_sem=b_recv.at[h, way, piece],
            device_id={"cp": d, "tp": t_up if way == 0 else t_dn},
        )

    summed = [slice(0, 256), slice(256, 512)]
    plain = [slice(256, 512), slice(0, 256)]

    def scatter_first(h):
        at_copy(h).wait_recv()
        far = project(h, 3)
        for way in range(2):
            send_a[h, way] = far[:, summed[way]].astype(BF16)
            a_copy(h, way).start()
        for way in range(2):
            near = project(h, 1 + way)
            accq[h * STRETCH : (h + 1) * STRETCH, way * 256 : (way + 1) * 256] = near[:, summed[way]]
            send_b[h, way, 1] = near[:, plain[way]].astype(BF16)
            b_copy(h, way, 1).start()

    def scatter_second(h):
        for way in range(2):
            a_copy(h, way).wait_recv()
            own = accq[h * STRETCH : (h + 1) * STRETCH, way * 256 : (way + 1) * 256]
            send_b[h, way, 0] = (own + recv_a[h, way].astype(F32)).astype(BF16)
            b_copy(h, way, 0).start()

    def scatter_mine(h):
        accq[h * STRETCH : (h + 1) * STRETCH, :] = project(h, 0)

    def scatter_last(h):
        rs = slice(h * STRETCH, (h + 1) * STRETCH)
        for piece in (1, 0):
            for way in range(2):
                b_copy(h, way, piece).wait_recv()
        out[rs, 0:256] = (
            accq[rs, 0:256] + recv_b[h, 0, 0].astype(F32) + recv_b[h, 1, 1].astype(F32)
        ).astype(BF16)
        out[rs, 256:512] = (
            accq[rs, 256:512] + recv_b[h, 0, 1].astype(F32) + recv_b[h, 1, 0].astype(F32)
        ).astype(BF16)

    block(0, cl, True)

    def main_step(i, carry):
        e = entry(i)
        p = lax.rem(e, 64)

        @pl.when(lax.rem(lax.div(e, 1024), 2) == 1)
        def _():
            kv_copy(p, 0).wait_recv()

        pass_on(e, lambda c: c.start())
        s = lax.div(p, 2)
        whole = lax.div(e, 2048) == 1

        @pl.when(whole & (s < d) & (s >= d - REACH))
        def _():
            block(0, s, False)

        @pl.when(i == at_whole)
        def _():
            finish(0)
            at_copy(0).start()
            block(1, cu, True)

        @pl.when(whole & (s >= 22 - d) & (s <= 30 - d))
        def _():
            block(1, s, False)

        @pl.when(i == at_first)
        def _():
            for k in range(4):
                wo_copy(k).wait()
                wos_copy(k).wait_recv()
            scatter_first(0)

        @pl.when(i == at_second)
        def _():
            scatter_second(0)
            scatter_mine(0)

        return carry

    lax.fori_loop(at_query, n_entries, main_step, 0)
    finish(1)
    at_copy(1).start()

    def drain(i, carry):
        pass_on(entry(i), lambda c: c.wait_send())
        return carry

    lax.fori_loop(0, n_entries, drain, 0)
    scatter_first(1)
    scatter_last(0)
    scatter_second(1)
    scatter_mine(1)
    for i in range(4):
        wos_copy(i).wait_send()
    for h in range(2):
        at_copy(h).wait_send()
    scatter_last(1)
    for h in range(2):
        for way in range(2):
            a_copy(h, way).wait_send()
            for piece in range(2):
                b_copy(h, way, piece).wait_send()


def step(tokens, gain, w_query, w_key, w_value, w_out, doc_ids):
    rope_in, rope_out = rope_tables()
    any_space = pl.BlockSpec(memory_space=pl.ANY)
    vmem = pl.BlockSpec(memory_space=pltpu.VMEM)
    rows = 2 * STRETCH
    dma = pltpu.SemaphoreType.DMA
    return pl.pallas_call(
        kernel,
        out_shape=jax.ShapeDtypeStruct((rows, 512), BF16),
        in_specs=[any_space, vmem, any_space, any_space, any_space, any_space, vmem, vmem, vmem],
        out_specs=vmem,
        scratch_shapes=[
            pltpu.VMEM((rows, D), BF16),
            pltpu.VMEM((rows, D), BF16),
            pltpu.VMEM((D, 2 * HD), BF16),
            pltpu.VMEM((D, GROUP * HD), BF16),
            pltpu.VMEM((4, 512, 512), BF16),
            pltpu.VMEM((4, 512, 512), BF16),
            pltpu.VMEM((rows, 2 * HD), F32),
            pltpu.VMEM((rows, GROUP * HD), F32),
            pltpu.VMEM((rows, HD), F32),
            pltpu.VMEM((4 * N_CP, STRETCH, HD), BF16),
            pltpu.VMEM((2, GROUP * STRETCH, HD), BF16),
            pltpu.VMEM((2, 8, STRETCH), F32),
            pltpu.VMEM((2, GROUP, HD + ONES, STRETCH), F32),
            pltpu.VMEM((2, STRETCH, 512), BF16),
            pltpu.VMEM((2, STRETCH, 512), BF16),
            pltpu.VMEM((2, 2, STRETCH, 256), BF16),
            pltpu.VMEM((2, 2, STRETCH, 256), BF16),
            pltpu.VMEM((2, 2, 2, STRETCH, 256), BF16),
            pltpu.VMEM((2, 2, 2, STRETCH, 256), BF16),
            pltpu.VMEM((8, STRETCH), jnp.int32),
            dma((3, N_CHUNK)),
            dma((N_CHUNK,)),
            dma((4,)),
            dma((4,)),
            dma((4,)),
            dma((4, 4 * N_CP)),
            dma((4 * N_CP,)),
            dma((2,)),
            dma((2,)),
            dma((2, 2)),
            dma((2, 2)),
            dma((2, 2, 2)),
            dma((2, 2, 2)),
        ],
        compiler_params=pltpu.CompilerParams(
            collective_id=0, has_side_effects=True, vmem_limit_bytes=60 * 1024 * 1024
        ),
        name="block",
    )(
        tokens, gain.reshape(1, D), w_query, w_key, w_value, w_out,
        doc_ids.reshape(2 * N_CP, STRETCH), jnp.asarray(rope_in), jnp.asarray(rope_out),
    )


def solution(mesh):
    in_specs = (P("cp", None), P(), P(None, "tp"), P(None, "tp"), P(None, "tp"), P("tp", None), P())
    return jax.shard_map(step, mesh=mesh, in_specs=in_specs, out_specs=P("cp", "tp"), check_vma=False)
```

```python
import math

import jax
import jax.numpy as jnp
import numpy as np
from jax import lax
from jax.experimental import pallas as pl
from jax.experimental.pallas import tpu as pltpu
from jax.sharding import PartitionSpec as P

D = 4096
HEADS = 32
HD = 128
GROUP = 4
STRETCH = 256
N_CP = 16
REACH = 9
CHUNK = 512
N_CHUNK = D // CHUNK
NEG = -1e30
EPS = 1e-05
THETA = 500000.0
QSCALE = math.log2(math.e) / math.sqrt(HD)
ONES = 16
F32 = jnp.float32
BF16 = jnp.bfloat16

TABLE = [
    [192, 257, 256, 193, 1271, 1080, 1270, 1081, 452668, 121, 1263, 1072, 468021, 1198, 1137, 500788, 388096, 401588, 437248, 1196, 1074, 181, 1069, 369971, 419898, 486400],
    [258, 67, 189, 66, 259, 188, 1280, 1269, 1082, 1025, 1268, 5179, 187, 1260, 1075, 435255, 486400, 1133, 1202, 1078, 118, 2104, 368826, 418927, 452650, 470016, 1070, 354352, 388096, 404480],
    [68, 261, 186, 260, 69, 187, 1347, 1203, 1081, 1090, 1202, 21560, 420864, 115, 467128, 1280, 1258, 1025, 1131, 6196, 1200, 1073, 1324, 352370, 437248, 1133, 403496, 370742, 338944, 452654, 388096],
    [262, 120, 185, 263, 184, 121, 1152, 1284, 1136, 256, 1153, 1029, 5233, 39936, 401585, 1283, 1192, 1079, 1026, 1193, 21558, 1139, 1071, 336055, 451882, 1198, 386091, 353330, 420864, 370732, 2086, 321588, 437248],
    [200, 265, 567, 264, 201, 566, 1473, 1583, 1073, 1280, 1646, 175, 1072, 6196, 388096, 174, 111, 1026, 1350, 402599, 437248, 1027, 1287, 21670, 103, 259, 1196, 54829, 319590, 1060, 369701, 173, 112, 2052, 2088, 38187, 165, 304170, 338944, 355328, 419890],
    [266, 75, 180, 565, 74, 267, 564, 181, 1474, 1032, 1580, 1075, 1411, 1097, 1581, 21554, 72704, 72, 173, 1024, 1025, 1285, 5284, 368749, 1284, 1707, 1070, 36964, 256, 1125, 1194, 558, 418863, 305186, 352434, 55302, 387110, 289792, 321584, 403496, 338944],
    [76, 269, 691, 268, 77, 690, 1221, 1291, 1578, 1072, 1412, 1098, 1579, 37937, 89088, 261, 75, 170, 560, 1090, 1027, 1286, 21667, 355328, 1159, 1033, 1058, 53347, 1288, 1192, 70697, 401506, 6144, 107, 177, 1316, 2080, 169, 2092, 1061, 288814, 338944, 272422, 371712, 306176, 388096, 322560],
    [271, 688, 113, 270, 112, 689, 1222, 1292, 1576, 1479, 2056, 1037, 54825, 72704, 262, 104, 169, 1153, 1284, 103493, 39936, 1024, 2080, 5295, 68, 261, 2058, 87214, 338944, 2050, 2078, 22439, 272038, 388096, 256034, 2090, 321580, 288804, 355328, 371712, 306176],
    [208, 273, 559, 272, 209, 558, 1481, 1575, 1065, 1068, 1480, 1574, 1064, 70701, 322560, 166, 103, 556, 1089, 1162, 1295, 337445, 371712, 1024, 1035, 1294, 1188, 102, 4649, 87070, 1350, 118949, 2080, 54599, 104460, 2050, 20574, 2076, 304159, 273408, 38916, 2090, 239650, 257024, 355328, 289792],
    [338, 684, 339, 685, 1482, 1040, 1572, 1067, 1419, 80, 1041, 1061, 1066, 86571, 81, 549, 135338, 1218, 304397, 1570, 1091, 2056, 21772, 141, 70691, 1308, 1127, 1157, 103453, 355328, 1156, 2074, 36965, 2062, 1062, 2048, 118947, 6176, 289792, 55302, 2078, 239656, 224256, 322560, 273408, 257024, 338944],
    [276, 85, 554, 171, 84, 277, 170, 555, 1485, 1042, 1571, 1065, 1420, 1107, 1570, 103464, 154624, 1180, 82, 552, 1034, 1099, 87439, 288288, 120206, 335970, 2052, 267, 2064, 1569, 2078, 160, 36963, 138240, 1115, 270505, 2050, 2054, 2056, 168, 21530, 55334, 70685, 2084, 256024, 224256, 322560, 240640, 306176, 207872],
    [278, 552, 233, 279, 232, 553, 1487, 1045, 189985, 1486, 2064, 1044, 120352, 138240, 1566, 276, 96, 161, 1161, 1356, 168973, 1567, 1159, 1032, 103699, 70749, 1030, 1042, 54438, 1116, 153610, 87193, 2052, 1122, 38436, 1048, 1059, 1061, 271399, 256026, 240640, 207872, 289792, 306176, 322560, 224256],
    [88, 153, 551, 152, 89, 550, 1233, 1056, 206373, 1232, 1057, 136740, 273408, 1566, 97, 304201, 1170, 545, 70728, 1043, 153622, 187392, 1103, 189983, 257024, 1102, 120842, 89088, 170004, 175104, 104460, 55302, 239644, 2074, 223266, 289792],
    [91, 548, 165, 90, 164, 549, 538, 155, 1170, 1112, 222754, 1235, 1049, 153123, 203776, 1565, 82, 1162, 156753, 205844, 1163, 1040, 86555, 74, 1173, 136737, 1037, 169503, 286861, 103436, 2056, 163, 1052, 71702, 184482, 173086, 120846, 238624, 191488, 257024, 273408],
    [92, 162, 547, 93, 546, 163, 540, 157, 1172, 1115, 239136, 1173, 1114, 169502, 220160, 1695, 85, 1101, 173080, 222358, 1036, 102939, 185495, 2066, 152090, 201753, 541, 158, 2062, 120848, 536, 135328, 2058, 87073, 257024, 191488, 158720, 207872, 142336, 273408],
    [224, 545, 158, 544, 97, 606, 159, 1238, 1049, 1052, 254495, 1239, 1048, 185885, 203776, 236544, 1041, 1051, 153, 540, 188511, 2062, 1168, 1050, 537, 118876, 1108, 1045, 536, 135329, 220160, 1100, 1037, 168474, 105472, 2066, 151645, 204890, 240640, 125952, 142336, 224256, 175104, 158720],
]
MARKS = [
    [4, 6, 6, 6, 6, 8, 6, 6, 6, 4, 8, 6, 6, 8, 8, 7],
    [4, 11, 19, 20, 35, 35, 32, 31, 40, 39, 42, 34, 31, 36, 33, 36],
    [8, 16, 24, 24, 39, 38, 40, 34, 44, 43, 46, 39, 200, 39, 36, 39],
    [21, 200, 200, 200, 200, 200, 200, 200, 200, 200, 200, 200, 200, 200, 200, 200],
    [26, 30, 31, 33, 41, 41, 47, 41, 46, 47, 50, 46, 36, 41, 40, 44],
]
ENTRIES = max(len(row) for row in TABLE)
SENDS = [sum((e // (64 << k)) % 2 for e in row for k in range(4)) for row in TABLE]


def rope_tables():
    half = HD // 2
    freqs = THETA ** (-2.0 * np.arange(half) / HD)
    inner = np.arange(STRETCH)[:, None] * freqs[None, :]
    outer = (np.arange(2 * N_CP) * STRETCH)[:, None] * freqs[None, :]

    def both(angles):
        c, s = np.cos(angles), np.sin(angles)
        return np.stack([np.concatenate([c, c], 1), np.concatenate([s, s], 1)])

    return both(inner).astype(np.float32), both(outer).astype(np.float32)


def kernel(
    tokens, gain, wq, wk, wv, wo, docs, rope_in, rope_out, out,
    x, xg, wkv, wqv, wo_own, wo_sib, acckv, accq, ssq, kvbuf, qs,
    m_ref, acc_ref, attn_own, attn_sib, send_a, recv_a, send_b, recv_b, qstart,
    gain_in, gain_row, doc_in, r_in, r_out, result,
    in_sems, x_sems, wo_sem, wos_send, wos_recv, kv_send, kv_recv,
    rs_send, at_recv, a_recv, b_recv, out_sems,
):
    d = lax.axis_index("cp")
    t = lax.axis_index("tp")
    z, core = t // 2, t % 2
    sib = t + 1 - 2 * core
    t_up = lax.rem(z + 1, 4) * 2 + core
    t_dn = lax.rem(z + 3, 4) * 2 + core
    zs = [z, lax.rem(z + 1, 4), lax.rem(z + 3, 4), lax.rem(z + 2, 4)]
    cl, cu = d, 2 * N_CP - 1 - d
    px, py = lax.rem(d, 4), lax.div(d, 4)
    beside = [
        py * 4 + lax.rem(px + 1, 4),
        py * 4 + lax.rem(px + 3, 4),
        lax.rem(py + 1, 4) * 4 + px,
        lax.rem(py + 3, 4) * 4 + px,
    ]

    def x_copy(i):
        cols = pl.ds(i * CHUNK, CHUNK)
        return pltpu.make_async_copy(tokens.at[:, cols], x.at[:, cols], x_sems.at[i])

    first_copies = [
        pltpu.make_async_copy(docs, doc_in, in_sems.at[0]),
        pltpu.make_async_copy(gain, gain_in, in_sems.at[1]),
        pltpu.make_async_copy(wk, wkv.at[:, 0:HD], in_sems.at[2]),
        pltpu.make_async_copy(wv, wkv.at[:, HD : 2 * HD], in_sems.at[3]),
    ]
    rope_copies = [
        pltpu.make_async_copy(rope_in, r_in, in_sems.at[4]),
        pltpu.make_async_copy(rope_out, r_out, in_sems.at[5]),
    ]
    wq_copy = pltpu.make_async_copy(wq, wqv, in_sems.at[6])

    def wo_copy(i):
        cols = pl.ds(pl.multiple_of((2 * i + core) * 512, 512), 512)
        return pltpu.make_async_copy(wo.at[:, cols], wo_own.at[i], wo_sem)

    for c in first_copies:
        c.start()
    for i in range(N_CHUNK):
        x_copy(i).start()
    for c in rope_copies:
        c.start()

    barrier = pltpu.get_barrier_semaphore()
    for e in beside:
        pl.semaphore_signal(barrier, 1, device_id={"cp": e, "tp": t})
    for other in (sib, t_up, t_dn):
        pl.semaphore_signal(barrier, 1, device_id={"cp": d, "tp": other})

    here = [(d == e).astype(jnp.int32) for e in range(N_CP)]

    def pick(values):
        total = jnp.int32(0)
        for e, v in enumerate(values):
            if v:
                total = total + here[e] * v
        return total

    words = [pick([row[i] if i < len(row) else 0 for row in TABLE]) for i in range(ENTRIES)]

    def chosen(values, i):
        while len(values) > 1:
            low = lax.rem(i, 2) == 0
            values = [
                jnp.where(low, values[k], values[k + 1]) if k + 1 < len(values) else values[k]
                for k in range(0, len(values), 2)
            ]
            i = lax.div(i, 2)
        return values[0]

    def entry(i):
        return chosen(words, i)

    at_query, at_whole, at_first, at_second, n_entries = [pick(m) for m in MARKS]
    n_sends = pick(SENDS)

    for c in first_copies[:2]:
        c.wait()
    table = doc_in[...].reshape(64, 128)
    rows = [
        doc_in[pl.ds(pl.multiple_of(c * STRETCH, STRETCH), STRETCH)].reshape(1, STRETCH) for c in (cl, cu)
    ]
    for i in range(N_CHUNK):
        cols = slice(i * CHUNK, (i + 1) * CHUNK)
        gain_row[:, cols] = gain_in[cols].astype(F32).reshape(1, CHUNK)
    starts = [jnp.zeros((1, STRETCH), F32) for _ in rows]
    for v in range(1, 16):
        below = jnp.where(table < v, 1.0, 0.0)
        count = jnp.sum(jnp.sum(below, axis=0, keepdims=True), axis=1, keepdims=True)
        starts = [jnp.where(r >= v, count, s) for r, s in zip(rows, starts)]
    qstart[0:1, :] = starts[0].astype(jnp.int32)
    qstart[1:2, :] = starts[1].astype(jnp.int32)
    m_ref[...] = jnp.full_like(m_ref, NEG)
    acc_ref[...] = jnp.zeros_like(acc_ref)

    acckv[...] = jnp.zeros_like(acckv)
    ssq[...] = jnp.zeros_like(ssq)
    for c in first_copies[2:]:
        c.wait()

    def kv_step(i, carry):
        x_copy(i).wait()

        @pl.when(i == N_CHUNK // 2)
        def _():
            wq_copy.start()

        cols = pl.ds(pl.multiple_of(i * CHUNK, CHUNK), CHUNK)
        xf = x[:, cols].astype(F32)
        sq = xf * xf
        ssq[...] += sq[:, 0:128] + sq[:, 128:256] + sq[:, 256:384] + sq[:, 384:512]
        scaled = (xf * gain_row[:, cols]).astype(BF16)
        xg[:, cols] = scaled
        acckv[...] += jnp.dot(scaled, wkv[cols, :], preferred_element_type=F32)
        return carry

    lax.fori_loop(0, N_CHUNK, kv_step, 0)
    for i in range(4):
        wo_copy(i).start()
    for c in rope_copies:
        c.wait()
    mean = jnp.sum(ssq[...], axis=1, keepdims=True) * (1.0 / D)
    factor = lax.rsqrt(mean + EPS)
    ssq[...] = jnp.broadcast_to(factor, (2 * STRETCH, HD))

    sign = jnp.where(lax.broadcasted_iota(jnp.int32, (1, HD), 1) < HD // 2, -1.0, 1.0)

    def rope(h):
        c = cl if h == 0 else cu
        co, so = r_out[0, pl.ds(c, 1), :], r_out[1, pl.ds(c, 1), :]
        ci, si = r_in[0], r_in[1]
        return ci * co - si * so, (ci * so + si * co) * sign

    for h, c in ((0, cl), (1, cu)):
        rs = slice(h * STRETCH, (h + 1) * STRETCH)
        cosine, sine = rope(h)
        kf = acckv[rs, 0:HD] * ssq[rs, :]
        kvbuf[2 * c] = (kf * cosine + pltpu.roll(kf, HD // 2, 1) * sine).astype(BF16)
        vf = acckv[rs, HD : 2 * HD] * ssq[rs, :]
        kvbuf[2 * c + 1, 0:HD, :] = vf[0:HD, :].T.astype(BF16)
        kvbuf[2 * c + 1, HD : 2 * HD, :] = vf[HD : 2 * HD, :].T.astype(BF16)

    pl.semaphore_wait(barrier, 7)

    def kv_slot(p, e):
        s = lax.div(p, 2)
        lower = (s < e) & (s >= e - REACH)
        return lax.rem(s, REACH) * 2 + lax.rem(p, 2) + jnp.where(lower, 0, 2 * REACH)

    def kv_copy(p, way):
        return pltpu.make_async_remote_copy(
            src_ref=kvbuf.at[p], dst_ref=kvbuf.at[p], send_sem=kv_send,
            recv_sem=kv_recv.at[kv_slot(p, beside[way])], device_id={"cp": beside[way], "tp": t},
        )

    def kv_wait(p):
        pltpu.make_async_remote_copy(
            src_ref=kvbuf.at[p], dst_ref=kvbuf.at[p], send_sem=kv_send,
            recv_sem=kv_recv.at[kv_slot(p, d)], device_id={"cp": beside[0], "tp": t},
        ).wait_recv()

    def pass_on(e, act):
        p, ways = lax.rem(e, 64), lax.rem(lax.div(e, 64), 16)

        @pl.when(ways > 0)
        def _():
            for way in range(4):
                @pl.when(lax.rem(lax.div(ways, 2**way), 2) == 1)
                def _():
                    act(kv_copy(p, way))

    def send_only(i, carry):
        pass_on(entry(i), lambda c: c.start())
        return carry

    lax.fori_loop(0, at_query, send_only, 0)

    def wos_copy(i):
        cols = pl.ds(pl.multiple_of((2 * i + 1 - core) * 512, 512), 512)
        return pltpu.make_async_remote_copy(
            src_ref=wo.at[:, cols], dst_ref=wo_sib.at[i], send_sem=wos_send,
            recv_sem=wos_recv, device_id={"cp": d, "tp": sib},
        )

    for i in range(4):
        wos_copy(i).start()

    wq_copy.wait()

    def q_step(i, carry):
        cols = pl.ds(pl.multiple_of(i * 256, 256), 256)
        accq[:, cols] = jnp.dot(xg[...], wqv[:, cols], preferred_element_type=F32)
        return carry

    lax.fori_loop(0, 2, q_step, 0)
    for h in range(2):
        rs = slice(h * STRETCH, (h + 1) * STRETCH)
        cosine, sine = rope(h)
        scale = ssq[rs, :] * QSCALE
        for g in range(GROUP):
            qf = accq[rs, g * HD : (g + 1) * HD] * scale
            qs[h, g * STRETCH : (g + 1) * STRETCH, :] = (
                qf * cosine + pltpu.roll(qf, HD // 2, 1) * sine
            ).astype(BF16)

    key_row = lax.broadcasted_iota(jnp.int32, (STRETCH, STRETCH), 0)
    query_col = lax.broadcasted_iota(jnp.int32, (STRETCH, STRETCH), 1)
    ones = jnp.ones((ONES, STRETCH), BF16)

    def block(h, s, own):
        keys = kvbuf[2 * s]
        vt = jnp.concatenate([kvbuf[2 * s + 1, 0:HD, :], kvbuf[2 * s + 1, HD : 2 * HD, :]], axis=1)
        vt = jnp.concatenate([vt, ones], axis=0)
        mask = key_row >= qstart[h : h + 1, :] - s * STRETCH
        if own:
            mask = mask & (key_row <= query_col)
        scores = [
            lax.dot_general(
                keys, qs[h, g * STRETCH : (g + 1) * STRETCH, :], (((1,), (1,)), ((), ())),
                preferred_element_type=F32,
            )
            for g in range(GROUP)
        ]
        before = [m_ref[h, g : g + 1, :] for g in range(GROUP)]
        held = [acc_ref[h, g] for g in range(GROUP)]
        tops, added = [], []
        for g in range(GROUP):
            sc = jnp.where(mask, scores[g], NEG)
            top = jnp.maximum(jnp.max(sc, axis=0, keepdims=True), before[g])
            weights = jnp.exp2(sc - top).astype(BF16)
            tops.append(top)
            added.append(jnp.dot(vt, weights, preferred_element_type=F32))
        for g in range(GROUP):
            acc_ref[h, g] = held[g] * jnp.exp2(before[g] - tops[g]) + added[g]
            m_ref[h, g : g + 1, :] = tops[g]

    def finish(h):
        for g in range(GROUP):
            o = acc_ref[h, g, 0:HD, :] / acc_ref[h, g, HD : HD + 1, :]
            attn_own[h, :, g * HD : (g + 1) * HD] = o.T.astype(BF16)

    def at_copy(h):
        return pltpu.make_async_remote_copy(
            src_ref=attn_own.at[h], dst_ref=attn_sib.at[h], send_sem=rs_send,
            recv_sem=at_recv.at[h], device_id={"cp": d, "tp": sib},
        )

    def project(h, i):
        zz = zs[i]
        return jnp.dot(attn_own[h], wo_own[zz], preferred_element_type=F32) + jnp.dot(
            attn_sib[h], wo_sib[zz], preferred_element_type=F32
        )

    def a_copy(h, way):
        return pltpu.make_async_remote_copy(
            src_ref=send_a.at[h, way], dst_ref=recv_a.at[h, way], send_sem=rs_send,
            recv_sem=a_recv.at[h, way], device_id={"cp": d, "tp": t_up if way == 0 else t_dn},
        )

    def b_copy(h, way, piece):
        return pltpu.make_async_remote_copy(
            src_ref=send_b.at[h, way, piece], dst_ref=recv_b.at[h, way, piece],
            send_sem=rs_send, recv_sem=b_recv.at[h],
            device_id={"cp": d, "tp": t_up if way == 0 else t_dn},
        )

    summed = [slice(0, 256), slice(256, 512)]
    plain = [slice(256, 512), slice(0, 256)]

    def scatter_first(h):
        at_copy(h).wait_recv()
        far = project(h, 3)
        for way in range(2):
            send_a[h, way] = far[:, summed[way]].astype(BF16)
            a_copy(h, way).start()
        for way in range(2):
            near = project(h, 1 + way)
            accq[h * STRETCH : (h + 1) * STRETCH, way * 256 : (way + 1) * 256] = near[:, summed[way]]
            send_b[h, way, 1] = near[:, plain[way]].astype(BF16)
            b_copy(h, way, 1).start()

    def scatter_second(h):
        for way in range(2):
            a_copy(h, way).wait_recv()
            own = accq[h * STRETCH : (h + 1) * STRETCH, way * 256 : (way + 1) * 256]
            send_b[h, way, 0] = (own + recv_a[h, way].astype(F32)).astype(BF16)
            b_copy(h, way, 0).start()

    def scatter_mine(h):
        accq[h * STRETCH : (h + 1) * STRETCH, :] = project(h, 0)

    def scatter_last(h):
        rs = slice(h * STRETCH, (h + 1) * STRETCH)
        pltpu.make_async_copy(recv_b.at[h], recv_b.at[h], b_recv.at[h]).wait()
        result[rs, 0:256] = (
            accq[rs, 0:256] + recv_b[h, 0, 0].astype(F32) + recv_b[h, 1, 1].astype(F32)
        ).astype(BF16)
        result[rs, 256:512] = (
            accq[rs, 256:512] + recv_b[h, 0, 1].astype(F32) + recv_b[h, 1, 0].astype(F32)
        ).astype(BF16)
        out_copy(h).start()

    def out_copy(h):
        rs = slice(h * STRETCH, (h + 1) * STRETCH)
        return pltpu.make_async_copy(result.at[rs], out.at[rs], out_sems.at[h])

    block(0, cl, True)

    @pl.when(at_whole < at_query)
    def _():
        finish(0)
        at_copy(0).start()
        block(1, cu, True)

    def weights_here():
        pltpu.make_async_copy(wo_own, wo_own, wo_sem).wait()
        pltpu.make_async_copy(wo_sib, wo_sib, wos_recv).wait()

    def main_step(i, carry):
        e = entry(i)
        p = lax.rem(e, 64)
        kind = lax.rem(lax.div(e, 1024), 4)
        job = lax.rem(lax.div(e, 4096), 4)
        s = lax.div(e, 16384)

        @pl.when(kind == 1)
        def _():
            kv_wait(p)

        @pl.when(kind == 2)
        def _():
            kv_wait(p)
            kv_wait(p + 1)

        pass_on(e, lambda c: c.start())

        @pl.when(job == 1)
        def _():
            block(0, s, False)

        @pl.when(i == at_whole)
        def _():
            finish(0)
            at_copy(0).start()
            block(1, cu, True)

        @pl.when(job == 2)
        def _():
            block(1, s, False)

        @pl.when(i == at_first)
        def _():
            weights_here()
            scatter_first(0)

        @pl.when(i == at_second)
        def _():
            scatter_second(0)
            scatter_mine(0)

        return carry

    lax.fori_loop(at_query, n_entries, main_step, 0)
    finish(1)
    at_copy(1).start()

    @pl.when(at_first >= n_entries)
    def _():
        weights_here()
        scatter_first(0)

    scatter_first(1)

    @pl.when(at_second >= n_entries)
    def _():
        scatter_second(0)
        scatter_mine(0)

    scatter_second(1)
    scatter_mine(1)
    scatter_last(0)
    scatter_last(1)
    for count in sorted(set(SENDS)):
        @pl.when(n_sends == count)
        def _():
            pltpu.make_async_copy(kvbuf.at[0:count], kvbuf.at[0:count], kv_send).wait()
    pltpu.make_async_copy(wo_sib, wo_sib, wos_send).wait()
    pltpu.make_async_copy(wo_own, wo_own, rs_send).wait()
    for h in range(2):
        out_copy(h).wait()


def step(tokens, gain, w_query, w_key, w_value, w_out, doc_ids):
    rope_in, rope_out = rope_tables()
    any_space = pl.BlockSpec(memory_space=pl.ANY)
    rows = 2 * STRETCH
    dma = pltpu.SemaphoreType.DMA
    return pl.pallas_call(
        kernel,
        out_shape=jax.ShapeDtypeStruct((rows, 512), BF16),
        in_specs=[any_space] * 9,
        out_specs=any_space,
        scratch_shapes=[
            pltpu.VMEM((rows, D), BF16),
            pltpu.VMEM((rows, D), BF16),
            pltpu.VMEM((D, 2 * HD), BF16),
            pltpu.VMEM((D, GROUP * HD), BF16),
            pltpu.VMEM((4, 512, 512), BF16),
            pltpu.VMEM((4, 512, 512), BF16),
            pltpu.VMEM((rows, 2 * HD), F32),
            pltpu.VMEM((rows, GROUP * HD), F32),
            pltpu.VMEM((rows, HD), F32),
            pltpu.VMEM((4 * N_CP, STRETCH, HD), BF16),
            pltpu.VMEM((2, GROUP * STRETCH, HD), BF16),
            pltpu.VMEM((2, 8, STRETCH), F32),
            pltpu.VMEM((2, GROUP, HD + ONES, STRETCH), F32),
            pltpu.VMEM((2, STRETCH, 512), BF16),
            pltpu.VMEM((2, STRETCH, 512), BF16),
            pltpu.VMEM((2, 2, STRETCH, 256), BF16),
            pltpu.VMEM((2, 2, STRETCH, 256), BF16),
            pltpu.VMEM((2, 2, 2, STRETCH, 256), BF16),
            pltpu.VMEM((2, 2, 2, STRETCH, 256), BF16),
            pltpu.VMEM((8, STRETCH), jnp.int32),
            pltpu.VMEM((D,), BF16),
            pltpu.VMEM((1, D), F32),
            pltpu.VMEM((2 * N_CP * STRETCH,), jnp.int32),
            pltpu.VMEM((2, STRETCH, HD), F32),
            pltpu.VMEM((2, 2 * N_CP, HD), F32),
            pltpu.VMEM((rows, 512), BF16),
            dma((7,)),
            dma((N_CHUNK,)),
            dma,
            dma,
            dma,
            dma,
            dma((4 * REACH,)),
            dma,
            dma((2,)),
            dma((2, 2)),
            dma((2,)),
            dma((2,)),
        ],
        compiler_params=pltpu.CompilerParams(
            collective_id=0, has_side_effects=True, vmem_limit_bytes=60 * 1024 * 1024
        ),
        name="block",
    )(
        tokens, gain, w_query, w_key, w_value, w_out,
        doc_ids, jnp.asarray(rope_in), jnp.asarray(rope_out),
    )


def solution(mesh):
    in_specs = (P("cp", None), P(), P(None, "tp"), P(None, "tp"), P(None, "tp"), P("tp", None), P())
    return jax.shard_map(step, mesh=mesh, in_specs=in_specs, out_specs=P("cp", "tp"), check_vma=False)
```

```python
import math

import jax
import jax.numpy as jnp
import numpy as np
from jax import lax
from jax.experimental import pallas as pl
from jax.experimental.pallas import tpu as pltpu
from jax.sharding import PartitionSpec as P

D = 4096
HEADS = 32
HD = 128
GROUP = 4
STRETCH = 256
N_CP = 16
REACH = 9
CHUNK = 512
N_CHUNK = D // CHUNK
NEG = -1e30
EPS = 1e-05
THETA = 500000.0
QSCALE = math.log2(math.e) / math.sqrt(HD)
ONES = 16
F32 = jnp.float32
BF16 = jnp.bfloat16

TABLE = [
    [256, 193, 192, 257, 1271, 16258104, 1270, 1081, 14673980, 16198656, 121, 1198, 1136, 1077, 1199, 1073, 1076, 12968046, 180, 1069, 11969708, 1075, 1330, 15624250],
    [66, 259, 189, 258, 67, 188, 1345, 1205, 1082, 1088, 1204, 21563, 117, 14131386, 1260, 1074, 1133, 1203, 2102, 12019768, 116, 187, 14575658, 11478127, 1070, 12970032],
    [260, 69, 186, 68, 261, 187, 1346, 1202, 1081, 1091, 1203, 562232, 13593600, 114, 184, 1281, 1259, 1072, 1024, 1066, 15209649, 115, 11478069, 106, 1324, 2088, 117, 10888237, 2102, 14525492, 12494894],
    [262, 120, 185, 263, 184, 121, 1025, 1285, 1264, 1024, 257, 1028, 54513, 13052928, 1282, 1192, 1079, 1027, 1065, 562358, 1138, 14491831, 1198, 1323, 1071, 13493299, 1066, 11888684, 2100, 10397734],
    [328, 137, 567, 136, 329, 566, 1472, 1582, 1073, 1281, 174, 1647, 1072, 71732, 110, 12509359, 1027, 1286, 1709, 14033009, 1026, 1287, 1594599, 258, 1190, 11854892, 112, 1028, 1285, 14193701, 172, 1188, 2088, 10789930, 1323, 13461554],
    [266, 75, 693, 74, 267, 692, 1475, 1032, 1580, 1074, 1410, 1097, 1581, 611379, 72, 11968684, 1088, 1025, 1412, 71210, 1285, 1125, 1583, 170, 1124, 1195, 9856046, 12413952, 179, 2054, 2082, 1611111, 1062, 10250288, 2088, 10890240],
    [268, 77, 690, 76, 269, 691, 1220, 1291, 1579, 260, 1157, 1098, 1578, 1153072, 261, 75, 11428011, 1026, 1091, 1414, 611362, 1159, 1577, 258, 98, 2056, 1123, 2151464, 169, 13113344, 168, 106, 9316384, 8727552, 2084, 2094, 12363820, 10332198],
    [270, 688, 113, 271, 112, 689, 1222, 1293, 1576, 1479, 2056, 1036, 1693225, 262, 168, 3215465, 1028, 1349, 10888353, 2048, 38062, 260, 104, 2058, 1056, 12330159, 2050, 2078, 612013, 1575, 2082, 1702, 2090, 9167916, 11332608, 9807908],
    [272, 209, 558, 208, 273, 559, 1480, 1063, 1581, 1481, 1062, 551, 2088, 2233388, 614, 10346663, 1088, 1294, 1573, 11870374, 1089, 2058, 1295, 1572, 2625701, 1055, 1350, 164, 2060, 3266592, 8693063, 1054, 2050, 577631, 12097540, 7596060, 2082, 11298858],
    [338, 556, 173, 339, 172, 557, 1482, 1041, 1060, 1578, 1419, 1040, 81, 1573, 2774059, 80, 548, 9805994, 1091, 1032, 1420, 1571, 1026, 1097, 660749, 131, 1570, 1309, 3216934, 1156, 1052, 9265252, 1029, 2074, 163, 101, 2048, 38926, 7053474, 2054, 1693728, 1063, 2078, 10233896, 10742784],
    [276, 85, 170, 555, 84, 277, 554, 171, 1484, 1042, 1570, 1064, 1421, 1107, 1059, 3315241, 1181, 82, 9265699, 1098, 1035, 1422, 2774044, 7677327, 75, 1568, 2052, 267, 2064, 1057, 99, 1167528, 161, 98, 2050, 2054, 661512, 2150569, 7088154, 2084, 2086, 10266648, 8071198],
    [279, 680, 105, 278, 104, 681, 1486, 1045, 6104609, 1487, 2064, 1044, 3855903, 1568, 276, 95, 5378209, 1160, 1036, 1357, 8136222, 1159, 1033, 2200669, 1030, 2066, 4773031, 1190, 2052, 2058, 2659877, 159, 1052, 7660580, 2072, 2082, 6596634, 7105536],
    [88, 153, 551, 152, 89, 550, 1232, 1056, 6612517, 1233, 1057, 4396580, 9710592, 1054, 96, 545, 1096, 1170, 544, 1097, 1171, 2070, 4788766, 1102, 8053791, 1103, 2058, 3855900, 95, 5330964, 2060, 1677318, 7513117, 2074, 9136162],
    [91, 548, 165, 90, 164, 549, 154, 539, 1234, 1048, 7120419, 1235, 1049, 4937250, 6450176, 1564, 88, 1226, 1040, 1044, 1163, 1105, 2822682, 1173, 5379616, 1036, 5531166, 140, 1037, 2056, 2199714, 1053, 8627233, 163, 2070, 3856398, 8053791],
    [93, 546, 163, 92, 162, 547, 156, 541, 1172, 1115, 7627806, 540, 1173, 1114, 5477920, 6990848, 1057, 85, 1100, 538, 158, 1175, 1037, 2066, 3363358, 1561, 1048, 6443169, 4990102, 539, 3856398, 2064, 536, 2058, 2757663, 5975040, 8006656],
    [158, 96, 545, 543, 160, 97, 94, 544, 161, 1239, 1049, 8135709, 542, 1110, 1048, 6018076, 153, 7541277, 1040, 1563, 150, 6479967, 2062, 1041, 1050, 144, 536, 4313180, 1108, 1045, 540, 5460127, 1036, 1101, 3908121, 2066, 538, 4821085, 6955099, 4893696],
]
MARKS = [
    [4, 6, 6, 6, 6, 6, 6, 6, 6, 6, 8, 6, 6, 8, 8, 9],
    [5, 11, 20, 19, 29, 31, 29, 28, 34, 40, 37, 30, 31, 35, 34, 37],
    [9, 15, 24, 23, 34, 34, 33, 31, 36, 200, 41, 35, 200, 200, 200, 200],
    [22, 200, 200, 200, 200, 200, 200, 200, 200, 200, 200, 200, 200, 200, 200, 200],
    [24, 26, 31, 30, 36, 36, 38, 36, 38, 45, 43, 38, 35, 37, 37, 40],
]
ENTRIES = max(len(row) for row in TABLE)
SENDS = [sum((e // (64 << k)) % 2 for e in row for k in range(4)) for row in TABLE]


def rope_tables():
    half = HD // 2
    freqs = THETA ** (-2.0 * np.arange(half) / HD)
    inner = np.arange(STRETCH)[:, None] * freqs[None, :]
    outer = (np.arange(2 * N_CP) * STRETCH)[:, None] * freqs[None, :]

    def both(angles):
        c, s = np.cos(angles), np.sin(angles)
        return np.stack([np.concatenate([c, c], 1), np.concatenate([s, s], 1)])

    return both(inner).astype(np.float32), both(outer).astype(np.float32)


def kernel(
    tokens, gain, wq, wk, wv, wo, docs, rope_in, rope_out, out,
    x, xg, wkv, wqv, wo_own, wo_sib, acckv, accq, ssq, kvbuf, qs,
    m_ref, acc_ref, attn_own, attn_sib, send_a, recv_a, send_b, recv_b, qstart,
    gain_in, gain_row, doc_in, r_in, r_out,
    in_sems, x_sems, wo_sem, wos_send, wos_recv, kv_send, kv_recv,
    rs_send, at_recv, a_recv, b_recv,
):
    d = lax.axis_index("cp")
    t = lax.axis_index("tp")
    z, core = t // 2, t % 2
    sib = t + 1 - 2 * core
    t_up = lax.rem(z + 1, 4) * 2 + core
    t_dn = lax.rem(z + 3, 4) * 2 + core
    zs = [z, lax.rem(z + 1, 4), lax.rem(z + 3, 4), lax.rem(z + 2, 4)]
    cl, cu = d, 2 * N_CP - 1 - d
    px, py = lax.rem(d, 4), lax.div(d, 4)
    beside = [
        py * 4 + lax.rem(px + 1, 4),
        py * 4 + lax.rem(px + 3, 4),
        lax.rem(py + 1, 4) * 4 + px,
        lax.rem(py + 3, 4) * 4 + px,
    ]

    def x_copy(i):
        cols = pl.ds(i * CHUNK, CHUNK)
        return pltpu.make_async_copy(tokens.at[:, cols], x.at[:, cols], x_sems.at[i])

    first_copies = [
        pltpu.make_async_copy(docs, doc_in, in_sems.at[0]),
        pltpu.make_async_copy(gain, gain_in, in_sems.at[1]),
        pltpu.make_async_copy(wk, wkv.at[:, 0:HD], in_sems.at[2]),
        pltpu.make_async_copy(wv, wkv.at[:, HD : 2 * HD], in_sems.at[3]),
    ]
    rope_copies = [
        pltpu.make_async_copy(rope_in, r_in, in_sems.at[4]),
        pltpu.make_async_copy(rope_out, r_out, in_sems.at[5]),
    ]
    wq_copy = pltpu.make_async_copy(wq, wqv, in_sems.at[6])

    def wo_copy(i):
        cols = pl.ds(pl.multiple_of((2 * i + core) * 512, 512), 512)
        return pltpu.make_async_copy(wo.at[:, cols], wo_own.at[i], wo_sem)

    for c in first_copies:
        c.start()
    for i in range(N_CHUNK):
        x_copy(i).start()
    for c in rope_copies:
        c.start()

    barrier = pltpu.get_barrier_semaphore()
    for e in beside:
        pl.semaphore_signal(barrier, 1, device_id={"cp": e, "tp": t})
    for other in (sib, t_up, t_dn):
        pl.semaphore_signal(barrier, 1, device_id={"cp": d, "tp": other})

    here = [(d == e).astype(jnp.int32) for e in range(N_CP)]

    def pick(values):
        total = jnp.int32(0)
        for e, v in enumerate(values):
            if v:
                total = total + here[e] * v
        return total

    words = [pick([row[i] if i < len(row) else 0 for row in TABLE]) for i in range(ENTRIES)]

    def chosen(values, i):
        while len(values) > 1:
            low = lax.rem(i, 2) == 0
            values = [
                jnp.where(low, values[k], values[k + 1]) if k + 1 < len(values) else values[k]
                for k in range(0, len(values), 2)
            ]
            i = lax.div(i, 2)
        return values[0]

    def entry(i):
        return chosen(words, i)

    at_query, at_whole, at_first, at_second, n_entries = [pick(m) for m in MARKS]
    n_sends = pick(SENDS)

    for c in first_copies[:2]:
        c.wait()
    table = doc_in[...].reshape(64, 128)
    rows = [
        doc_in[pl.ds(pl.multiple_of(c * STRETCH, STRETCH), STRETCH)].reshape(1, STRETCH) for c in (cl, cu)
    ]
    for i in range(N_CHUNK):
        cols = slice(i * CHUNK, (i + 1) * CHUNK)
        gain_row[:, cols] = gain_in[cols].astype(F32).reshape(1, CHUNK)
    starts = [jnp.zeros((1, STRETCH), F32) for _ in rows]
    for v in range(1, 16):
        below = jnp.where(table < v, 1.0, 0.0)
        count = jnp.sum(jnp.sum(below, axis=0, keepdims=True), axis=1, keepdims=True)
        starts = [jnp.where(r >= v, count, s) for r, s in zip(rows, starts)]
    qstart[0:1, :] = starts[0].astype(jnp.int32)
    qstart[1:2, :] = starts[1].astype(jnp.int32)
    m_ref[...] = jnp.full_like(m_ref, NEG)
    acc_ref[...] = jnp.zeros_like(acc_ref)

    acckv[...] = jnp.zeros_like(acckv)
    ssq[...] = jnp.zeros_like(ssq)
    for c in first_copies[2:]:
        c.wait()

    def kv_step(i, carry):
        x_copy(i).wait()

        @pl.when(i == N_CHUNK // 2)
        def _():
            wq_copy.start()

        cols = pl.ds(pl.multiple_of(i * CHUNK, CHUNK), CHUNK)
        xf = x[:, cols].astype(F32)
        sq = xf * xf
        ssq[...] += sq[:, 0:128] + sq[:, 128:256] + sq[:, 256:384] + sq[:, 384:512]
        scaled = (xf * gain_row[:, cols]).astype(BF16)
        xg[:, cols] = scaled
        acckv[...] += jnp.dot(scaled, wkv[cols, :], preferred_element_type=F32)
        return carry

    lax.fori_loop(0, N_CHUNK, kv_step, 0)
    for i in range(4):
        wo_copy(i).start()
    for c in rope_copies:
        c.wait()
    mean = jnp.sum(ssq[...], axis=1, keepdims=True) * (1.0 / D)
    factor = lax.rsqrt(mean + EPS)
    ssq[...] = jnp.broadcast_to(factor, (2 * STRETCH, HD))

    sign = jnp.where(lax.broadcasted_iota(jnp.int32, (1, HD), 1) < HD // 2, -1.0, 1.0)

    def rope(h):
        c = cl if h == 0 else cu
        co, so = r_out[0, pl.ds(c, 1), :], r_out[1, pl.ds(c, 1), :]
        ci, si = r_in[0], r_in[1]
        return ci * co - si * so, (ci * so + si * co) * sign

    for h, c in ((0, cl), (1, cu)):
        rs = slice(h * STRETCH, (h + 1) * STRETCH)
        cosine, sine = rope(h)
        kf = acckv[rs, 0:HD] * ssq[rs, :]
        kvbuf[2 * c] = (kf * cosine + pltpu.roll(kf, HD // 2, 1) * sine).astype(BF16)
        vf = acckv[rs, HD : 2 * HD] * ssq[rs, :]
        kvbuf[2 * c + 1, 0:HD, :] = vf[0:HD, :].T.astype(BF16)
        kvbuf[2 * c + 1, HD : 2 * HD, :] = vf[HD : 2 * HD, :].T.astype(BF16)

    pl.semaphore_wait(barrier, 7)

    def kv_slot(p, e):
        s = lax.div(p, 2)
        lower = (s < e) & (s >= e - REACH)
        return lax.rem(s, REACH) * 2 + lax.rem(p, 2) + jnp.where(lower, 0, 2 * REACH)

    def kv_copy(p, way):
        return pltpu.make_async_remote_copy(
            src_ref=kvbuf.at[p], dst_ref=kvbuf.at[p], send_sem=kv_send,
            recv_sem=kv_recv.at[kv_slot(p, beside[way])], device_id={"cp": beside[way], "tp": t},
        )

    def kv_wait(p):
        pltpu.make_async_remote_copy(
            src_ref=kvbuf.at[p], dst_ref=kvbuf.at[p], send_sem=kv_send,
            recv_sem=kv_recv.at[kv_slot(p, d)], device_id={"cp": beside[0], "tp": t},
        ).wait_recv()

    def pass_on(e, act):
        p, ways = lax.rem(e, 64), lax.rem(lax.div(e, 64), 16)

        @pl.when(ways > 0)
        def _():
            for way in range(4):
                @pl.when(lax.rem(lax.div(ways, 2**way), 2) == 1)
                def _():
                    act(kv_copy(p, way))

    def send_only(i, carry):
        pass_on(entry(i), lambda c: c.start())
        return carry

    lax.fori_loop(0, at_query, send_only, 0)

    def wos_copy(i):
        cols = pl.ds(pl.multiple_of((2 * i + 1 - core) * 512, 512), 512)
        return pltpu.make_async_remote_copy(
            src_ref=wo.at[:, cols], dst_ref=wo_sib.at[i], send_sem=wos_send,
            recv_sem=wos_recv, device_id={"cp": d, "tp": sib},
        )

    for i in range(4):
        wos_copy(i).start()

    wq_copy.wait()

    def q_step(i, carry):
        cols = pl.ds(pl.multiple_of(i * 256, 256), 256)
        accq[:, cols] = jnp.dot(xg[...], wqv[:, cols], preferred_element_type=F32)
        return carry

    lax.fori_loop(0, 2, q_step, 0)
    for h in range(2):
        rs = slice(h * STRETCH, (h + 1) * STRETCH)
        cosine, sine = rope(h)
        scale = ssq[rs, :] * QSCALE
        for g in range(GROUP):
            qf = accq[rs, g * HD : (g + 1) * HD] * scale
            qs[h, g * STRETCH : (g + 1) * STRETCH, :] = (
                qf * cosine + pltpu.roll(qf, HD // 2, 1) * sine
            ).astype(BF16)

    key_row = lax.broadcasted_iota(jnp.int32, (STRETCH, STRETCH), 0)
    query_col = lax.broadcasted_iota(jnp.int32, (STRETCH, STRETCH), 1)
    ones = jnp.ones((ONES, 2 * STRETCH), BF16)

    def attend(h, s1, s2):
        c = jnp.where(h == 0, cl, cu)
        keys = jnp.concatenate([kvbuf[2 * s1], kvbuf[2 * s2]], axis=0)
        vt = jnp.concatenate([kvbuf[2 * s + 1, r : r + HD, :] for s in (s1, s2) for r in (0, HD)], axis=1)
        vt = jnp.concatenate([vt, ones], axis=0)
        begin = qstart[pl.ds(h, 1), :]
        mask = jnp.concatenate(
            [
                (key_row >= begin - s * STRETCH) & (key_row <= query_col + (c - s) * STRETCH)
                for s in (s1, s2)
            ],
            axis=0,
        )
        scores = [
            lax.dot_general(
                keys, qs[h, g * STRETCH : (g + 1) * STRETCH, :], (((1,), (1,)), ((), ())),
                preferred_element_type=F32,
            )
            for g in range(GROUP)
        ]
        before = [m_ref[h, g : g + 1, :] for g in range(GROUP)]
        held = [acc_ref[h, g] for g in range(GROUP)]
        tops, added = [], []
        for g in range(GROUP):
            sc = jnp.where(mask, scores[g], NEG)
            top = jnp.maximum(jnp.max(sc, axis=0, keepdims=True), before[g])
            weights = jnp.exp2(sc - top).astype(BF16)
            tops.append(top)
            added.append(jnp.dot(vt, weights, preferred_element_type=F32))
        for g in range(GROUP):
            acc_ref[h, g] = held[g] * jnp.exp2(before[g] - tops[g]) + added[g]
            m_ref[h, g : g + 1, :] = tops[g]

    def finish(h):
        for g in range(GROUP):
            o = acc_ref[h, g, 0:HD, :] / acc_ref[h, g, HD : HD + 1, :]
            attn_own[h, :, g * HD : (g + 1) * HD] = o.T.astype(BF16)

    def at_copy(h):
        return pltpu.make_async_remote_copy(
            src_ref=attn_own.at[h], dst_ref=attn_sib.at[h], send_sem=rs_send,
            recv_sem=at_recv.at[h], device_id={"cp": d, "tp": sib},
        )

    def project(h, i):
        zz = zs[i]
        return jnp.dot(attn_own[h], wo_own[zz], preferred_element_type=F32) + jnp.dot(
            attn_sib[h], wo_sib[zz], preferred_element_type=F32
        )

    def a_copy(h, way):
        return pltpu.make_async_remote_copy(
            src_ref=send_a.at[h, way], dst_ref=recv_a.at[h, way], send_sem=rs_send,
            recv_sem=a_recv.at[h, way], device_id={"cp": d, "tp": t_up if way == 0 else t_dn},
        )

    def b_copy(h, way, piece):
        return pltpu.make_async_remote_copy(
            src_ref=send_b.at[h, way, piece], dst_ref=recv_b.at[h, way, piece],
            send_sem=rs_send, recv_sem=b_recv.at[h],
            device_id={"cp": d, "tp": t_up if way == 0 else t_dn},
        )

    summed = [slice(0, 256), slice(256, 512)]
    plain = [slice(256, 512), slice(0, 256)]

    def scatter_first(h):
        at_copy(h).wait_recv()
        far = project(h, 3)
        for way in range(2):
            send_a[h, way] = far[:, summed[way]].astype(BF16)
            a_copy(h, way).start()
        for way in range(2):
            near = project(h, 1 + way)
            accq[h * STRETCH : (h + 1) * STRETCH, way * 256 : (way + 1) * 256] = near[:, summed[way]]
            send_b[h, way, 1] = near[:, plain[way]].astype(BF16)
            b_copy(h, way, 1).start()

    def scatter_second(h):
        for way in range(2):
            a_copy(h, way).wait_recv()
            own = accq[h * STRETCH : (h + 1) * STRETCH, way * 256 : (way + 1) * 256]
            send_b[h, way, 0] = (own + recv_a[h, way].astype(F32)).astype(BF16)
            b_copy(h, way, 0).start()

    def scatter_mine(h):
        accq[h * STRETCH : (h + 1) * STRETCH, :] = project(h, 0)

    def scatter_last(h):
        rs = slice(h * STRETCH, (h + 1) * STRETCH)
        pltpu.make_async_copy(recv_b.at[h], recv_b.at[h], b_recv.at[h]).wait()
        out[rs, 0:256] = (
            accq[rs, 0:256] + recv_b[h, 0, 0].astype(F32) + recv_b[h, 1, 1].astype(F32)
        ).astype(BF16)
        out[rs, 256:512] = (
            accq[rs, 256:512] + recv_b[h, 0, 1].astype(F32) + recv_b[h, 1, 0].astype(F32)
        ).astype(BF16)

    def weights_here():
        pltpu.make_async_copy(wo_own, wo_own, wo_sem).wait()
        pltpu.make_async_copy(wo_sib, wo_sib, wos_recv).wait()

    def main_step(i, carry):
        e = entry(i)
        p = lax.rem(e, 64)
        kind = lax.rem(lax.div(e, 1024), 4)
        job = lax.rem(lax.div(e, 4096), 4)
        s1, s2 = lax.rem(lax.div(e, 16384), 32), lax.div(e, 524288)

        @pl.when(kind == 1)
        def _():
            kv_wait(p)

        @pl.when(kind == 2)
        def _():
            kv_wait(p)
            kv_wait(p + 1)

        pass_on(e, lambda c: c.start())

        @pl.when(job > 0)
        def _():
            attend(job - 1, s1, s2)

        @pl.when(i == at_whole)
        def _():
            finish(0)
            at_copy(0).start()

        @pl.when(i == at_first)
        def _():
            weights_here()
            scatter_first(0)

        @pl.when(i == at_second)
        def _():
            scatter_second(0)
            scatter_mine(0)

        return carry

    lax.fori_loop(at_query, n_entries, main_step, 0)
    finish(1)
    at_copy(1).start()

    @pl.when(at_first >= n_entries)
    def _():
        weights_here()
        scatter_first(0)

    scatter_first(1)

    @pl.when(at_second >= n_entries)
    def _():
        scatter_second(0)
        scatter_mine(0)

    scatter_second(1)
    scatter_mine(1)
    scatter_last(0)
    scatter_last(1)
    for count in sorted(set(SENDS)):
        @pl.when(n_sends == count)
        def _():
            pltpu.make_async_copy(kvbuf.at[0:count], kvbuf.at[0:count], kv_send).wait()
    pltpu.make_async_copy(wo_sib, wo_sib, wos_send).wait()
    pltpu.make_async_copy(wo_own, wo_own, rs_send).wait()


def step(tokens, gain, w_query, w_key, w_value, w_out, doc_ids):
    rope_in, rope_out = rope_tables()
    any_space = pl.BlockSpec(memory_space=pl.ANY)
    rows = 2 * STRETCH
    dma = pltpu.SemaphoreType.DMA
    return pl.pallas_call(
        kernel,
        out_shape=pltpu.VMEM((rows, 512), BF16),
        in_specs=[any_space] * 9,
        out_specs=pl.BlockSpec(memory_space=pltpu.VMEM),
        scratch_shapes=[
            pltpu.VMEM((rows, D), BF16),
            pltpu.VMEM((rows, D), BF16),
            pltpu.VMEM((D, 2 * HD), BF16),
            pltpu.VMEM((D, GROUP * HD), BF16),
            pltpu.VMEM((4, 512, 512), BF16),
            pltpu.VMEM((4, 512, 512), BF16),
            pltpu.VMEM((rows, 2 * HD), F32),
            pltpu.VMEM((rows, GROUP * HD), F32),
            pltpu.VMEM((rows, HD), F32),
            pltpu.VMEM((4 * N_CP, STRETCH, HD), BF16),
            pltpu.VMEM((2, GROUP * STRETCH, HD), BF16),
            pltpu.VMEM((2, 8, STRETCH), F32),
            pltpu.VMEM((2, GROUP, HD + ONES, STRETCH), F32),
            pltpu.VMEM((2, STRETCH, 512), BF16),
            pltpu.VMEM((2, STRETCH, 512), BF16),
            pltpu.VMEM((2, 2, STRETCH, 256), BF16),
            pltpu.VMEM((2, 2, STRETCH, 256), BF16),
            pltpu.VMEM((2, 2, 2, STRETCH, 256), BF16),
            pltpu.VMEM((2, 2, 2, STRETCH, 256), BF16),
            pltpu.VMEM((8, STRETCH), jnp.int32),
            pltpu.VMEM((D,), BF16),
            pltpu.VMEM((1, D), F32),
            pltpu.VMEM((2 * N_CP * STRETCH,), jnp.int32),
            pltpu.VMEM((2, STRETCH, HD), F32),
            pltpu.VMEM((2, 2 * N_CP, HD), F32),
            dma((7,)),
            dma((N_CHUNK,)),
            dma,
            dma,
            dma,
            dma,
            dma((4 * REACH,)),
            dma,
            dma((2,)),
            dma((2, 2)),
            dma((2,)),
        ],
        compiler_params=pltpu.CompilerParams(
            collective_id=0, has_side_effects=True, vmem_limit_bytes=60 * 1024 * 1024
        ),
        name="block",
    )(
        tokens, gain, w_query, w_key, w_value, w_out,
        doc_ids, jnp.asarray(rope_in), jnp.asarray(rope_out),
    )


def solution(mesh):
    in_specs = (P("cp", None), P(), P(None, "tp"), P(None, "tp"), P(None, "tp"), P("tp", None), P())
    return jax.shard_map(step, mesh=mesh, in_specs=in_specs, out_specs=P("cp", "tp"), check_vma=False)
```

```python
import math

import jax
import jax.numpy as jnp
import numpy as np
from jax import lax
from jax.experimental import pallas as pl
from jax.experimental.pallas import tpu as pltpu
from jax.sharding import PartitionSpec as P

D = 4096
HEADS = 32
HD = 128
GROUP = 4
STRETCH = 256
N_CP = 16
REACH = 9
CHUNK = 512
N_CHUNK = D // CHUNK
NEG = -1e30
EPS = 1e-05
THETA = 500000.0
QSCALE = math.log2(math.e) / math.sqrt(HD)
ONES = 16
F32 = jnp.float32
BF16 = jnp.bfloat16

TABLE = [
    [449, 448, 1271, 1081, 16258109, 1270, 1080, 14672956, 121, 1198, 1076, 1072, 16195694, 1073, 113, 180, 1071, 12461109, 1331, 13542450, 2092, 15575098],
    [322, 323, 189, 188, 1344, 1204, 1083, 116, 187, 1025, 1077, 21562, 117, 14131381, 1075, 1202, 1143, 1078, 13591608, 1081, 2092, 186, 118, 15131952, 2090, 11379761, 12462126],
    [324, 325, 187, 186, 1346, 1203, 1080, 115, 184, 1027, 1074, 1081, 561411, 13590595, 1280, 1200, 1067, 114, 1076, 1025, 1066, 171, 15208554, 1077, 1073, 11477109, 1132, 13018167, 2088, 1069, 11871286, 12511278],
    [262, 263, 249, 248, 1284, 1024, 1264, 256, 1025, 1029, 1073, 53377, 261, 13050033, 1026, 1064, 258, 168, 1139, 2102, 10937385, 1283, 561321, 1070, 1074, 174, 2090, 1071, 11429940, 14017575, 2092, 10331174],
    [456, 457, 567, 566, 1473, 1582, 1072, 174, 110, 1071, 1280, 1585, 71732, 111, 559, 12509359, 1282, 1030, 1127, 14033063, 1581, 1068, 1065, 70, 262, 173, 1027, 1031, 1062, 1593900, 1188, 1284, 10331240, 259, 14193669, 11348010, 1061, 13412402],
    [331, 330, 692, 693, 1410, 1097, 1580, 1075, 172, 108, 1027, 1069, 1288, 611890, 131, 259, 557, 11968621, 1028, 1025, 1188, 1280, 69697, 1070, 1578, 1195, 110, 265, 1071, 1029, 11428901, 559, 1127, 165, 9822469, 1030, 100, 178, 262, 1031, 1611810, 263, 10774568, 1062, 12904496],
    [332, 333, 691, 690, 1412, 1099, 1579, 1073, 171, 107, 1029, 1290, 1066, 1072, 1151530, 133, 74, 11428107, 1030, 1186, 1026, 261, 106, 2056, 1580, 1027, 2184233, 1415, 1581, 1064, 1593452, 1059, 2048, 262, 177, 13111395, 1583, 1125, 1070, 11936002, 2080, 1060, 9249027, 8775718, 10267648],
    [270, 271, 752, 753, 1478, 1032, 1576, 1036, 136, 268, 1031, 1037, 1129, 1033, 1692201, 135, 71, 2199821, 1028, 1035, 1184, 68, 263, 1070, 1579, 2048, 10888222, 1349, 1711, 1053706, 1063, 264, 1066, 11395623, 1069, 557, 267, 2050, 611494, 1068, 11854374, 1055, 2082, 1057, 9168932, 9710592],
    [558, 464, 465, 559, 1767, 1064, 1288, 1069, 104, 557, 1062, 1161, 1065, 1068, 10346761, 102, 166, 11870758, 1060, 1376, 1025, 164, 552, 1067, 1061, 1039, 2233344, 1249, 2078, 1578, 8691983, 11265356, 1030, 65, 262, 1038, 2082, 7628828, 78, 1287, 3675146, 2050, 2052, 578571, 2659341, 12164096],
    [339, 338, 685, 684, 1764, 1067, 1291, 1041, 171, 81, 1061, 1578, 1040, 9807114, 101, 170, 549, 4346128, 1058, 1127, 162, 1577, 1288, 2076, 7693352, 1699, 1126, 2050, 9249819, 138, 550, 610384, 1033, 1050, 2080, 2078, 73, 7135371, 72, 8136708, 2060, 1120256, 2054, 104462, 3726336],
    [341, 340, 683, 682, 1762, 1065, 1298, 1037, 169, 553, 1059, 1107, 1036, 1064, 9265421, 99, 163, 552, 4886796, 1060, 1115, 1156, 1056, 547, 1297, 1050, 1034, 7152655, 1637, 1057, 1182, 1035, 8691983, 1029, 2076, 141, 545, 2723914, 2086, 143, 10199108, 2072, 8070175, 2054, 1040, 1610766, 3807240, 595970],
    [279, 278, 744, 745, 1760, 1296, 1038, 6104084, 1054, 1041, 1301, 1231, 4379166, 158, 271, 3838046, 1570, 1053, 1030, 1063, 270, 157, 1100, 1049, 268, 153, 78, 1574, 1052, 1037, 7660579, 1183, 1095, 8151583, 1048, 142, 2084, 1569, 9643077, 2074, 7086157, 2056, 1677330, 2058, 4789252, 1137664],
    [551, 550, 216, 217, 1631, 1040, 6612004, 1057, 1573, 4396241, 545, 97, 1053, 1047, 1032, 541, 87, 1170, 1046, 6071305, 86, 1054, 7595548, 94, 1056, 7088154, 73, 2282517, 1039, 79, 1044, 9087010, 1038, 3838982, 2060, 1031, 1676307, 2775050],
    [676, 677, 91, 90, 1693, 1107, 7119897, 1052, 1048, 1170, 540, 6529113, 156, 88, 6509083, 1055, 1035, 543, 154, 75, 1034, 2774033, 538, 1187, 2080, 1040, 8544330, 1058, 162, 139, 5531668, 5380118, 1054, 8052883, 2060, 2056, 3330186, 3741710],
    [546, 547, 221, 220, 1627, 1184, 7627797, 1057, 1626, 7087252, 545, 163, 7049300, 1043, 1042, 162, 83, 4891164, 1049, 2070, 1037, 149, 4886605, 1560, 1036, 6480013, 2078, 6475916, 4450320, 2058, 4297743, 1166, 3759104],
    [672, 542, 95, 225, 1565, 1239, 8135704, 1052, 1561, 6530262, 540, 94, 7590047, 1040, 1051, 543, 158, 5967963, 1045, 1050, 1041, 536, 85, 7004304, 1044, 1039, 538, 5382228, 1166, 1043, 1042, 78, 4842002, 1037, 1036, 4411469, 3841024, 3300352],
]
CUT = 8
MARKS = [
    [2, 4, 4, 4, 4, 4, 4, 4, 4, 4, 4, 4, 4, 4, 4, 4],
    [4, 11, 22, 22, 34, 40, 35, 38, 37, 39, 42, 40, 31, 33, 28, 32],
    [8, 14, 25, 25, 36, 42, 39, 41, 40, 41, 45, 42, 33, 36, 31, 36],
    [18, 25, 200, 200, 200, 200, 200, 200, 200, 200, 200, 200, 200, 200, 200, 200],
    [22, 27, 32, 32, 38, 45, 45, 46, 46, 45, 48, 46, 38, 38, 33, 38],
]
ENTRIES = max(len(row) for row in TABLE)
SENDS = [sum((e // (64 << k)) % 2 for e in row for k in range(4)) for row in TABLE]


def rope_tables():
    half = HD // 2
    freqs = THETA ** (-2.0 * np.arange(half) / HD)
    inner = np.arange(STRETCH)[:, None] * freqs[None, :]
    outer = (np.arange(2 * N_CP) * STRETCH)[:, None] * freqs[None, :]

    def both(angles):
        c, s = np.cos(angles), np.sin(angles)
        return np.stack([np.concatenate([c, c], 1), np.concatenate([s, s], 1)])

    return both(inner).astype(np.float32), both(outer).astype(np.float32)


def kernel(
    tokens, gain, wq, wk, wv, wo, docs, rope_in, rope_out, out,
    x, xg, wkv, wqv, wo_own, wo_sib, acckv, accq, ssq, kvbuf, qs,
    m_ref, acc_ref, attn_own, attn_sib, send_a, recv_a, send_b, recv_b, qstart,
    gain_in, gain_row, doc_in, r_in, r_out,
    in_sems, x_sems, wo_sem, wos_send, wos_recv, kv_send, kv_recv,
    rs_send, at_recv, a_recv, b_recv,
):
    d = lax.axis_index("cp")
    t = lax.axis_index("tp")
    z, core = t // 2, t % 2
    sib = t + 1 - 2 * core
    t_up = lax.rem(z + 1, 4) * 2 + core
    t_dn = lax.rem(z + 3, 4) * 2 + core
    zs = [z, lax.rem(z + 1, 4), lax.rem(z + 3, 4), lax.rem(z + 2, 4)]
    cl, cu = d, 2 * N_CP - 1 - d
    early = jnp.where(d < CUT, 0, 1)
    late = 1 - early

    def of(h):
        return pl.ds(pl.multiple_of(h * STRETCH, STRETCH), STRETCH)

    px, py = lax.rem(d, 4), lax.div(d, 4)
    beside = [
        py * 4 + lax.rem(px + 1, 4),
        py * 4 + lax.rem(px + 3, 4),
        lax.rem(py + 1, 4) * 4 + px,
        lax.rem(py + 3, 4) * 4 + px,
    ]

    def x_copy(i):
        cols = pl.ds(i * CHUNK, CHUNK)
        return pltpu.make_async_copy(tokens.at[:, cols], x.at[:, cols], x_sems.at[i])

    first_copies = [
        pltpu.make_async_copy(docs, doc_in, in_sems.at[0]),
        pltpu.make_async_copy(gain, gain_in, in_sems.at[1]),
        pltpu.make_async_copy(wk, wkv.at[:, 0:HD], in_sems.at[2]),
        pltpu.make_async_copy(wv, wkv.at[:, HD : 2 * HD], in_sems.at[3]),
    ]
    rope_copies = [
        pltpu.make_async_copy(rope_in, r_in, in_sems.at[4]),
        pltpu.make_async_copy(rope_out, r_out, in_sems.at[5]),
    ]
    wq_copy = pltpu.make_async_copy(wq, wqv, in_sems.at[6])

    def wo_copy(i):
        cols = pl.ds(pl.multiple_of((2 * i + core) * 512, 512), 512)
        return pltpu.make_async_copy(wo.at[:, cols], wo_own.at[i], wo_sem)

    first_copies[1].start()
    for i in range(N_CHUNK):
        x_copy(i).start()
    for c in (first_copies[2], first_copies[3], first_copies[0]):
        c.start()
    for c in rope_copies:
        c.start()

    barrier = pltpu.get_barrier_semaphore()
    for e in beside:
        pl.semaphore_signal(barrier, 1, device_id={"cp": e, "tp": t})
    for other in (sib, t_up, t_dn):
        pl.semaphore_signal(barrier, 1, device_id={"cp": d, "tp": other})

    here = [(d == e).astype(jnp.int32) for e in range(N_CP)]

    def pick(values):
        total = jnp.int32(0)
        for e, v in enumerate(values):
            if v:
                total = total + here[e] * v
        return total

    words = [pick([row[i] if i < len(row) else 0 for row in TABLE]) for i in range(ENTRIES)]

    def chosen(values, i):
        while len(values) > 1:
            low = lax.rem(i, 2) == 0
            values = [
                jnp.where(low, values[k], values[k + 1]) if k + 1 < len(values) else values[k]
                for k in range(0, len(values), 2)
            ]
            i = lax.div(i, 2)
        return values[0]

    def entry(i):
        return chosen(words, i)

    at_query, at_whole, at_first, at_second, n_entries = [pick(m) for m in MARKS]
    n_sends = pick(SENDS)

    ssq[...] = jnp.zeros_like(ssq)
    first_copies[1].wait()
    for i in range(N_CHUNK):
        cols = slice(i * CHUNK, (i + 1) * CHUNK)
        gain_row[:, cols] = gain_in[cols].astype(F32).reshape(1, CHUNK)

    def scale_chunk(i):
        x_copy(i).wait()
        cols = pl.ds(pl.multiple_of(i * CHUNK, CHUNK), CHUNK)
        xf = x[:, cols].astype(F32)
        sq = xf * xf
        ssq[...] += sq[:, 0:128] + sq[:, 128:256] + sq[:, 256:384] + sq[:, 384:512]
        xg[:, cols] = (xf * gain_row[:, cols]).astype(BF16)

    def scale_step(i, carry):
        @pl.when(i == N_CHUNK // 2)
        def _():
            wq_copy.start()

        scale_chunk(i)
        return carry

    lax.fori_loop(0, N_CHUNK, scale_step, 0)
    for c in first_copies[2:]:
        c.wait()
    acckv[...] = jnp.dot(xg[...], wkv[...], preferred_element_type=F32)
    for i in range(4):
        wo_copy(i).start()
    for c in rope_copies:
        c.wait()
    mean = jnp.sum(ssq[...], axis=1, keepdims=True) * (1.0 / D)
    factor = lax.rsqrt(mean + EPS)
    ssq[...] = jnp.broadcast_to(factor, (2 * STRETCH, HD))

    sign = jnp.where(lax.broadcasted_iota(jnp.int32, (1, HD), 1) < HD // 2, -1.0, 1.0)

    def rope(h):
        c = cl if h == 0 else cu
        co, so = r_out[0, pl.ds(c, 1), :], r_out[1, pl.ds(c, 1), :]
        ci, si = r_in[0], r_in[1]
        return ci * co - si * so, (ci * so + si * co) * sign

    for h, c in ((0, cl), (1, cu)):
        rs = slice(h * STRETCH, (h + 1) * STRETCH)
        cosine, sine = rope(h)
        kf = acckv[rs, 0:HD] * ssq[rs, :]
        kvbuf[2 * c] = (kf * cosine + pltpu.roll(kf, HD // 2, 1) * sine).astype(BF16)
        vf = acckv[rs, HD : 2 * HD] * ssq[rs, :]
        kvbuf[2 * c + 1, 0:HD, :] = vf[0:HD, :].T.astype(BF16)
        kvbuf[2 * c + 1, HD : 2 * HD, :] = vf[HD : 2 * HD, :].T.astype(BF16)

    pl.semaphore_wait(barrier, 7)

    def kv_slot(p, e):
        s = lax.div(p, 2)
        lower = (s < e) & (s >= e - REACH)
        return lax.rem(s, REACH) * 2 + lax.rem(p, 2) + jnp.where(lower, 0, 2 * REACH)

    def kv_copy(p, way):
        return pltpu.make_async_remote_copy(
            src_ref=kvbuf.at[p], dst_ref=kvbuf.at[p], send_sem=kv_send,
            recv_sem=kv_recv.at[kv_slot(p, beside[way])], device_id={"cp": beside[way], "tp": t},
        )

    def kv_wait(p):
        pltpu.make_async_remote_copy(
            src_ref=kvbuf.at[p], dst_ref=kvbuf.at[p], send_sem=kv_send,
            recv_sem=kv_recv.at[kv_slot(p, d)], device_id={"cp": beside[0], "tp": t},
        ).wait_recv()

    def pass_on(e, act):
        p, ways = lax.rem(e, 64), lax.rem(lax.div(e, 64), 16)

        @pl.when(ways > 0)
        def _():
            for way in range(4):
                @pl.when(lax.rem(lax.div(ways, 2**way), 2) == 1)
                def _():
                    act(kv_copy(p, way))

    def send_only(i, carry):
        pass_on(entry(i), lambda c: c.start())
        return carry

    lax.fori_loop(0, at_query, send_only, 0)

    def wos_copy(i):
        cols = pl.ds(pl.multiple_of((2 * i + 1 - core) * 512, 512), 512)
        return pltpu.make_async_remote_copy(
            src_ref=wo.at[:, cols], dst_ref=wo_sib.at[i], send_sem=wos_send,
            recv_sem=wos_recv, device_id={"cp": d, "tp": sib},
        )

    for i in range(4):
        wos_copy(i).start()

    first_copies[0].wait()
    table = doc_in[...].reshape(64, 128)
    rows = [
        doc_in[pl.ds(pl.multiple_of(c * STRETCH, STRETCH), STRETCH)].reshape(1, STRETCH) for c in (cl, cu)
    ]
    starts = [jnp.zeros((1, STRETCH), F32) for _ in rows]
    for v in range(1, 16):
        below = jnp.where(table < v, 1.0, 0.0)
        count = jnp.sum(jnp.sum(below, axis=0, keepdims=True), axis=1, keepdims=True)
        starts = [jnp.where(r >= v, count, s) for r, s in zip(rows, starts)]
    qstart[0:1, :] = starts[0].astype(jnp.int32)
    qstart[1:2, :] = starts[1].astype(jnp.int32)
    m_ref[...] = jnp.full_like(m_ref, NEG)
    acc_ref[...] = jnp.zeros_like(acc_ref)

    wq_copy.wait()

    def q_step(i, carry):
        cols = pl.ds(pl.multiple_of(i * 256, 256), 256)
        accq[:, cols] = jnp.dot(xg[...], wqv[:, cols], preferred_element_type=F32)
        return carry

    lax.fori_loop(0, 2, q_step, 0)
    for h in range(2):
        rs = slice(h * STRETCH, (h + 1) * STRETCH)
        cosine, sine = rope(h)
        scale = ssq[rs, :] * QSCALE
        for g in range(GROUP):
            qf = accq[rs, g * HD : (g + 1) * HD] * scale
            qs[h, g * STRETCH : (g + 1) * STRETCH, :] = (
                qf * cosine + pltpu.roll(qf, HD // 2, 1) * sine
            ).astype(BF16)

    key_row = lax.broadcasted_iota(jnp.int32, (STRETCH, STRETCH), 0)
    query_col = lax.broadcasted_iota(jnp.int32, (STRETCH, STRETCH), 1)
    ones = jnp.ones((ONES, 2 * STRETCH), BF16)

    def attend(h, s1, s2):
        c = jnp.where(h == 0, cl, cu)
        keys = jnp.concatenate([kvbuf[2 * s1], kvbuf[2 * s2]], axis=0)
        vt = jnp.concatenate([kvbuf[2 * s + 1, r : r + HD, :] for s in (s1, s2) for r in (0, HD)], axis=1)
        vt = jnp.concatenate([vt, ones], axis=0)
        begin = qstart[pl.ds(h, 1), :]
        mask = jnp.concatenate(
            [
                (key_row >= begin - s * STRETCH) & (key_row <= query_col + (c - s) * STRETCH)
                for s in (s1, s2)
            ],
            axis=0,
        )
        scores = [
            lax.dot_general(
                keys, qs[h, g * STRETCH : (g + 1) * STRETCH, :], (((1,), (1,)), ((), ())),
                preferred_element_type=F32,
            )
            for g in range(GROUP)
        ]
        before = [m_ref[h, g : g + 1, :] for g in range(GROUP)]
        held = [acc_ref[h, g] for g in range(GROUP)]
        tops, added = [], []
        for g in range(GROUP):
            sc = jnp.where(mask, scores[g], NEG)
            top = jnp.maximum(jnp.max(sc, axis=0, keepdims=True), before[g])
            weights = jnp.exp2(sc - top).astype(BF16)
            tops.append(top)
            added.append(jnp.dot(vt, weights, preferred_element_type=F32))
        for g in range(GROUP):
            acc_ref[h, g] = held[g] * jnp.exp2(before[g] - tops[g]) + added[g]
            m_ref[h, g : g + 1, :] = tops[g]

    def finish(h):
        for g in range(GROUP):
            o = acc_ref[h, g, 0:HD, :] / acc_ref[h, g, HD : HD + 1, :]
            attn_own[h, :, g * HD : (g + 1) * HD] = o.T.astype(BF16)

    def at_copy(h):
        return pltpu.make_async_remote_copy(
            src_ref=attn_own.at[h], dst_ref=attn_sib.at[h], send_sem=rs_send,
            recv_sem=at_recv.at[h], device_id={"cp": d, "tp": sib},
        )

    def project(h, i):
        zz = zs[i]
        return jnp.dot(attn_own[h], wo_own[zz], preferred_element_type=F32) + jnp.dot(
            attn_sib[h], wo_sib[zz], preferred_element_type=F32
        )

    def a_copy(h, way):
        return pltpu.make_async_remote_copy(
            src_ref=send_a.at[h, way], dst_ref=recv_a.at[h, way], send_sem=rs_send,
            recv_sem=a_recv.at[h, way], device_id={"cp": d, "tp": t_up if way == 0 else t_dn},
        )

    def b_copy(h, way, piece):
        return pltpu.make_async_remote_copy(
            src_ref=send_b.at[h, way, piece], dst_ref=recv_b.at[h, way, piece],
            send_sem=rs_send, recv_sem=b_recv.at[h],
            device_id={"cp": d, "tp": t_up if way == 0 else t_dn},
        )

    summed = [slice(0, 256), slice(256, 512)]
    plain = [slice(256, 512), slice(0, 256)]

    def scatter_first(h):
        at_copy(h).wait_recv()
        far = project(h, 3)
        for way in range(2):
            send_a[h, way] = far[:, summed[way]].astype(BF16)
            a_copy(h, way).start()
        for way in range(2):
            near = project(h, 1 + way)
            accq[of(h), way * 256 : (way + 1) * 256] = near[:, summed[way]]
            send_b[h, way, 1] = near[:, plain[way]].astype(BF16)
            b_copy(h, way, 1).start()

    def scatter_second(h):
        for way in range(2):
            a_copy(h, way).wait_recv()
            own = accq[of(h), way * 256 : (way + 1) * 256]
            send_b[h, way, 0] = (own + recv_a[h, way].astype(F32)).astype(BF16)
            b_copy(h, way, 0).start()

    def scatter_mine(h):
        accq[of(h), :] = project(h, 0)

    def scatter_last(h):
        rs = of(h)
        pltpu.make_async_copy(recv_b.at[h], recv_b.at[h], b_recv.at[h]).wait()
        out[rs, 0:256] = (
            accq[rs, 0:256] + recv_b[h, 0, 0].astype(F32) + recv_b[h, 1, 1].astype(F32)
        ).astype(BF16)
        out[rs, 256:512] = (
            accq[rs, 256:512] + recv_b[h, 0, 1].astype(F32) + recv_b[h, 1, 0].astype(F32)
        ).astype(BF16)

    def weights_here():
        pltpu.make_async_copy(wo_own, wo_own, wo_sem).wait()
        pltpu.make_async_copy(wo_sib, wo_sib, wos_recv).wait()

    def main_step(i, carry):
        e = entry(i)
        p = lax.rem(e, 64)
        kind = lax.rem(lax.div(e, 1024), 4)
        job = lax.rem(lax.div(e, 4096), 4)
        s1, s2 = lax.rem(lax.div(e, 16384), 32), lax.div(e, 524288)

        @pl.when(kind == 1)
        def _():
            kv_wait(p)

        @pl.when(kind == 2)
        def _():
            kv_wait(p)
            kv_wait(p + 1)

        pass_on(e, lambda c: c.start())

        @pl.when(job > 0)
        def _():
            attend(job - 1, s1, s2)

        @pl.when(i == at_whole)
        def _():
            finish(early)
            at_copy(early).start()

        @pl.when(i == at_first)
        def _():
            weights_here()
            scatter_first(early)

        @pl.when(i == at_second)
        def _():
            scatter_second(early)
            scatter_mine(early)

        return carry

    lax.fori_loop(at_query, n_entries, main_step, 0)
    finish(late)
    at_copy(late).start()

    @pl.when(at_first >= n_entries)
    def _():
        weights_here()
        scatter_first(early)

    scatter_first(late)

    @pl.when(at_second >= n_entries)
    def _():
        scatter_second(early)
        scatter_mine(early)

    scatter_second(late)
    scatter_mine(late)
    scatter_last(early)
    scatter_last(late)
    for count in sorted(set(SENDS)):
        @pl.when(n_sends == count)
        def _():
            pltpu.make_async_copy(kvbuf.at[0:count], kvbuf.at[0:count], kv_send).wait()
    pltpu.make_async_copy(wo_sib, wo_sib, wos_send).wait()
    pltpu.make_async_copy(wo_own, wo_own, rs_send).wait()


def step(tokens, gain, w_query, w_key, w_value, w_out, doc_ids):
    rope_in, rope_out = rope_tables()
    any_space = pl.BlockSpec(memory_space=pl.ANY)
    rows = 2 * STRETCH
    dma = pltpu.SemaphoreType.DMA
    return pl.pallas_call(
        kernel,
        out_shape=pltpu.VMEM((rows, 512), BF16),
        in_specs=[any_space] * 9,
        out_specs=pl.BlockSpec(memory_space=pltpu.VMEM),
        scratch_shapes=[
            pltpu.VMEM((rows, D), BF16),
            pltpu.VMEM((rows, D), BF16),
            pltpu.VMEM((D, 2 * HD), BF16),
            pltpu.VMEM((D, GROUP * HD), BF16),
            pltpu.VMEM((4, 512, 512), BF16),
            pltpu.VMEM((4, 512, 512), BF16),
            pltpu.VMEM((rows, 2 * HD), F32),
            pltpu.VMEM((rows, GROUP * HD), F32),
            pltpu.VMEM((rows, HD), F32),
            pltpu.VMEM((4 * N_CP, STRETCH, HD), BF16),
            pltpu.VMEM((2, GROUP * STRETCH, HD), BF16),
            pltpu.VMEM((2, 8, STRETCH), F32),
            pltpu.VMEM((2, GROUP, HD + ONES, STRETCH), F32),
            pltpu.VMEM((2, STRETCH, 512), BF16),
            pltpu.VMEM((2, STRETCH, 512), BF16),
            pltpu.VMEM((2, 2, STRETCH, 256), BF16),
            pltpu.VMEM((2, 2, STRETCH, 256), BF16),
            pltpu.VMEM((2, 2, 2, STRETCH, 256), BF16),
            pltpu.VMEM((2, 2, 2, STRETCH, 256), BF16),
            pltpu.VMEM((8, STRETCH), jnp.int32),
            pltpu.VMEM((D,), BF16),
            pltpu.VMEM((1, D), F32),
            pltpu.VMEM((2 * N_CP * STRETCH,), jnp.int32),
            pltpu.VMEM((2, STRETCH, HD), F32),
            pltpu.VMEM((2, 2 * N_CP, HD), F32),
            dma((7,)),
            dma((N_CHUNK,)),
            dma,
            dma,
            dma,
            dma,
            dma((4 * REACH,)),
            dma,
            dma((2,)),
            dma((2, 2)),
            dma((2,)),
        ],
        compiler_params=pltpu.CompilerParams(
            collective_id=0, has_side_effects=True, vmem_limit_bytes=60 * 1024 * 1024
        ),
        name="block",
    )(
        tokens, gain, w_query, w_key, w_value, w_out,
        doc_ids, jnp.asarray(rope_in), jnp.asarray(rope_out),
    )


def solution(mesh):
    in_specs = (P("cp", None), P(), P(None, "tp"), P(None, "tp"), P(None, "tp"), P("tp", None), P())
    return jax.shard_map(step, mesh=mesh, in_specs=in_specs, out_specs=P("cp", "tp"), check_vma=False)
```

```python
import math

import jax
import jax.numpy as jnp
import numpy as np
from jax import lax
from jax.experimental import pallas as pl
from jax.experimental.pallas import tpu as pltpu
from jax.sharding import PartitionSpec as P

D = 4096
HEADS = 32
HD = 128
GROUP = 4
STRETCH = 256
N_CP = 16
REACH = 9
CHUNK = 512
N_CHUNK = D // CHUNK
NEG = -1e30
EPS = 1e-05
THETA = 500000.0
QSCALE = math.log2(math.e) / math.sqrt(HD)
ONES = 16
F32 = jnp.float32
BF16 = jnp.bfloat16

TABLE = [
    [449, 448, 1271, 1081, 16258109, 1270, 1080, 14672956, 121, 1198, 1076, 1072, 16195694, 1073, 113, 180, 1071, 12461109, 1331, 13542450, 2092, 15575098],
    [322, 323, 189, 188, 1344, 1204, 1083, 116, 187, 1025, 1077, 21562, 117, 14131381, 1075, 1202, 1143, 1078, 13591608, 1081, 2092, 186, 118, 15131952, 2090, 11379761, 12462126],
    [324, 325, 187, 186, 1346, 1203, 1080, 115, 184, 1027, 1074, 1081, 561411, 13590595, 1280, 1200, 1067, 114, 1076, 1025, 1066, 171, 15208554, 1077, 1073, 11477109, 1132, 13018167, 2088, 1069, 11871286, 12511278],
    [262, 263, 249, 248, 1284, 1024, 1264, 256, 1025, 1029, 1073, 53377, 261, 13050033, 1026, 1064, 258, 168, 1139, 2102, 10937385, 1283, 561321, 1070, 1074, 174, 2090, 1071, 11429940, 14017575, 2092, 10331174],
    [456, 457, 567, 566, 1473, 1582, 1072, 174, 110, 1071, 1280, 1585, 71732, 111, 559, 12509359, 1282, 1030, 1127, 14033063, 1581, 1068, 1065, 70, 262, 173, 1027, 1031, 1062, 1593900, 1188, 1284, 10331240, 259, 14193669, 11348010, 1061, 13412402],
    [331, 330, 692, 693, 1410, 1097, 1580, 1075, 172, 108, 1027, 1069, 1288, 611890, 131, 259, 557, 11968621, 1028, 1025, 1188, 1280, 69697, 1070, 1578, 1195, 110, 265, 1071, 1029, 11428901, 559, 1127, 165, 9822469, 1030, 100, 178, 262, 1031, 1611810, 263, 10774568, 1062, 12904496],
    [332, 333, 691, 690, 1412, 1099, 1579, 1073, 171, 107, 1029, 1290, 1066, 1072, 1151530, 133, 74, 11428107, 1030, 1186, 1026, 261, 106, 2056, 1580, 1027, 2184233, 1415, 1581, 1064, 1593452, 1059, 2048, 262, 177, 13111395, 1583, 1125, 1070, 11936002, 2080, 1060, 9249027, 8775718, 10267648],
    [270, 271, 752, 753, 1478, 1032, 1576, 1036, 136, 268, 1031, 1037, 1129, 1033, 1692201, 135, 71, 2199821, 1028, 1035, 1184, 68, 263, 1070, 1579, 2048, 10888222, 1349, 1711, 1053706, 1063, 264, 1066, 11395623, 1069, 557, 267, 2050, 611494, 1068, 11854374, 1055, 2082, 1057, 9168932, 9710592],
    [558, 464, 465, 559, 1767, 1064, 1288, 1069, 104, 557, 1062, 1161, 1065, 1068, 10346761, 102, 166, 11870758, 1060, 1376, 1025, 164, 552, 1067, 1061, 1039, 2233344, 1249, 2078, 1578, 8691983, 11265356, 1030, 65, 262, 1038, 2082, 7628828, 78, 1287, 3675146, 2050, 2052, 578571, 2659341, 12164096],
    [339, 338, 685, 684, 1764, 1067, 1291, 1041, 171, 81, 1061, 1578, 1040, 9807114, 101, 170, 549, 4346128, 1058, 1127, 162, 1577, 1288, 2076, 7693352, 1699, 1126, 2050, 9249819, 138, 550, 610384, 1033, 1050, 2080, 2078, 73, 7135371, 72, 8136708, 2060, 1120256, 2054, 104462, 3726336],
    [341, 340, 683, 682, 1762, 1065, 1298, 1037, 169, 553, 1059, 1107, 1036, 1064, 9265421, 99, 163, 552, 4886796, 1060, 1115, 1156, 1056, 547, 1297, 1050, 1034, 7152655, 1637, 1057, 1182, 1035, 8691983, 1029, 2076, 141, 545, 2723914, 2086, 143, 10199108, 2072, 8070175, 2054, 1040, 1610766, 3807240, 595970],
    [279, 278, 744, 745, 1760, 1296, 1038, 6104084, 1054, 1041, 1301, 1231, 4379166, 158, 271, 3838046, 1570, 1053, 1030, 1063, 270, 157, 1100, 1049, 268, 153, 78, 1574, 1052, 1037, 7660579, 1183, 1095, 8151583, 1048, 142, 2084, 1569, 9643077, 2074, 7086157, 2056, 1677330, 2058, 4789252, 1137664],
    [551, 550, 216, 217, 1631, 1040, 6612004, 1057, 1573, 4396241, 545, 97, 1053, 1047, 1032, 541, 87, 1170, 1046, 6071305, 86, 1054, 7595548, 94, 1056, 7088154, 73, 2282517, 1039, 79, 1044, 9087010, 1038, 3838982, 2060, 1031, 1676307, 2775050],
    [676, 677, 91, 90, 1693, 1107, 7119897, 1052, 1048, 1170, 540, 6529113, 156, 88, 6509083, 1055, 1035, 543, 154, 75, 1034, 2774033, 538, 1187, 2080, 1040, 8544330, 1058, 162, 139, 5531668, 5380118, 1054, 8052883, 2060, 2056, 3330186, 3741710],
    [546, 547, 221, 220, 1627, 1184, 7627797, 1057, 1626, 7087252, 545, 163, 7049300, 1043, 1042, 162, 83, 4891164, 1049, 2070, 1037, 149, 4886605, 1560, 1036, 6480013, 2078, 6475916, 4450320, 2058, 4297743, 1166, 3759104],
    [672, 542, 95, 225, 1565, 1239, 8135704, 1052, 1561, 6530262, 540, 94, 7590047, 1040, 1051, 543, 158, 5967963, 1045, 1050, 1041, 536, 85, 7004304, 1044, 1039, 538, 5382228, 1166, 1043, 1042, 78, 4842002, 1037, 1036, 4411469, 3841024, 3300352],
]
CUT = 8
MARKS = [
    [2, 4, 4, 4, 4, 4, 4, 4, 4, 4, 4, 4, 4, 4, 4, 4],
    [4, 11, 22, 22, 34, 40, 35, 38, 37, 39, 42, 40, 31, 33, 28, 32],
    [8, 14, 25, 25, 36, 42, 39, 41, 40, 41, 45, 42, 33, 36, 31, 36],
    [18, 25, 200, 200, 200, 200, 200, 200, 200, 200, 200, 200, 200, 200, 200, 200],
    [22, 27, 32, 32, 38, 45, 45, 46, 46, 45, 48, 46, 38, 38, 33, 38],
]
ENTRIES = max(len(row) for row in TABLE)
SENDS = [sum((e // (64 << k)) % 2 for e in row for k in range(4)) for row in TABLE]


def rope_tables():
    half = HD // 2
    freqs = THETA ** (-2.0 * np.arange(half) / HD)
    inner = np.arange(STRETCH)[:, None] * freqs[None, :]
    outer = (np.arange(2 * N_CP) * STRETCH)[:, None] * freqs[None, :]

    def both(angles):
        c, s = np.cos(angles), np.sin(angles)
        return np.stack([np.concatenate([c, c], 1), np.concatenate([s, s], 1)])

    return both(inner).astype(np.float32), both(outer).astype(np.float32)


def kernel(
    tokens, gain, wq, wk, wv, wo, docs, rope_in, rope_out, out,
    x, xg, wkv, wqv, wo_own, wo_sib, acckv, accq, ssq, kvbuf, qs,
    m_ref, acc_ref, attn_own, attn_sib, send_a, recv_a, send_b, recv_b, qstart,
    gain_in, gain_row, doc_in, r_in, r_out,
    in_sems, x_sems, wo_sem, wos_send, wos_recv, kv_send, kv_recv,
    rs_send, at_recv, a_recv, b_recv,
):
    d = lax.axis_index("cp")
    t = lax.axis_index("tp")
    z, core = t // 2, t % 2
    sib = t + 1 - 2 * core
    t_up = lax.rem(z + 1, 4) * 2 + core
    t_dn = lax.rem(z + 3, 4) * 2 + core
    zs = [z, lax.rem(z + 1, 4), lax.rem(z + 3, 4), lax.rem(z + 2, 4)]
    cl, cu = d, 2 * N_CP - 1 - d
    early = jnp.where(d < CUT, 0, 1)
    late = 1 - early

    def of(h):
        return pl.ds(pl.multiple_of(h * STRETCH, STRETCH), STRETCH)

    px, py = lax.rem(d, 4), lax.div(d, 4)
    beside = [
        py * 4 + lax.rem(px + 1, 4),
        py * 4 + lax.rem(px + 3, 4),
        lax.rem(py + 1, 4) * 4 + px,
        lax.rem(py + 3, 4) * 4 + px,
    ]

    def x_copy(i):
        cols = pl.ds(i * CHUNK, CHUNK)
        return pltpu.make_async_copy(tokens.at[:, cols], x.at[:, cols], x_sems.at[i])

    first_copies = [
        pltpu.make_async_copy(docs, doc_in, in_sems.at[0]),
        pltpu.make_async_copy(gain, gain_in, in_sems.at[1]),
        pltpu.make_async_copy(wk, wkv.at[:, 0:HD], in_sems.at[2]),
        pltpu.make_async_copy(wv, wkv.at[:, HD : 2 * HD], in_sems.at[3]),
    ]
    rope_copies = [
        pltpu.make_async_copy(rope_in, r_in, in_sems.at[4]),
        pltpu.make_async_copy(rope_out, r_out, in_sems.at[5]),
    ]
    wq_copy = pltpu.make_async_copy(wq, wqv, in_sems.at[6])

    def wo_copy(i):
        cols = pl.ds(pl.multiple_of((2 * i + core) * 512, 512), 512)
        return pltpu.make_async_copy(wo.at[:, cols], wo_own.at[i], wo_sem)

    first_copies[1].start()
    for i in range(N_CHUNK):
        x_copy(i).start()
    for c in (first_copies[2], first_copies[3], first_copies[0]):
        c.start()
    for c in rope_copies:
        c.start()

    barrier = pltpu.get_barrier_semaphore()
    for e in beside:
        pl.semaphore_signal(barrier, 1, device_id={"cp": e, "tp": t})
    for other in (sib, t_up, t_dn):
        pl.semaphore_signal(barrier, 1, device_id={"cp": d, "tp": other})

    here = [(d == e).astype(jnp.int32) for e in range(N_CP)]

    def pick(values):
        total = jnp.int32(0)
        for e, v in enumerate(values):
            if v:
                total = total + here[e] * v
        return total

    words = [pick([row[i] if i < len(row) else 0 for row in TABLE]) for i in range(ENTRIES)]

    def chosen(values, i):
        while len(values) > 1:
            low = lax.rem(i, 2) == 0
            values = [
                jnp.where(low, values[k], values[k + 1]) if k + 1 < len(values) else values[k]
                for k in range(0, len(values), 2)
            ]
            i = lax.div(i, 2)
        return values[0]

    def entries(group):
        return [chosen(words[k::8], group) for k in range(8)]

    at_query, at_whole, at_first, at_second, n_entries = [pick(m) for m in MARKS]
    n_sends = pick(SENDS)

    ssq[...] = jnp.zeros_like(ssq)
    first_copies[1].wait()
    for i in range(N_CHUNK):
        cols = slice(i * CHUNK, (i + 1) * CHUNK)
        gain_row[:, cols] = gain_in[cols].astype(F32).reshape(1, CHUNK)

    def scale_chunk(i):
        x_copy(i).wait()
        cols = pl.ds(pl.multiple_of(i * CHUNK, CHUNK), CHUNK)
        xf = x[:, cols].astype(F32)
        sq = xf * xf
        ssq[...] += sq[:, 0:128] + sq[:, 128:256] + sq[:, 256:384] + sq[:, 384:512]
        xg[:, cols] = (xf * gain_row[:, cols]).astype(BF16)

    def scale_step(i, carry):
        @pl.when(i == N_CHUNK // 2)
        def _():
            wq_copy.start()

        scale_chunk(i)
        return carry

    lax.fori_loop(0, N_CHUNK, scale_step, 0)
    for c in first_copies[2:]:
        c.wait()
    acckv[...] = jnp.dot(xg[...], wkv[...], preferred_element_type=F32)
    for i in range(4):
        wo_copy(i).start()
    for c in rope_copies:
        c.wait()
    mean = jnp.sum(ssq[...], axis=1, keepdims=True) * (1.0 / D)
    factor = lax.rsqrt(mean + EPS)
    ssq[...] = jnp.broadcast_to(factor, (2 * STRETCH, HD))

    sign = jnp.where(lax.broadcasted_iota(jnp.int32, (1, HD), 1) < HD // 2, -1.0, 1.0)

    def rope(h):
        c = cl if h == 0 else cu
        co, so = r_out[0, pl.ds(c, 1), :], r_out[1, pl.ds(c, 1), :]
        ci, si = r_in[0], r_in[1]
        return ci * co - si * so, (ci * so + si * co) * sign

    for h, c in ((0, cl), (1, cu)):
        rs = slice(h * STRETCH, (h + 1) * STRETCH)
        cosine, sine = rope(h)
        kf = acckv[rs, 0:HD] * ssq[rs, :]
        kvbuf[2 * c] = (kf * cosine + pltpu.roll(kf, HD // 2, 1) * sine).astype(BF16)
        vf = acckv[rs, HD : 2 * HD] * ssq[rs, :]
        kvbuf[2 * c + 1, 0:HD, :] = vf[0:HD, :].T.astype(BF16)
        kvbuf[2 * c + 1, HD : 2 * HD, :] = vf[HD : 2 * HD, :].T.astype(BF16)

    pl.semaphore_wait(barrier, 7)

    def kv_copy(p, way):
        return pltpu.make_async_remote_copy(
            src_ref=kvbuf.at[p], dst_ref=kvbuf.at[p], send_sem=kv_send,
            recv_sem=kv_recv.at[p], device_id={"cp": beside[way], "tp": t},
        )

    def kv_wait(p):
        pltpu.make_async_remote_copy(
            src_ref=kvbuf.at[p], dst_ref=kvbuf.at[p], send_sem=kv_send,
            recv_sem=kv_recv.at[p], device_id={"cp": beside[0], "tp": t},
        ).wait_recv()

    def pass_on(e, act):
        p, ways = lax.rem(e, 64), lax.rem(lax.div(e, 64), 16)

        @pl.when(ways > 0)
        def _():
            for way in range(4):
                @pl.when(lax.rem(lax.div(ways, 2**way), 2) == 1)
                def _():
                    act(kv_copy(p, way))

    def send_only(i, carry):
        pass_on(chosen(words[:8], i), lambda c: c.start())
        return carry

    lax.fori_loop(0, at_query, send_only, 0)

    def wos_copy(i):
        cols = pl.ds(pl.multiple_of((2 * i + 1 - core) * 512, 512), 512)
        return pltpu.make_async_remote_copy(
            src_ref=wo.at[:, cols], dst_ref=wo_sib.at[i], send_sem=wos_send,
            recv_sem=wos_recv, device_id={"cp": d, "tp": sib},
        )

    for i in range(4):
        wos_copy(i).start()

    first_copies[0].wait()
    table = doc_in[...].reshape(64, 128)
    rows = [
        doc_in[pl.ds(pl.multiple_of(c * STRETCH, STRETCH), STRETCH)].reshape(1, STRETCH) for c in (cl, cu)
    ]
    starts = [jnp.zeros((1, STRETCH), F32) for _ in rows]
    for v in range(1, 16):
        below = jnp.where(table < v, 1.0, 0.0)
        count = jnp.sum(jnp.sum(below, axis=0, keepdims=True), axis=1, keepdims=True)
        starts = [jnp.where(r >= v, count, s) for r, s in zip(rows, starts)]
    qstart[0:1, :] = starts[0].astype(jnp.int32)
    qstart[1:2, :] = starts[1].astype(jnp.int32)
    m_ref[...] = jnp.full_like(m_ref, NEG)
    acc_ref[...] = jnp.zeros_like(acc_ref)

    wq_copy.wait()

    def q_step(i, carry):
        cols = pl.ds(pl.multiple_of(i * 256, 256), 256)
        accq[:, cols] = jnp.dot(xg[...], wqv[:, cols], preferred_element_type=F32)
        return carry

    lax.fori_loop(0, 2, q_step, 0)
    for h in range(2):
        rs = slice(h * STRETCH, (h + 1) * STRETCH)
        cosine, sine = rope(h)
        scale = ssq[rs, :] * QSCALE
        for g in range(GROUP):
            qf = accq[rs, g * HD : (g + 1) * HD] * scale
            qs[h, g * STRETCH : (g + 1) * STRETCH, :] = (
                qf * cosine + pltpu.roll(qf, HD // 2, 1) * sine
            ).astype(BF16)

    key_row = lax.broadcasted_iota(jnp.int32, (STRETCH, STRETCH), 0)
    query_col = lax.broadcasted_iota(jnp.int32, (STRETCH, STRETCH), 1)
    ones = jnp.ones((ONES, 2 * STRETCH), BF16)

    def attend(h, s1, s2):
        c = jnp.where(h == 0, cl, cu)
        keys = jnp.concatenate([kvbuf[2 * s1], kvbuf[2 * s2]], axis=0)
        vt = jnp.concatenate([kvbuf[2 * s + 1, r : r + HD, :] for s in (s1, s2) for r in (0, HD)], axis=1)
        vt = jnp.concatenate([vt, ones], axis=0)
        begin = qstart[pl.ds(h, 1), :]
        mask = jnp.concatenate(
            [
                (key_row >= begin - s * STRETCH) & (key_row <= query_col + (c - s) * STRETCH)
                for s in (s1, s2)
            ],
            axis=0,
        )
        scores = [
            lax.dot_general(
                keys, qs[h, g * STRETCH : (g + 1) * STRETCH, :], (((1,), (1,)), ((), ())),
                preferred_element_type=F32,
            )
            for g in range(GROUP)
        ]
        before = [m_ref[h, g : g + 1, :] for g in range(GROUP)]
        held = [acc_ref[h, g] for g in range(GROUP)]
        tops, added = [], []
        for g in range(GROUP):
            sc = jnp.where(mask, scores[g], NEG)
            top = jnp.maximum(jnp.max(sc, axis=0, keepdims=True), before[g])
            weights = jnp.exp2(sc - top).astype(BF16)
            tops.append(top)
            added.append(jnp.dot(vt, weights, preferred_element_type=F32))
        for g in range(GROUP):
            acc_ref[h, g] = held[g] * jnp.exp2(before[g] - tops[g]) + added[g]
            m_ref[h, g : g + 1, :] = tops[g]

    def finish(h):
        for g in range(GROUP):
            o = acc_ref[h, g, 0:HD, :] / acc_ref[h, g, HD : HD + 1, :]
            attn_own[h, :, g * HD : (g + 1) * HD] = o.T.astype(BF16)

    def at_copy(h):
        return pltpu.make_async_remote_copy(
            src_ref=attn_own.at[h], dst_ref=attn_sib.at[h], send_sem=rs_send,
            recv_sem=at_recv.at[h], device_id={"cp": d, "tp": sib},
        )

    def project(h, i):
        zz = zs[i]
        return jnp.dot(attn_own[h], wo_own[zz], preferred_element_type=F32) + jnp.dot(
            attn_sib[h], wo_sib[zz], preferred_element_type=F32
        )

    def a_copy(h, way):
        return pltpu.make_async_remote_copy(
            src_ref=send_a.at[h, way], dst_ref=recv_a.at[h, way], send_sem=rs_send,
            recv_sem=a_recv.at[h, way], device_id={"cp": d, "tp": t_up if way == 0 else t_dn},
        )

    def b_copy(h, way, piece):
        return pltpu.make_async_remote_copy(
            src_ref=send_b.at[h, way, piece], dst_ref=recv_b.at[h, way, piece],
            send_sem=rs_send, recv_sem=b_recv.at[h],
            device_id={"cp": d, "tp": t_up if way == 0 else t_dn},
        )

    summed = [slice(0, 256), slice(256, 512)]
    plain = [slice(256, 512), slice(0, 256)]

    def scatter_first(h):
        at_copy(h).wait_recv()
        far = project(h, 3)
        for way in range(2):
            send_a[h, way] = far[:, summed[way]].astype(BF16)
            a_copy(h, way).start()
        for way in range(2):
            near = project(h, 1 + way)
            accq[of(h), way * 256 : (way + 1) * 256] = near[:, summed[way]]
            send_b[h, way, 1] = near[:, plain[way]].astype(BF16)
            b_copy(h, way, 1).start()

    def scatter_second(h):
        for way in range(2):
            a_copy(h, way).wait_recv()
            own = accq[of(h), way * 256 : (way + 1) * 256]
            send_b[h, way, 0] = (own + recv_a[h, way].astype(F32)).astype(BF16)
            b_copy(h, way, 0).start()

    def scatter_mine(h):
        accq[of(h), :] = project(h, 0)

    def scatter_last(h):
        rs = of(h)
        pltpu.make_async_copy(recv_b.at[h], recv_b.at[h], b_recv.at[h]).wait()
        out[rs, 0:256] = (
            accq[rs, 0:256] + recv_b[h, 0, 0].astype(F32) + recv_b[h, 1, 1].astype(F32)
        ).astype(BF16)
        out[rs, 256:512] = (
            accq[rs, 256:512] + recv_b[h, 0, 1].astype(F32) + recv_b[h, 1, 0].astype(F32)
        ).astype(BF16)

    def weights_here():
        pltpu.make_async_copy(wo_own, wo_own, wo_sem).wait()
        pltpu.make_async_copy(wo_sib, wo_sib, wos_recv).wait()

    def main_step(i, near):
        e = chosen(list(near), lax.rem(i, 8))
        p = lax.rem(e, 64)
        kind = lax.rem(lax.div(e, 1024), 4)
        job = lax.rem(lax.div(e, 4096), 4)
        s1, s2 = lax.rem(lax.div(e, 16384), 32), lax.div(e, 524288)

        @pl.when(kind == 1)
        def _():
            kv_wait(p)

        @pl.when(kind == 2)
        def _():
            kv_wait(p)
            kv_wait(p + 1)

        pass_on(e, lambda c: c.start())

        @pl.when(job > 0)
        def _():
            attend(job - 1, s1, s2)

        @pl.when(i == at_whole)
        def _():
            finish(early)
            at_copy(early).start()

        @pl.when(i == at_first)
        def _():
            weights_here()
            scatter_first(early)

        @pl.when(i == at_second)
        def _():
            scatter_second(early)
            scatter_mine(early)

        return near

    def group_step(group, carry):
        low = jnp.maximum(at_query, group * 8)
        high = jnp.minimum(n_entries, group * 8 + 8)
        lax.fori_loop(low, high, main_step, tuple(entries(group)))
        return carry

    lax.fori_loop(lax.div(at_query, 8), lax.div(n_entries + 7, 8), group_step, 0)
    finish(late)
    at_copy(late).start()

    @pl.when(at_first >= n_entries)
    def _():
        weights_here()
        scatter_first(early)

    scatter_first(late)

    @pl.when(at_second >= n_entries)
    def _():
        scatter_second(early)
        scatter_mine(early)

    scatter_second(late)
    scatter_mine(late)
    scatter_last(early)
    scatter_last(late)
    for count in sorted(set(SENDS)):
        @pl.when(n_sends == count)
        def _():
            pltpu.make_async_copy(kvbuf.at[0:count], kvbuf.at[0:count], kv_send).wait()
    pltpu.make_async_copy(wo_sib, wo_sib, wos_send).wait()
    pltpu.make_async_copy(wo_own, wo_own, rs_send).wait()


def step(tokens, gain, w_query, w_key, w_value, w_out, doc_ids):
    rope_in, rope_out = rope_tables()
    any_space = pl.BlockSpec(memory_space=pl.ANY)
    rows = 2 * STRETCH
    dma = pltpu.SemaphoreType.DMA
    return pl.pallas_call(
        kernel,
        out_shape=pltpu.VMEM((rows, 512), BF16),
        in_specs=[any_space] * 9,
        out_specs=pl.BlockSpec(memory_space=pltpu.VMEM),
        scratch_shapes=[
            pltpu.VMEM((rows, D), BF16),
            pltpu.VMEM((rows, D), BF16),
            pltpu.VMEM((D, 2 * HD), BF16),
            pltpu.VMEM((D, GROUP * HD), BF16),
            pltpu.VMEM((4, 512, 512), BF16),
            pltpu.VMEM((4, 512, 512), BF16),
            pltpu.VMEM((rows, 2 * HD), F32),
            pltpu.VMEM((rows, GROUP * HD), F32),
            pltpu.VMEM((rows, HD), F32),
            pltpu.VMEM((4 * N_CP, STRETCH, HD), BF16),
            pltpu.VMEM((2, GROUP * STRETCH, HD), BF16),
            pltpu.VMEM((2, 8, STRETCH), F32),
            pltpu.VMEM((2, GROUP, HD + ONES, STRETCH), F32),
            pltpu.VMEM((2, STRETCH, 512), BF16),
            pltpu.VMEM((2, STRETCH, 512), BF16),
            pltpu.VMEM((2, 2, STRETCH, 256), BF16),
            pltpu.VMEM((2, 2, STRETCH, 256), BF16),
            pltpu.VMEM((2, 2, 2, STRETCH, 256), BF16),
            pltpu.VMEM((2, 2, 2, STRETCH, 256), BF16),
            pltpu.VMEM((8, STRETCH), jnp.int32),
            pltpu.VMEM((D,), BF16),
            pltpu.VMEM((1, D), F32),
            pltpu.VMEM((2 * N_CP * STRETCH,), jnp.int32),
            pltpu.VMEM((2, STRETCH, HD), F32),
            pltpu.VMEM((2, 2 * N_CP, HD), F32),
            dma((7,)),
            dma((N_CHUNK,)),
            dma,
            dma,
            dma,
            dma,
            dma((4 * N_CP,)),
            dma,
            dma((2,)),
            dma((2, 2)),
            dma((2,)),
        ],
        compiler_params=pltpu.CompilerParams(
            collective_id=0, has_side_effects=True, vmem_limit_bytes=60 * 1024 * 1024
        ),
        name="block",
    )(
        tokens, gain, w_query, w_key, w_value, w_out,
        doc_ids, jnp.asarray(rope_in), jnp.asarray(rope_out),
    )


def solution(mesh):
    in_specs = (P("cp", None), P(), P(None, "tp"), P(None, "tp"), P(None, "tp"), P("tp", None), P())
    return jax.shard_map(step, mesh=mesh, in_specs=in_specs, out_specs=P("cp", "tp"), check_vma=False)
```

```python
import math

import jax
import jax.numpy as jnp
import numpy as np
from jax import lax
from jax.experimental import pallas as pl
from jax.experimental.pallas import tpu as pltpu
from jax.sharding import PartitionSpec as P

D = 4096
HEADS = 32
HD = 128
GROUP = 4
STRETCH = 256
N_CP = 16
REACH = 9
CHUNK = 512
N_CHUNK = D // CHUNK
NEG = -1e30
EPS = 1e-05
THETA = 500000.0
QSCALE = math.log2(math.e) / math.sqrt(HD)
ONES = 16
F32 = jnp.float32
BF16 = jnp.bfloat16

TABLE = [
    [448, 449, 16260096, 1270, 1079, 2104, 14673980, 1262, 1073, 16196660, 183, 1136, 12461103, 111, 1077, 175, 181, 119, 1196, 11969581, 2098, 15624250],
    [323, 322, 188, 189, 1345, 1204, 1082, 116, 186, 1077, 1083, 21504, 117, 14131381, 1068, 1075, 1261, 12018745, 1074, 178, 108, 1070, 1080, 15098043, 2096, 1135, 12462122, 14510134],
    [324, 325, 186, 187, 1347, 1203, 1081, 115, 185, 1026, 1074, 562232, 66, 13590706, 1281, 1024, 1066, 106, 15208632, 1073, 1067, 1140, 11477169, 1077, 1072, 13017202, 1069, 2088, 109, 11871276, 2102, 12511278],
    [262, 263, 249, 248, 1284, 1152, 1137, 177, 1029, 1281, 1072, 1101936, 261, 13050032, 1027, 1064, 259, 168, 1078, 1139, 182, 1065, 529410, 1198, 1207, 1071, 2090, 14492724, 11398144, 1077, 13542450, 2092, 10332198],
    [456, 457, 566, 567, 1472, 1582, 1072, 110, 174, 1025, 1071, 1073, 2100, 559, 69889, 111, 12509359, 1286, 1026, 70, 14033026, 1580, 1064, 1065, 172, 105, 1283, 1031, 2086, 1593415, 263, 1028, 1197, 10297457, 260, 1061, 165, 9806884, 14193925, 2090, 13461554],
    [331, 330, 692, 693, 1474, 1032, 1580, 1074, 72, 172, 1027, 1069, 1289, 1075, 610861, 131, 109, 11968771, 1028, 1024, 1061, 1025, 132, 64, 69896, 1578, 1070, 1067, 165, 108, 11428100, 1029, 1060, 1071, 111, 261, 178, 12362283, 1062, 1030, 102, 257, 179, 2082, 1611015, 1063, 2088, 10250288, 12921856],
    [333, 332, 691, 690, 1412, 1099, 1578, 1072, 170, 267, 1029, 1034, 1131, 1073, 1151531, 133, 74, 11428101, 1030, 1026, 1058, 1027, 262, 176, 610410, 1577, 2056, 259, 162, 98, 1031, 1643560, 2048, 263, 168, 13112419, 2080, 2092, 10887426, 2094, 2084, 8676390, 12430336, 10265639],
    [271, 270, 753, 752, 1478, 1033, 1037, 1576, 137, 269, 1031, 1036, 1129, 1032, 1692201, 135, 71, 2199815, 1028, 1035, 1185, 10887435, 1070, 1643, 2048, 260, 1184, 1029, 1071, 1034, 69, 174, 265, 1053727, 2050, 1066, 610565, 1574, 12330018, 1191, 2092, 1059, 10314279, 2084, 9282590, 8170496],
    [558, 559, 465, 464, 1766, 1064, 1289, 1068, 104, 552, 1063, 1069, 1160, 1065, 10346760, 103, 167, 10854951, 1061, 1060, 1121, 1024, 164, 2232877, 1025, 1359, 1067, 1056, 165, 8692260, 1055, 1066, 1054, 95, 8217130, 1286, 2082, 64, 1034, 266, 70, 3675150, 2050, 7628828, 1287, 1035, 1594381, 1036, 3233796, 12098560],
    [339, 684, 338, 685, 1765, 1067, 1291, 1040, 171, 555, 1060, 1066, 1098, 9807121, 100, 170, 266, 2773540, 1062, 1058, 1154, 102, 550, 9266211, 1289, 2088, 138, 80, 547, 1052, 1063, 1037, 1027, 269, 156, 103, 10297895, 1036, 1032, 2080, 268, 141, 659528, 1039, 1053, 73, 7610639, 2074, 2078, 8087556, 1038, 2201600, 3708934, 1580032],
    [683, 682, 341, 340, 1762, 1065, 1298, 1037, 169, 553, 1059, 1100, 1043, 1064, 9265421, 99, 268, 141, 3314216, 1061, 1052, 92, 140, 1053, 7676451, 1290, 1035, 2080, 157, 549, 2773074, 1050, 1060, 2052, 90, 9708068, 1166, 2078, 74, 1051, 7070736, 1039, 3708966, 2054, 6613016, 2050, 1041, 579592, 2235392],
    [744, 745, 278, 279, 6106112, 1761, 1295, 1044, 1056, 1038, 1045, 2064, 270, 160, 79, 3854880, 277, 1055, 95, 159, 4362783, 1058, 1062, 1054, 276, 98, 142, 8135206, 1037, 1036, 78, 269, 143, 1049, 1575, 2054, 9233443, 1099, 1572, 2076, 1675417, 1048, 1061, 76, 6529566, 2056, 7120922, 1120260, 1034, 4806674],
    [550, 551, 216, 217, 6614016, 1572, 1120, 1169, 1040, 1054, 1061, 544, 94, 4395152, 542, 80, 1055, 8168474, 1033, 95, 1571, 1053, 1032, 72, 541, 1057, 7611420, 1110, 1058, 6054935, 5837851, 5466132, 2062, 3838987, 1034, 2066, 4805645, 2054, 3200012],
    [677, 676, 90, 91, 539, 7119002, 1059, 1107, 1049, 547, 163, 1052, 1048, 4924434, 540, 88, 6508700, 1058, 1035, 162, 1568, 89, 7627805, 1566, 155, 75, 1044, 1034, 2064, 538, 2773140, 1057, 1055, 8134795, 1045, 2056, 5378194, 1037, 5941270, 5837964, 3774478],
    [546, 675, 220, 93, 162, 7627292, 1054, 1114, 1045, 541, 157, 1051, 1057, 5465108, 91, 538, 7049364, 1056, 1042, 542, 161, 82, 4989971, 1037, 1055, 83, 539, 4886677, 1048, 1047, 1036, 536, 151, 76, 6022166, 5870617, 1553, 2824202, 4400144, 1166, 3806223],
    [673, 608, 222, 543, 95, 8134816, 1053, 1046, 1048, 542, 159, 93, 1052, 1049, 6530071, 97, 151, 7590425, 150, 541, 5967958, 1041, 1050, 1039, 536, 87, 145, 1038, 3859472, 1051, 144, 1109, 6955547, 1042, 78, 4313230, 1044, 1555, 143, 4890707, 1037, 77, 5461004, 3300352],
]
CUT = 8
MARKS = [
    [2, 4, 4, 4, 4, 4, 4, 4, 4, 4, 4, 4, 4, 4, 4, 3],
    [2, 11, 18, 22, 38, 44, 35, 36, 43, 49, 44, 46, 31, 38, 38, 39],
    [6, 15, 22, 23, 200, 200, 38, 39, 46, 51, 47, 200, 33, 39, 200, 200],
    [17, 24, 29, 31, 200, 200, 200, 200, 200, 200, 200, 200, 200, 200, 200, 200],
    [22, 28, 32, 33, 41, 49, 44, 46, 50, 54, 49, 50, 39, 41, 41, 44],
]
ENTRIES = max(len(row) for row in TABLE)
SENDS = [sum((e // (64 << k)) % 2 for e in row for k in range(4)) for row in TABLE]


def rope_tables():
    half = HD // 2
    freqs = THETA ** (-2.0 * np.arange(half) / HD)
    inner = np.arange(STRETCH)[:, None] * freqs[None, :]
    outer = (np.arange(2 * N_CP) * STRETCH)[:, None] * freqs[None, :]

    def both(angles):
        c, s = np.cos(angles), np.sin(angles)
        return np.stack([np.concatenate([c, c], 1), np.concatenate([s, s], 1)])

    return both(inner).astype(np.float32), both(outer).astype(np.float32)


def kernel(
    tokens, gain, wq, wk, wv, wo, docs, rope_in, rope_out, out,
    x, xg, wkv, wqv, wo_own, wo_sib, acckv, accq, ssq, kvbuf, qs,
    m_ref, acc_ref, attn_own, attn_sib, send_a, recv_a, send_b, recv_b, qstart,
    gain_in, gain_row, doc_in, r_in, r_out, part,
    in_sems, x_sems, wo_sem, wos_send, wos_recv, kv_send, kv_recv,
    rs_send, at_recv, a_recv, b_recv,
):
    d = lax.axis_index("cp")
    t = lax.axis_index("tp")
    z, core = t // 2, t % 2
    sib = t + 1 - 2 * core
    t_up = lax.rem(z + 1, 4) * 2 + core
    t_dn = lax.rem(z + 3, 4) * 2 + core
    zs = [z, lax.rem(z + 1, 4), lax.rem(z + 3, 4), lax.rem(z + 2, 4)]
    cl, cu = d, 2 * N_CP - 1 - d
    early = jnp.where(d < CUT, 0, 1)
    late = 1 - early

    def of(h):
        return pl.ds(pl.multiple_of(h * STRETCH, STRETCH), STRETCH)

    px, py = lax.rem(d, 4), lax.div(d, 4)
    beside = [
        py * 4 + lax.rem(px + 1, 4),
        py * 4 + lax.rem(px + 3, 4),
        lax.rem(py + 1, 4) * 4 + px,
        lax.rem(py + 3, 4) * 4 + px,
    ]

    def x_copy(i):
        cols = pl.ds(i * CHUNK, CHUNK)
        return pltpu.make_async_copy(tokens.at[:, cols], x.at[:, cols], x_sems.at[i])

    first_copies = [
        pltpu.make_async_copy(docs, doc_in, in_sems.at[0]),
        pltpu.make_async_copy(gain, gain_in, in_sems.at[1]),
        pltpu.make_async_copy(wk, wkv.at[:, 0:HD], in_sems.at[2]),
        pltpu.make_async_copy(wv, wkv.at[:, HD : 2 * HD], in_sems.at[3]),
    ]
    rope_copies = [
        pltpu.make_async_copy(rope_in, r_in, in_sems.at[4]),
        pltpu.make_async_copy(rope_out, r_out, in_sems.at[5]),
    ]
    wq_copy = pltpu.make_async_copy(wq, wqv, in_sems.at[6])

    def wo_copy(i):
        cols = pl.ds(pl.multiple_of((2 * i + core) * 512, 512), 512)
        return pltpu.make_async_copy(wo.at[:, cols], wo_own.at[i], wo_sem)

    first_copies[1].start()
    for i in range(N_CHUNK):
        x_copy(i).start()
    for c in (first_copies[2], first_copies[3], first_copies[0]):
        c.start()
    for c in rope_copies:
        c.start()

    barrier = pltpu.get_barrier_semaphore()
    for e in beside:
        pl.semaphore_signal(barrier, 1, device_id={"cp": e, "tp": t})
    for other in (sib, t_up, t_dn):
        pl.semaphore_signal(barrier, 1, device_id={"cp": d, "tp": other})

    here = [(d == e).astype(jnp.int32) for e in range(N_CP)]

    def pick(values):
        total = jnp.int32(0)
        for e, v in enumerate(values):
            if v:
                total = total + here[e] * v
        return total

    words = [pick([row[i] if i < len(row) else 0 for row in TABLE]) for i in range(ENTRIES)]

    def chosen(values, i):
        while len(values) > 1:
            low = lax.rem(i, 2) == 0
            values = [
                jnp.where(low, values[k], values[k + 1]) if k + 1 < len(values) else values[k]
                for k in range(0, len(values), 2)
            ]
            i = lax.div(i, 2)
        return values[0]

    def entries(group):
        return [chosen(words[k::8], group) for k in range(8)]

    at_query, at_whole, at_first, at_second, n_entries = [pick(m) for m in MARKS]
    n_sends = pick(SENDS)

    ssq[...] = jnp.zeros_like(ssq)
    first_copies[1].wait()
    for i in range(N_CHUNK):
        cols = slice(i * CHUNK, (i + 1) * CHUNK)
        gain_row[:, cols] = gain_in[cols].astype(F32).reshape(1, CHUNK)

    def scale_chunk(i):
        x_copy(i).wait()
        cols = pl.ds(pl.multiple_of(i * CHUNK, CHUNK), CHUNK)
        xf = x[:, cols].astype(F32)
        sq = xf * xf
        ssq[...] += sq[:, 0:128] + sq[:, 128:256] + sq[:, 256:384] + sq[:, 384:512]
        xg[:, cols] = (xf * gain_row[:, cols]).astype(BF16)

    def scale_step(i, carry):
        @pl.when(i == N_CHUNK // 2)
        def _():
            wq_copy.start()

        scale_chunk(i)
        return carry

    lax.fori_loop(0, N_CHUNK, scale_step, 0)
    for c in first_copies[2:]:
        c.wait()
    acckv[...] = jnp.dot(xg[...], wkv[...], preferred_element_type=F32)
    for i in range(4):
        wo_copy(i).start()
    for c in rope_copies:
        c.wait()
    mean = jnp.sum(ssq[...], axis=1, keepdims=True) * (1.0 / D)
    factor = lax.rsqrt(mean + EPS)
    ssq[...] = jnp.broadcast_to(factor, (2 * STRETCH, HD))

    sign = jnp.where(lax.broadcasted_iota(jnp.int32, (1, HD), 1) < HD // 2, -1.0, 1.0)

    def rope(h):
        c = cl if h == 0 else cu
        co, so = r_out[0, pl.ds(c, 1), :], r_out[1, pl.ds(c, 1), :]
        ci, si = r_in[0], r_in[1]
        return ci * co - si * so, (ci * so + si * co) * sign

    for h, c in ((0, cl), (1, cu)):
        rs = slice(h * STRETCH, (h + 1) * STRETCH)
        cosine, sine = rope(h)
        kf = acckv[rs, 0:HD] * ssq[rs, :]
        kvbuf[2 * c] = (kf * cosine + pltpu.roll(kf, HD // 2, 1) * sine).astype(BF16)
        vf = acckv[rs, HD : 2 * HD] * ssq[rs, :]
        kvbuf[2 * c + 1, 0:HD, :] = vf[0:HD, :].T.astype(BF16)
        kvbuf[2 * c + 1, HD : 2 * HD, :] = vf[HD : 2 * HD, :].T.astype(BF16)

    pl.semaphore_wait(barrier, 7)

    def kv_copy(p, way):
        return pltpu.make_async_remote_copy(
            src_ref=kvbuf.at[p], dst_ref=kvbuf.at[p], send_sem=kv_send,
            recv_sem=kv_recv.at[p], device_id={"cp": beside[way], "tp": t},
        )

    def kv_wait(p):
        pltpu.make_async_remote_copy(
            src_ref=kvbuf.at[p], dst_ref=kvbuf.at[p], send_sem=kv_send,
            recv_sem=kv_recv.at[p], device_id={"cp": beside[0], "tp": t},
        ).wait_recv()

    def pass_on(e, act):
        p, ways = lax.rem(e, 64), lax.rem(lax.div(e, 64), 16)

        @pl.when(ways > 0)
        def _():
            for way in range(4):
                @pl.when(lax.rem(lax.div(ways, 2**way), 2) == 1)
                def _():
                    act(kv_copy(p, way))

    def send_only(i, carry):
        pass_on(chosen(words[:8], i), lambda c: c.start())
        return carry

    lax.fori_loop(0, at_query, send_only, 0)

    def wos_copy(i):
        cols = pl.ds(pl.multiple_of((2 * i + 1 - core) * 512, 512), 512)
        return pltpu.make_async_remote_copy(
            src_ref=wo.at[:, cols], dst_ref=wo_sib.at[i], send_sem=wos_send,
            recv_sem=wos_recv, device_id={"cp": d, "tp": sib},
        )

    for i in range(4):
        wos_copy(i).start()

    first_copies[0].wait()
    table = doc_in[...].reshape(64, 128)
    rows = [
        doc_in[pl.ds(pl.multiple_of(c * STRETCH, STRETCH), STRETCH)].reshape(1, STRETCH) for c in (cl, cu)
    ]
    starts = [jnp.zeros((1, STRETCH), F32) for _ in rows]
    for v in range(1, 16):
        below = jnp.where(table < v, 1.0, 0.0)
        count = jnp.sum(jnp.sum(below, axis=0, keepdims=True), axis=1, keepdims=True)
        starts = [jnp.where(r >= v, count, s) for r, s in zip(rows, starts)]
    qstart[0:1, :] = starts[0].astype(jnp.int32)
    qstart[1:2, :] = starts[1].astype(jnp.int32)
    m_ref[...] = jnp.full_like(m_ref, NEG)
    acc_ref[...] = jnp.zeros_like(acc_ref)

    wq_copy.wait()

    def q_step(i, carry):
        cols = pl.ds(pl.multiple_of(i * 256, 256), 256)
        accq[:, cols] = jnp.dot(xg[...], wqv[:, cols], preferred_element_type=F32)
        return carry

    lax.fori_loop(0, 2, q_step, 0)
    for h in range(2):
        rs = slice(h * STRETCH, (h + 1) * STRETCH)
        cosine, sine = rope(h)
        scale = ssq[rs, :] * QSCALE
        for g in range(GROUP):
            qf = accq[rs, g * HD : (g + 1) * HD] * scale
            qs[h, g * STRETCH : (g + 1) * STRETCH, :] = (
                qf * cosine + pltpu.roll(qf, HD // 2, 1) * sine
            ).astype(BF16)

    key_row = lax.broadcasted_iota(jnp.int32, (STRETCH, STRETCH), 0)
    query_col = lax.broadcasted_iota(jnp.int32, (STRETCH, STRETCH), 1)
    ones = jnp.ones((ONES, 2 * STRETCH), BF16)

    def attend(h, s1, s2):
        c = jnp.where(h == 0, cl, cu)
        keys = jnp.concatenate([kvbuf[2 * s1], kvbuf[2 * s2]], axis=0)
        vt = jnp.concatenate([kvbuf[2 * s + 1, r : r + HD, :] for s in (s1, s2) for r in (0, HD)], axis=1)
        vt = jnp.concatenate([vt, ones], axis=0)
        begin = qstart[pl.ds(h, 1), :]
        mask = jnp.concatenate(
            [
                (key_row >= begin - s * STRETCH) & (key_row <= query_col + (c - s) * STRETCH)
                for s in (s1, s2)
            ],
            axis=0,
        )
        scores = [
            lax.dot_general(
                keys, qs[h, g * STRETCH : (g + 1) * STRETCH, :], (((1,), (1,)), ((), ())),
                preferred_element_type=F32,
            )
            for g in range(GROUP)
        ]
        before = [m_ref[h, g : g + 1, :] for g in range(GROUP)]
        held = [acc_ref[h, g] for g in range(GROUP)]
        tops, added = [], []
        for g in range(GROUP):
            sc = jnp.where(mask, scores[g], NEG)
            top = jnp.maximum(jnp.max(sc, axis=0, keepdims=True), before[g])
            weights = jnp.exp2(sc - top).astype(BF16)
            tops.append(top)
            added.append(jnp.dot(vt, weights, preferred_element_type=F32))
        for g in range(GROUP):
            acc_ref[h, g] = held[g] * jnp.exp2(before[g] - tops[g]) + added[g]
            m_ref[h, g : g + 1, :] = tops[g]

    def finish(h):
        for g in range(GROUP):
            o = acc_ref[h, g, 0:HD, :] / acc_ref[h, g, HD : HD + 1, :]
            attn_own[h, :, g * HD : (g + 1) * HD] = o.T.astype(BF16)

    def at_copy(h):
        return pltpu.make_async_remote_copy(
            src_ref=attn_own.at[h], dst_ref=attn_sib.at[h], send_sem=rs_send,
            recv_sem=at_recv.at[h], device_id={"cp": d, "tp": sib},
        )

    def project(h, i):
        zz = zs[i]
        return jnp.dot(attn_own[h], wo_own[zz], preferred_element_type=F32) + jnp.dot(
            attn_sib[h], wo_sib[zz], preferred_element_type=F32
        )

    def a_copy(h, way):
        return pltpu.make_async_remote_copy(
            src_ref=send_a.at[h, way], dst_ref=recv_a.at[h, way], send_sem=rs_send,
            recv_sem=a_recv.at[h, way], device_id={"cp": d, "tp": t_up if way == 0 else t_dn},
        )

    def b_copy(h, way, piece):
        return pltpu.make_async_remote_copy(
            src_ref=send_b.at[h, way, piece], dst_ref=recv_b.at[h, way, piece],
            send_sem=rs_send, recv_sem=b_recv.at[h],
            device_id={"cp": d, "tp": t_up if way == 0 else t_dn},
        )

    summed = [slice(0, 256), slice(256, 512)]
    plain = [slice(256, 512), slice(0, 256)]

    def own_part(h):
        for j, i in enumerate((3, 1, 2)):
            part[j] = jnp.dot(attn_own[h], wo_own[zs[i]], preferred_element_type=F32)

    def with_sibling(h, j, i):
        return part[j] + jnp.dot(attn_sib[h], wo_sib[zs[i]], preferred_element_type=F32)

    def scatter_first(h):
        at_copy(h).wait_recv()
        far = with_sibling(h, 0, 3)
        for way in range(2):
            send_a[h, way] = far[:, summed[way]].astype(BF16)
            a_copy(h, way).start()
        for way in range(2):
            near = with_sibling(h, 1 + way, 1 + way)
            accq[of(h), way * 256 : (way + 1) * 256] = near[:, summed[way]]
            send_b[h, way, 1] = near[:, plain[way]].astype(BF16)
            b_copy(h, way, 1).start()

    def scatter_second(h):
        for way in range(2):
            a_copy(h, way).wait_recv()
            own = accq[of(h), way * 256 : (way + 1) * 256]
            send_b[h, way, 0] = (own + recv_a[h, way].astype(F32)).astype(BF16)
            b_copy(h, way, 0).start()

    def scatter_mine(h):
        accq[of(h), :] = project(h, 0)

    def scatter_last(h):
        rs = of(h)
        pltpu.make_async_copy(recv_b.at[h], recv_b.at[h], b_recv.at[h]).wait()
        out[rs, 0:256] = (
            accq[rs, 0:256] + recv_b[h, 0, 0].astype(F32) + recv_b[h, 1, 1].astype(F32)
        ).astype(BF16)
        out[rs, 256:512] = (
            accq[rs, 256:512] + recv_b[h, 0, 1].astype(F32) + recv_b[h, 1, 0].astype(F32)
        ).astype(BF16)

    def weights_here():
        pltpu.make_async_copy(wo_sib, wo_sib, wos_recv).wait()

    def main_step(i, near):
        e = chosen(list(near), lax.rem(i, 8))
        p = lax.rem(e, 64)
        kind = lax.rem(lax.div(e, 1024), 4)
        job = lax.rem(lax.div(e, 4096), 4)
        s1, s2 = lax.rem(lax.div(e, 16384), 32), lax.div(e, 524288)

        @pl.when(kind == 1)
        def _():
            kv_wait(p)

        @pl.when(kind == 2)
        def _():
            kv_wait(p)
            kv_wait(p + 1)

        pass_on(e, lambda c: c.start())

        @pl.when(job > 0)
        def _():
            attend(job - 1, s1, s2)

        @pl.when(i == at_whole)
        def _():
            finish(early)
            at_copy(early).start()
            pltpu.make_async_copy(wo_own, wo_own, wo_sem).wait()
            own_part(early)

        @pl.when(i == at_first)
        def _():
            weights_here()
            scatter_first(early)

        @pl.when(i == at_second)
        def _():
            scatter_second(early)
            scatter_mine(early)

        return near

    def group_step(group, carry):
        low = jnp.maximum(at_query, group * 8)
        high = jnp.minimum(n_entries, group * 8 + 8)
        lax.fori_loop(low, high, main_step, tuple(entries(group)))
        return carry

    lax.fori_loop(lax.div(at_query, 8), lax.div(n_entries + 7, 8), group_step, 0)
    finish(late)
    at_copy(late).start()

    @pl.when(at_first >= n_entries)
    def _():
        weights_here()
        scatter_first(early)

    own_part(late)
    scatter_first(late)

    @pl.when(at_second >= n_entries)
    def _():
        scatter_second(early)
        scatter_mine(early)

    scatter_second(late)
    scatter_mine(late)
    scatter_last(early)
    scatter_last(late)
    for count in sorted(set(SENDS)):
        @pl.when(n_sends == count)
        def _():
            pltpu.make_async_copy(kvbuf.at[0:count], kvbuf.at[0:count], kv_send).wait()
    pltpu.make_async_copy(wo_sib, wo_sib, wos_send).wait()
    pltpu.make_async_copy(wo_own, wo_own, rs_send).wait()


def step(tokens, gain, w_query, w_key, w_value, w_out, doc_ids):
    rope_in, rope_out = rope_tables()
    any_space = pl.BlockSpec(memory_space=pl.ANY)
    rows = 2 * STRETCH
    dma = pltpu.SemaphoreType.DMA
    return pl.pallas_call(
        kernel,
        out_shape=pltpu.VMEM((rows, 512), BF16),
        in_specs=[any_space] * 9,
        out_specs=pl.BlockSpec(memory_space=pltpu.VMEM),
        scratch_shapes=[
            pltpu.VMEM((rows, D), BF16),
            pltpu.VMEM((rows, D), BF16),
            pltpu.VMEM((D, 2 * HD), BF16),
            pltpu.VMEM((D, GROUP * HD), BF16),
            pltpu.VMEM((4, 512, 512), BF16),
            pltpu.VMEM((4, 512, 512), BF16),
            pltpu.VMEM((rows, 2 * HD), F32),
            pltpu.VMEM((rows, GROUP * HD), F32),
            pltpu.VMEM((rows, HD), F32),
            pltpu.VMEM((4 * N_CP, STRETCH, HD), BF16),
            pltpu.VMEM((2, GROUP * STRETCH, HD), BF16),
            pltpu.VMEM((2, 8, STRETCH), F32),
            pltpu.VMEM((2, GROUP, HD + ONES, STRETCH), F32),
            pltpu.VMEM((2, STRETCH, 512), BF16),
            pltpu.VMEM((2, STRETCH, 512), BF16),
            pltpu.VMEM((2, 2, STRETCH, 256), BF16),
            pltpu.VMEM((2, 2, STRETCH, 256), BF16),
            pltpu.VMEM((2, 2, 2, STRETCH, 256), BF16),
            pltpu.VMEM((2, 2, 2, STRETCH, 256), BF16),
            pltpu.VMEM((8, STRETCH), jnp.int32),
            pltpu.VMEM((D,), BF16),
            pltpu.VMEM((1, D), F32),
            pltpu.VMEM((2 * N_CP * STRETCH,), jnp.int32),
            pltpu.VMEM((2, STRETCH, HD), F32),
            pltpu.VMEM((2, 2 * N_CP, HD), F32),
            pltpu.VMEM((3, STRETCH, 512), F32),
            dma((7,)),
            dma((N_CHUNK,)),
            dma,
            dma,
            dma,
            dma,
            dma((4 * N_CP,)),
            dma,
            dma((2,)),
            dma((2, 2)),
            dma((2,)),
        ],
        compiler_params=pltpu.CompilerParams(
            collective_id=0, has_side_effects=True, vmem_limit_bytes=60 * 1024 * 1024
        ),
        name="block",
    )(
        tokens, gain, w_query, w_key, w_value, w_out,
        doc_ids, jnp.asarray(rope_in), jnp.asarray(rope_out),
    )


def solution(mesh):
    in_specs = (P("cp", None), P(), P(None, "tp"), P(None, "tp"), P(None, "tp"), P("tp", None), P())
    return jax.shard_map(step, mesh=mesh, in_specs=in_specs, out_specs=P("cp", "tp"), check_vma=False)
```

```python
import math

import jax
import jax.numpy as jnp
import numpy as np
from jax import lax
from jax.experimental import pallas as pl
from jax.experimental.pallas import tpu as pltpu
from jax.sharding import PartitionSpec as P

D = 4096
HEADS = 32
HD = 128
GROUP = 4
STRETCH = 256
N_CP = 16
REACH = 9
CHUNK = 512
N_CHUNK = D // CHUNK
NEG = -1e30
EPS = 1e-05
THETA = 500000.0
QSCALE = math.log2(math.e) / math.sqrt(HD)
ONES = 16
F32 = jnp.float32
BF16 = jnp.bfloat16

TABLE = [
    [448, 449, 16260096, 1270, 1079, 2104, 14673980, 1262, 1073, 16196660, 183, 1136, 12461103, 111, 1077, 175, 181, 119, 1196, 11969581, 2098, 15624250],
    [323, 322, 188, 189, 1345, 1204, 1082, 116, 186, 1077, 1083, 21504, 117, 14131381, 1068, 1075, 1261, 12018745, 1074, 178, 108, 1070, 1080, 15098043, 2096, 1135, 12462122, 14510134],
    [324, 325, 186, 187, 1347, 1203, 1081, 115, 185, 1026, 1074, 562232, 66, 13590706, 1281, 1024, 1066, 106, 15208632, 1073, 1067, 1140, 11477169, 1077, 1072, 13017202, 1069, 2088, 109, 11871276, 2102, 12511278],
    [262, 263, 249, 248, 1284, 1152, 1137, 177, 1029, 1281, 1072, 1101936, 261, 13050032, 1027, 1064, 259, 168, 1078, 1139, 182, 1065, 529410, 1198, 1207, 1071, 2090, 14492724, 11398144, 1077, 13542450, 2092, 10332198],
    [456, 457, 566, 567, 1472, 1582, 1072, 110, 174, 1025, 1071, 1073, 2100, 559, 69889, 111, 12509359, 1286, 1026, 70, 14033026, 1580, 1064, 1065, 172, 105, 1283, 1031, 2086, 1593415, 263, 1028, 1197, 10297457, 260, 1061, 165, 9806884, 14193925, 2090, 13461554],
    [331, 330, 692, 693, 1474, 1032, 1580, 1074, 72, 172, 1027, 1069, 1289, 1075, 610861, 131, 109, 11968771, 1028, 1024, 1061, 1025, 132, 64, 69896, 1578, 1070, 1067, 165, 108, 11428100, 1029, 1060, 1071, 111, 261, 178, 12362283, 1062, 1030, 102, 257, 179, 2082, 1611015, 1063, 2088, 10250288, 12921856],
    [333, 332, 691, 690, 1412, 1099, 1578, 1072, 170, 267, 1029, 1034, 1131, 1073, 1151531, 133, 74, 11428101, 1030, 1026, 1058, 1027, 262, 176, 610410, 1577, 2056, 259, 162, 98, 1031, 1643560, 2048, 263, 168, 13112419, 2080, 2092, 10887426, 2094, 2084, 8676390, 12430336, 10265639],
    [271, 270, 753, 752, 1478, 1033, 1037, 1576, 137, 269, 1031, 1036, 1129, 1032, 1692201, 135, 71, 2199815, 1028, 1035, 1185, 10887435, 1070, 1643, 2048, 260, 1184, 1029, 1071, 1034, 69, 174, 265, 1053727, 2050, 1066, 610565, 1574, 12330018, 1191, 2092, 1059, 10314279, 2084, 9282590, 8170496],
    [558, 559, 465, 464, 1766, 1064, 1289, 1068, 104, 552, 1063, 1069, 1160, 1065, 10346760, 103, 167, 10854951, 1061, 1060, 1121, 1024, 164, 2232877, 1025, 1359, 1067, 1056, 165, 8692260, 1055, 1066, 1054, 95, 8217130, 1286, 2082, 64, 1034, 266, 70, 3675150, 2050, 7628828, 1287, 1035, 1594381, 1036, 3233796, 12098560],
    [339, 684, 338, 685, 1765, 1067, 1291, 1040, 171, 555, 1060, 1066, 1098, 9807121, 100, 170, 266, 2773540, 1062, 1058, 1154, 102, 550, 9266211, 1289, 2088, 138, 80, 547, 1052, 1063, 1037, 1027, 269, 156, 103, 10297895, 1036, 1032, 2080, 268, 141, 659528, 1039, 1053, 73, 7610639, 2074, 2078, 8087556, 1038, 2201600, 3708934, 1580032],
    [683, 682, 341, 340, 1762, 1065, 1298, 1037, 169, 553, 1059, 1100, 1043, 1064, 9265421, 99, 268, 141, 3314216, 1061, 1052, 92, 140, 1053, 7676451, 1290, 1035, 2080, 157, 549, 2773074, 1050, 1060, 2052, 90, 9708068, 1166, 2078, 74, 1051, 7070736, 1039, 3708966, 2054, 6613016, 2050, 1041, 579592, 2235392],
    [744, 745, 278, 279, 6106112, 1761, 1295, 1044, 1056, 1038, 1045, 2064, 270, 160, 79, 3854880, 277, 1055, 95, 159, 4362783, 1058, 1062, 1054, 276, 98, 142, 8135206, 1037, 1036, 78, 269, 143, 1049, 1575, 2054, 9233443, 1099, 1572, 2076, 1675417, 1048, 1061, 76, 6529566, 2056, 7120922, 1120260, 1034, 4806674],
    [550, 551, 216, 217, 6614016, 1572, 1120, 1169, 1040, 1054, 1061, 544, 94, 4395152, 542, 80, 1055, 8168474, 1033, 95, 1571, 1053, 1032, 72, 541, 1057, 7611420, 1110, 1058, 6054935, 5837851, 5466132, 2062, 3838987, 1034, 2066, 4805645, 2054, 3200012],
    [677, 676, 90, 91, 539, 7119002, 1059, 1107, 1049, 547, 163, 1052, 1048, 4924434, 540, 88, 6508700, 1058, 1035, 162, 1568, 89, 7627805, 1566, 155, 75, 1044, 1034, 2064, 538, 2773140, 1057, 1055, 8134795, 1045, 2056, 5378194, 1037, 5941270, 5837964, 3774478],
    [546, 675, 220, 93, 162, 7627292, 1054, 1114, 1045, 541, 157, 1051, 1057, 5465108, 91, 538, 7049364, 1056, 1042, 542, 161, 82, 4989971, 1037, 1055, 83, 539, 4886677, 1048, 1047, 1036, 536, 151, 76, 6022166, 5870617, 1553, 2824202, 4400144, 1166, 3806223],
    [673, 608, 222, 543, 95, 8134816, 1053, 1046, 1048, 542, 159, 93, 1052, 1049, 6530071, 97, 151, 7590425, 150, 541, 5967958, 1041, 1050, 1039, 536, 87, 145, 1038, 3859472, 1051, 144, 1109, 6955547, 1042, 78, 4313230, 1044, 1555, 143, 4890707, 1037, 77, 5461004, 3300352],
]
CUT = 8
MARKS = [
    [2, 4, 4, 4, 4, 4, 4, 4, 4, 4, 4, 4, 4, 4, 4, 3],
    [2, 11, 18, 22, 38, 44, 35, 36, 43, 49, 44, 46, 31, 38, 38, 39],
    [6, 15, 22, 23, 200, 200, 38, 39, 46, 51, 47, 200, 33, 39, 200, 200],
    [17, 24, 29, 31, 200, 200, 200, 200, 200, 200, 200, 200, 200, 200, 200, 200],
    [22, 28, 32, 33, 41, 49, 44, 46, 50, 54, 49, 50, 39, 41, 41, 44],
]
ENTRIES = max(len(row) for row in TABLE)
SENDS = [sum((e // (64 << k)) % 2 for e in row for k in range(4)) for row in TABLE]


def rope_tables():
    half = HD // 2
    freqs = THETA ** (-2.0 * np.arange(half) / HD)
    inner = np.arange(STRETCH)[:, None] * freqs[None, :]
    outer = (np.arange(2 * N_CP) * STRETCH)[:, None] * freqs[None, :]

    def both(angles):
        c, s = np.cos(angles), np.sin(angles)
        return np.stack([np.concatenate([c, c], 1), np.concatenate([s, s], 1)])

    return both(inner).astype(np.float32), both(outer).astype(np.float32)


def kernel(
    tokens, gain, wq, wk, wv, wo, docs, rope_in, rope_out, out,
    x, xg, wkv, wqv, wo_own, wo_sib, acckv, accq, ssq, kvbuf, qs,
    m_ref, acc_ref, attn_own, attn_sib, send_a, recv_a, send_b, recv_b, qstart,
    gain_in, gain_row, doc_in, r_in, r_out, part,
    in_sems, x_sems, wo_sem, wos_send, wos_recv, kv_send, kv_recv,
    rs_send, at_recv, a_recv, b_recv,
):
    d = lax.axis_index("cp")
    t = lax.axis_index("tp")
    z, core = t // 2, t % 2
    sib = t + 1 - 2 * core
    t_up = lax.rem(z + 1, 4) * 2 + core
    t_dn = lax.rem(z + 3, 4) * 2 + core
    zs = [z, lax.rem(z + 1, 4), lax.rem(z + 3, 4), lax.rem(z + 2, 4)]
    cl, cu = d, 2 * N_CP - 1 - d
    early = jnp.where(d < CUT, 0, 1)
    late = 1 - early

    def of(h):
        return pl.ds(pl.multiple_of(h * STRETCH, STRETCH), STRETCH)

    px, py = lax.rem(d, 4), lax.div(d, 4)
    beside = [
        py * 4 + lax.rem(px + 1, 4),
        py * 4 + lax.rem(px + 3, 4),
        lax.rem(py + 1, 4) * 4 + px,
        lax.rem(py + 3, 4) * 4 + px,
    ]

    def x_copy(i):
        cols = pl.ds(i * CHUNK, CHUNK)
        return pltpu.make_async_copy(tokens.at[:, cols], x.at[:, cols], x_sems.at[i])

    first_copies = [
        pltpu.make_async_copy(docs, doc_in, in_sems.at[0]),
        pltpu.make_async_copy(gain, gain_in, in_sems.at[1]),
        pltpu.make_async_copy(wk, wkv.at[:, 0:HD], in_sems.at[2]),
        pltpu.make_async_copy(wv, wkv.at[:, HD : 2 * HD], in_sems.at[3]),
    ]
    rope_copies = [
        pltpu.make_async_copy(rope_in, r_in, in_sems.at[4]),
        pltpu.make_async_copy(rope_out, r_out, in_sems.at[5]),
    ]
    wq_copy = pltpu.make_async_copy(wq, wqv, in_sems.at[6])

    def wo_copy(i):
        cols = pl.ds(pl.multiple_of((2 * i + core) * 512, 512), 512)
        return pltpu.make_async_copy(wo.at[:, cols], wo_own.at[i], wo_sem)

    first_copies[1].start()
    for i in range(N_CHUNK):
        x_copy(i).start()
    for c in (first_copies[2], first_copies[3], first_copies[0]):
        c.start()
    for c in rope_copies:
        c.start()

    barrier = pltpu.get_barrier_semaphore()
    for e in beside:
        pl.semaphore_signal(barrier, 1, device_id={"cp": e, "tp": t})
    for other in (sib, t_up, t_dn):
        pl.semaphore_signal(barrier, 1, device_id={"cp": d, "tp": other})

    here = [(d == e).astype(jnp.int32) for e in range(N_CP)]

    def pick(values):
        total = jnp.int32(0)
        for e, v in enumerate(values):
            if v:
                total = total + here[e] * v
        return total

    words = [pick([row[i] if i < len(row) else 0 for row in TABLE]) for i in range(ENTRIES)]

    def chosen(values, i):
        while len(values) > 1:
            low = lax.rem(i, 2) == 0
            values = [
                jnp.where(low, values[k], values[k + 1]) if k + 1 < len(values) else values[k]
                for k in range(0, len(values), 2)
            ]
            i = lax.div(i, 2)
        return values[0]

    def entries(group):
        return [chosen(words[k::8], group) for k in range(8)]

    at_query, at_whole, at_first, at_second, n_entries = [pick(m) for m in MARKS]
    n_sends = pick(SENDS)

    ssq[...] = jnp.zeros_like(ssq)
    first_copies[1].wait()
    for i in range(N_CHUNK):
        cols = slice(i * CHUNK, (i + 1) * CHUNK)
        gain_row[:, cols] = gain_in[cols].astype(F32).reshape(1, CHUNK)

    def scale_chunk(i):
        x_copy(i).wait()
        cols = pl.ds(pl.multiple_of(i * CHUNK, CHUNK), CHUNK)
        xf = x[:, cols].astype(F32)
        sq = xf * xf
        ssq[...] += sq[:, 0:128] + sq[:, 128:256] + sq[:, 256:384] + sq[:, 384:512]
        xg[:, cols] = (xf * gain_row[:, cols]).astype(BF16)

    def scale_step(i, carry):
        @pl.when(i == N_CHUNK - 1)
        def _():
            wq_copy.start()

        scale_chunk(i)
        return carry

    lax.fori_loop(0, N_CHUNK, scale_step, 0)
    for c in first_copies[2:]:
        c.wait()
    acckv[...] = jnp.dot(xg[...], wkv[...], preferred_element_type=F32)
    for i in range(4):
        wo_copy(i).start()
    for c in rope_copies:
        c.wait()
    mean = jnp.sum(ssq[...], axis=1, keepdims=True) * (1.0 / D)
    factor = lax.rsqrt(mean + EPS)
    ssq[...] = jnp.broadcast_to(factor, (2 * STRETCH, HD))

    sign = jnp.where(lax.broadcasted_iota(jnp.int32, (1, HD), 1) < HD // 2, -1.0, 1.0)

    def rope(h):
        c = cl if h == 0 else cu
        co, so = r_out[0, pl.ds(c, 1), :], r_out[1, pl.ds(c, 1), :]
        ci, si = r_in[0], r_in[1]
        return ci * co - si * so, (ci * so + si * co) * sign

    for h, c in ((0, cl), (1, cu)):
        rs = slice(h * STRETCH, (h + 1) * STRETCH)
        cosine, sine = rope(h)
        kf = acckv[rs, 0:HD] * ssq[rs, :]
        kvbuf[2 * c] = (kf * cosine + pltpu.roll(kf, HD // 2, 1) * sine).astype(BF16)
        vf = acckv[rs, HD : 2 * HD] * ssq[rs, :]
        kvbuf[2 * c + 1, 0:HD, :] = vf[0:HD, :].T.astype(BF16)
        kvbuf[2 * c + 1, HD : 2 * HD, :] = vf[HD : 2 * HD, :].T.astype(BF16)

    pl.semaphore_wait(barrier, 7)

    def kv_copy(p, way):
        return pltpu.make_async_remote_copy(
            src_ref=kvbuf.at[p], dst_ref=kvbuf.at[p], send_sem=kv_send,
            recv_sem=kv_recv.at[p], device_id={"cp": beside[way], "tp": t},
        )

    def kv_wait(p):
        pltpu.make_async_remote_copy(
            src_ref=kvbuf.at[p], dst_ref=kvbuf.at[p], send_sem=kv_send,
            recv_sem=kv_recv.at[p], device_id={"cp": beside[0], "tp": t},
        ).wait_recv()

    def pass_on(e, act):
        p, ways = lax.rem(e, 64), lax.rem(lax.div(e, 64), 16)

        @pl.when(ways > 0)
        def _():
            for way in range(4):
                @pl.when(lax.rem(lax.div(ways, 2**way), 2) == 1)
                def _():
                    act(kv_copy(p, way))

    def send_only(i, carry):
        pass_on(chosen(words[:8], i), lambda c: c.start())
        return carry

    lax.fori_loop(0, at_query, send_only, 0)

    def wos_copy(i):
        cols = pl.ds(pl.multiple_of((2 * i + 1 - core) * 512, 512), 512)
        return pltpu.make_async_remote_copy(
            src_ref=wo.at[:, cols], dst_ref=wo_sib.at[i], send_sem=wos_send,
            recv_sem=wos_recv, device_id={"cp": d, "tp": sib},
        )

    for i in range(4):
        wos_copy(i).start()

    first_copies[0].wait()
    table = doc_in[...].reshape(64, 128)
    rows = [
        doc_in[pl.ds(pl.multiple_of(c * STRETCH, STRETCH), STRETCH)].reshape(1, STRETCH) for c in (cl, cu)
    ]
    starts = [jnp.zeros((1, STRETCH), F32) for _ in rows]
    for v in range(1, 16):
        below = jnp.where(table < v, 1.0, 0.0)
        count = jnp.sum(jnp.sum(below, axis=0, keepdims=True), axis=1, keepdims=True)
        starts = [jnp.where(r >= v, count, s) for r, s in zip(rows, starts)]
    qstart[0:1, :] = starts[0].astype(jnp.int32)
    qstart[1:2, :] = starts[1].astype(jnp.int32)
    m_ref[...] = jnp.full_like(m_ref, NEG)
    acc_ref[...] = jnp.zeros_like(acc_ref)

    wq_copy.wait()

    def q_step(i, carry):
        cols = pl.ds(pl.multiple_of(i * 256, 256), 256)
        accq[:, cols] = jnp.dot(xg[...], wqv[:, cols], preferred_element_type=F32)
        return carry

    lax.fori_loop(0, 2, q_step, 0)
    for h in range(2):
        rs = slice(h * STRETCH, (h + 1) * STRETCH)
        cosine, sine = rope(h)
        scale = ssq[rs, :] * QSCALE
        for g in range(GROUP):
            qf = accq[rs, g * HD : (g + 1) * HD] * scale
            qs[h, g * STRETCH : (g + 1) * STRETCH, :] = (
                qf * cosine + pltpu.roll(qf, HD // 2, 1) * sine
            ).astype(BF16)

    key_row = lax.broadcasted_iota(jnp.int32, (STRETCH, STRETCH), 0)
    query_col = lax.broadcasted_iota(jnp.int32, (STRETCH, STRETCH), 1)
    ones = jnp.ones((ONES, 2 * STRETCH), BF16)

    def attend(h, s1, s2):
        c = jnp.where(h == 0, cl, cu)
        keys = jnp.concatenate([kvbuf[2 * s1], kvbuf[2 * s2]], axis=0)
        vt = jnp.concatenate([kvbuf[2 * s + 1, r : r + HD, :] for s in (s1, s2) for r in (0, HD)], axis=1)
        vt = jnp.concatenate([vt, ones], axis=0)
        begin = qstart[pl.ds(h, 1), :]
        mask = jnp.concatenate(
            [
                (key_row >= begin - s * STRETCH) & (key_row <= query_col + (c - s) * STRETCH)
                for s in (s1, s2)
            ],
            axis=0,
        )
        scores = [
            lax.dot_general(
                keys, qs[h, g * STRETCH : (g + 1) * STRETCH, :], (((1,), (1,)), ((), ())),
                preferred_element_type=F32,
            )
            for g in range(GROUP)
        ]
        before = [m_ref[h, g : g + 1, :] for g in range(GROUP)]
        held = [acc_ref[h, g] for g in range(GROUP)]
        tops, added = [], []
        for g in range(GROUP):
            sc = jnp.where(mask, scores[g], NEG)
            top = jnp.maximum(jnp.max(sc, axis=0, keepdims=True), before[g])
            weights = jnp.exp2(sc - top).astype(BF16)
            tops.append(top)
            added.append(jnp.dot(vt, weights, preferred_element_type=F32))
        for g in range(GROUP):
            acc_ref[h, g] = held[g] * jnp.exp2(before[g] - tops[g]) + added[g]
            m_ref[h, g : g + 1, :] = tops[g]

    def finish(h):
        for g in range(GROUP):
            o = acc_ref[h, g, 0:HD, :] / acc_ref[h, g, HD : HD + 1, :]
            attn_own[h, :, g * HD : (g + 1) * HD] = o.T.astype(BF16)

    def at_copy(h):
        return pltpu.make_async_remote_copy(
            src_ref=attn_own.at[h], dst_ref=attn_sib.at[h], send_sem=rs_send,
            recv_sem=at_recv.at[h], device_id={"cp": d, "tp": sib},
        )

    def project(h, i):
        zz = zs[i]
        return jnp.dot(attn_own[h], wo_own[zz], preferred_element_type=F32) + jnp.dot(
            attn_sib[h], wo_sib[zz], preferred_element_type=F32
        )

    def a_copy(h, way):
        return pltpu.make_async_remote_copy(
            src_ref=send_a.at[h, way], dst_ref=recv_a.at[h, way], send_sem=rs_send,
            recv_sem=a_recv.at[h, way], device_id={"cp": d, "tp": t_up if way == 0 else t_dn},
        )

    def b_copy(h, way, piece):
        return pltpu.make_async_remote_copy(
            src_ref=send_b.at[h, way, piece], dst_ref=recv_b.at[h, way, piece],
            send_sem=rs_send, recv_sem=b_recv.at[h],
            device_id={"cp": d, "tp": t_up if way == 0 else t_dn},
        )

    summed = [slice(0, 256), slice(256, 512)]
    plain = [slice(256, 512), slice(0, 256)]

    def own_part(h):
        for j, i in enumerate((3, 1, 2)):
            part[j] = jnp.dot(attn_own[h], wo_own[zs[i]], preferred_element_type=F32)

    def with_sibling(h, j, i):
        return part[j] + jnp.dot(attn_sib[h], wo_sib[zs[i]], preferred_element_type=F32)

    def scatter_first(h):
        at_copy(h).wait_recv()
        far = with_sibling(h, 0, 3)
        for way in range(2):
            send_a[h, way] = far[:, summed[way]].astype(BF16)
            a_copy(h, way).start()
        for way in range(2):
            near = with_sibling(h, 1 + way, 1 + way)
            accq[of(h), way * 256 : (way + 1) * 256] = near[:, summed[way]]
            send_b[h, way, 1] = near[:, plain[way]].astype(BF16)
            b_copy(h, way, 1).start()

    def scatter_second(h):
        for way in range(2):
            a_copy(h, way).wait_recv()
            own = accq[of(h), way * 256 : (way + 1) * 256]
            send_b[h, way, 0] = (own + recv_a[h, way].astype(F32)).astype(BF16)
            b_copy(h, way, 0).start()

    def scatter_mine(h):
        accq[of(h), :] = project(h, 0)

    def scatter_last(h):
        rs = of(h)
        pltpu.make_async_copy(recv_b.at[h], recv_b.at[h], b_recv.at[h]).wait()
        out[rs, 0:256] = (
            accq[rs, 0:256] + recv_b[h, 0, 0].astype(F32) + recv_b[h, 1, 1].astype(F32)
        ).astype(BF16)
        out[rs, 256:512] = (
            accq[rs, 256:512] + recv_b[h, 0, 1].astype(F32) + recv_b[h, 1, 0].astype(F32)
        ).astype(BF16)

    def weights_here():
        pltpu.make_async_copy(wo_sib, wo_sib, wos_recv).wait()

    def main_step(i, near):
        e = chosen(list(near), lax.rem(i, 8))
        p = lax.rem(e, 64)
        kind = lax.rem(lax.div(e, 1024), 4)
        job = lax.rem(lax.div(e, 4096), 4)
        s1, s2 = lax.rem(lax.div(e, 16384), 32), lax.div(e, 524288)

        @pl.when(kind == 1)
        def _():
            kv_wait(p)

        @pl.when(kind == 2)
        def _():
            kv_wait(p)
            kv_wait(p + 1)

        pass_on(e, lambda c: c.start())

        @pl.when(job > 0)
        def _():
            attend(job - 1, s1, s2)

        @pl.when(i == at_whole)
        def _():
            finish(early)
            at_copy(early).start()
            pltpu.make_async_copy(wo_own, wo_own, wo_sem).wait()
            own_part(early)

        @pl.when(i == at_first)
        def _():
            weights_here()
            scatter_first(early)

        @pl.when(i == at_second)
        def _():
            scatter_second(early)
            scatter_mine(early)

        return near

    def group_step(group, carry):
        low = jnp.maximum(at_query, group * 8)
        high = jnp.minimum(n_entries, group * 8 + 8)
        lax.fori_loop(low, high, main_step, tuple(entries(group)))
        return carry

    lax.fori_loop(lax.div(at_query, 8), lax.div(n_entries + 7, 8), group_step, 0)
    finish(late)
    at_copy(late).start()

    @pl.when(at_first >= n_entries)
    def _():
        weights_here()
        scatter_first(early)

    own_part(late)
    scatter_first(late)

    @pl.when(at_second >= n_entries)
    def _():
        scatter_second(early)
        scatter_mine(early)

    scatter_second(late)
    scatter_mine(late)
    scatter_last(early)
    scatter_last(late)
    for count in sorted(set(SENDS)):
        @pl.when(n_sends == count)
        def _():
            pltpu.make_async_copy(kvbuf.at[0:count], kvbuf.at[0:count], kv_send).wait()
    pltpu.make_async_copy(wo_sib, wo_sib, wos_send).wait()
    pltpu.make_async_copy(wo_own, wo_own, rs_send).wait()


def step(tokens, gain, w_query, w_key, w_value, w_out, doc_ids):
    rope_in, rope_out = rope_tables()
    any_space = pl.BlockSpec(memory_space=pl.ANY)
    rows = 2 * STRETCH
    dma = pltpu.SemaphoreType.DMA
    return pl.pallas_call(
        kernel,
        out_shape=pltpu.VMEM((rows, 512), BF16),
        in_specs=[any_space] * 9,
        out_specs=pl.BlockSpec(memory_space=pltpu.VMEM),
        scratch_shapes=[
            pltpu.VMEM((rows, D), BF16),
            pltpu.VMEM((rows, D), BF16),
            pltpu.VMEM((D, 2 * HD), BF16),
            pltpu.VMEM((D, GROUP * HD), BF16),
            pltpu.VMEM((4, 512, 512), BF16),
            pltpu.VMEM((4, 512, 512), BF16),
            pltpu.VMEM((rows, 2 * HD), F32),
            pltpu.VMEM((rows, GROUP * HD), F32),
            pltpu.VMEM((rows, HD), F32),
            pltpu.VMEM((4 * N_CP, STRETCH, HD), BF16),
            pltpu.VMEM((2, GROUP * STRETCH, HD), BF16),
            pltpu.VMEM((2, 8, STRETCH), F32),
            pltpu.VMEM((2, GROUP, HD + ONES, STRETCH), F32),
            pltpu.VMEM((2, STRETCH, 512), BF16),
            pltpu.VMEM((2, STRETCH, 512), BF16),
            pltpu.VMEM((2, 2, STRETCH, 256), BF16),
            pltpu.VMEM((2, 2, STRETCH, 256), BF16),
            pltpu.VMEM((2, 2, 2, STRETCH, 256), BF16),
            pltpu.VMEM((2, 2, 2, STRETCH, 256), BF16),
            pltpu.VMEM((8, STRETCH), jnp.int32),
            pltpu.VMEM((D,), BF16),
            pltpu.VMEM((1, D), F32),
            pltpu.VMEM((2 * N_CP * STRETCH,), jnp.int32),
            pltpu.VMEM((2, STRETCH, HD), F32),
            pltpu.VMEM((2, 2 * N_CP, HD), F32),
            pltpu.VMEM((3, STRETCH, 512), F32),
            dma((7,)),
            dma((N_CHUNK,)),
            dma,
            dma,
            dma,
            dma,
            dma((4 * N_CP,)),
            dma,
            dma((2,)),
            dma((2, 2)),
            dma((2,)),
        ],
        compiler_params=pltpu.CompilerParams(
            collective_id=0, has_side_effects=True, vmem_limit_bytes=60 * 1024 * 1024
        ),
        name="block",
    )(
        tokens, gain, w_query, w_key, w_value, w_out,
        doc_ids, jnp.asarray(rope_in), jnp.asarray(rope_out),
    )


def solution(mesh):
    in_specs = (P("cp", None), P(), P(None, "tp"), P(None, "tp"), P(None, "tp"), P("tp", None), P())
    return jax.shard_map(step, mesh=mesh, in_specs=in_specs, out_specs=P("cp", "tp"), check_vma=False)
```
